8 devices in a mesh: dp: 1 (over z), sp: 8 (over y, x, core).
Axes of the slice: x: 2, y: 2, z: 1, core: 2. Of those that a mesh axis runs over, the one named last changes fastest.
Arguments:
- patches: bfloat16 [2, 2048, 1536], P('dp', 'sp')
- vis_mask: int32 [2, 2048], P('dp', 'sp')
- enc_pos: bfloat16 [2048, 1280], P(('dp', 'sp'))
- dec_pos: bfloat16 [2048, 512], P(('dp', 'sp'))
- w_pe: bfloat16 [1536, 1280], replicated
- b_pe: bfloat16 [1280], replicated
- enc_qkv: bfloat16 [2, 1280, 3, 16, 80], replicated
- enc_proj: bfloat16 [2, 16, 80, 1280], replicated
- enc_up: bfloat16 [2, 1280, 5120], replicated
- enc_down: bfloat16 [2, 5120, 1280], replicated
- w_ed: bfloat16 [1280, 512], replicated
- mask_token: bfloat16 [512], replicated
- dec_qkv: bfloat16 [2, 512, 3, 16, 32], replicated
- dec_proj: bfloat16 [2, 16, 32, 512], replicated
- dec_up: bfloat16 [2, 512, 2048], replicated
- dec_down: bfloat16 [2, 2048, 512], replicated
- w_out: bfloat16 [512, 1536], replicated
Outputs:
- output: float32 [2, 2048, 1536], P('dp', 'sp')
All inputs are finite; a program needn't handle non-finite values.
Results may differ from the reference program's by a relative error of at most 0.0159664.
Values are sent between devices in bfloat16 or wider.
A program may use at most 1 GiB of HBM per device.

```python
import jax
import jax.numpy as jnp
from jax import lax

P = 1536
D = 1280
ENC_HEADS = 16
DD = 512
DEC_HEADS = 16
TOK_DEV = 256
SP = 8
KEEP_DIV = 8
CLIPS = 2
LAYERS = 2

SEQ = TOK_DEV * SP
VIS_SHARD = TOK_DEV // KEEP_DIV
VIS_ALL = VIS_SHARD * SP
ENC_HD = D // ENC_HEADS
DEC_HD = DD // DEC_HEADS


def shard_ranks(key):
    return jax.random.permutation(key, TOK_DEV)


def draw_mask(key):
    half_shard = VIS_SHARD // 2
    key_shift, key_pick, key_perm = jax.random.split(key, 3)
    inner_shift = jax.random.randint(key_shift, (CLIPS, SP - 1), -half_shard, half_shard + 1)
    pick_at = jax.random.randint(key_pick, (CLIPS, 1), 1, SP - 2)
    shard_idx = jnp.arange(1, SP)[None, :]
    inner_shift = jnp.where(shard_idx == pick_at, half_shard, inner_shift)
    inner_shift = jnp.where(shard_idx == pick_at + 1, -half_shard, inner_shift)
    inner_shift = jnp.where(shard_idx == pick_at + 2, half_shard, inner_shift)
    edge_zero = jnp.zeros((CLIPS, 1), jnp.int32)
    shift_all = jnp.concatenate([edge_zero, inner_shift, edge_zero], axis=1)
    shard_counts = VIS_SHARD + shift_all[:, 1:] - shift_all[:, :-1]
    tok_ranks = jax.vmap(shard_ranks)(jax.random.split(key_perm, CLIPS * SP))
    tok_ranks = tok_ranks.reshape(CLIPS, SP, TOK_DEV)
    return (tok_ranks < shard_counts[:, :, None]).astype(jnp.int32).reshape(CLIPS, SEQ)


def draw_normal(key, shape, scale):
    return (scale * jax.random.normal(key, shape, jnp.float32)).astype(jnp.bfloat16)


def setup_inputs(seed: int = 0, part: int = 0) -> dict:
    key_shared, key_local = jax.random.split(jax.random.key(seed))
    part_keys = jax.random.split(jax.random.fold_in(key_local, part), 4)
    weight_keys = jax.random.split(key_shared, 13)
    return {
        'patches': draw_normal(part_keys[0], (CLIPS, SEQ, P), 1.0),
        'vis_mask': draw_mask(part_keys[1]),
        'enc_pos': draw_normal(part_keys[2], (SEQ, D), 0.5),
        'dec_pos': draw_normal(part_keys[3], (SEQ, DD), 0.5),
        'w_pe': draw_normal(weight_keys[0], (P, D), P ** -0.5),
        'b_pe': draw_normal(weight_keys[1], (D,), 0.5),
        'enc_qkv': draw_normal(weight_keys[2], (LAYERS, D, 3, ENC_HEADS, ENC_HD), 1.5 * D ** -0.5),
        'enc_proj': draw_normal(weight_keys[3], (LAYERS, ENC_HEADS, ENC_HD, D), D ** -0.5),
        'enc_up': draw_normal(weight_keys[4], (LAYERS, D, 4 * D), D ** -0.5),
        'enc_down': draw_normal(weight_keys[5], (LAYERS, 4 * D, D), (4 * D) ** -0.5),
        'w_ed': draw_normal(weight_keys[6], (D, DD), D ** -0.5),
        'mask_token': draw_normal(weight_keys[7], (DD,), 1.0),
        'dec_qkv': draw_normal(weight_keys[8], (LAYERS, DD, 3, DEC_HEADS, DEC_HD), 1.5 * DD ** -0.5),
        'dec_proj': draw_normal(weight_keys[9], (LAYERS, DEC_HEADS, DEC_HD, DD), DD ** -0.5),
        'dec_up': draw_normal(weight_keys[10], (LAYERS, DD, 4 * DD), DD ** -0.5),
        'dec_down': draw_normal(weight_keys[11], (LAYERS, 4 * DD, DD), (4 * DD) ** -0.5),
        'w_out': draw_normal(weight_keys[12], (DD, P), DD ** -0.5),
    }


def layer_norm(hidden):
    hid_f32 = hidden.astype(jnp.float32)
    centred = hid_f32 - jnp.mean(hid_f32, axis=-1, keepdims=True)
    row_var = jnp.mean(centred * centred, axis=-1, keepdims=True)
    return (centred * lax.rsqrt(row_var + 1e-6)).astype(jnp.bfloat16)


def attend(queries, key_rows, value_rows):
    q_rows, n_heads, head_dim = queries.shape
    keys_f32 = key_rows.astype(jnp.float32)
    values_f32 = value_rows.astype(jnp.float32)

    def one_block(q_block):
        scores = jnp.einsum('qhk,shk->hqs', q_block.astype(jnp.float32), keys_f32) * head_dim ** -0.5
        attn_probs = jax.nn.softmax(scores, axis=-1).astype(jnp.bfloat16)
        return jnp.einsum('hqs,shk->qhk', attn_probs.astype(jnp.float32), values_f32).astype(jnp.bfloat16)

    q_blocks = queries.reshape(SP, q_rows // SP, n_heads, head_dim)
    return lax.map(one_block, q_blocks).reshape(q_rows, n_heads, head_dim)


def block(hidden, w_qkv, w_proj, w_up, w_down):
    proj_qkv = jnp.einsum('nd,dshk->snhk', layer_norm(hidden).astype(jnp.float32), w_qkv.astype(jnp.float32)).astype(jnp.bfloat16)
    attended = attend(proj_qkv[0], proj_qkv[1], proj_qkv[2])
    att_out = jnp.einsum('nhk,hkd->nd', attended.astype(jnp.float32), w_proj.astype(jnp.float32))
    mid_state = (hidden.astype(jnp.float32) + att_out).astype(jnp.bfloat16)
    up_act = jax.nn.gelu(jnp.dot(layer_norm(mid_state), w_up, preferred_element_type=jnp.float32), approximate=False).astype(jnp.bfloat16)
    return (mid_state.astype(jnp.float32) + jnp.dot(up_act, w_down, preferred_element_type=jnp.float32)).astype(jnp.bfloat16)


def run_stack(hidden, w_qkv, w_proj, w_up, w_down):
    def body(carry, layer_w):
        return block(carry, layer_w[0], layer_w[1], layer_w[2], layer_w[3]), None

    final_state, unused = lax.scan(body, hidden, (w_qkv, w_proj, w_up, w_down))
    return final_state


def reference(patches, vis_mask, enc_pos, dec_pos, w_pe, b_pe, enc_qkv, enc_proj, enc_up, enc_down, w_ed, mask_token, dec_qkv, dec_proj, dec_up, dec_down, w_out):
    def one_clip(clip_in):
        clip_patches, visible = clip_in
        vis_idx = jnp.nonzero(visible, size=VIS_ALL)[0]
        embedded = (jnp.dot(clip_patches[vis_idx], w_pe, preferred_element_type=jnp.float32)
                    + b_pe.astype(jnp.float32) + enc_pos[vis_idx].astype(jnp.float32)).astype(jnp.bfloat16)
        encoded = run_stack(embedded, enc_qkv, enc_proj, enc_up, enc_down)
        z_vis = jnp.dot(layer_norm(encoded), w_ed, preferred_element_type=jnp.float32).astype(jnp.bfloat16)
        vis_rank = jnp.clip(jnp.cumsum(visible) - visible, 0, VIS_ALL - 1)
        dec_tok = jnp.where(visible[:, None] == 1, z_vis[vis_rank], mask_token[None, :])
        dec_in = (dec_tok.astype(jnp.float32) + dec_pos.astype(jnp.float32)).astype(jnp.bfloat16)
        decoded = run_stack(dec_in, dec_qkv, dec_proj, dec_up, dec_down)
        return jnp.dot(layer_norm(decoded), w_out, preferred_element_type=jnp.float32)

    return lax.map(one_clip, (patches, vis_mask))
```

```python
import functools

import jax
import jax.numpy as jnp
from jax import lax
from jax.experimental import pallas as pl
from jax.experimental.pallas import tpu as pltpu
from jax.sharding import PartitionSpec as P

KEEP_DIV = 8

BF = jnp.bfloat16
F32 = jnp.float32
NT = (((1,), (1,)), ((), ()))
TN = (((0,), (0,)), ((), ()))
NN = (((1,), (0,)), ((), ()))
LOG2E = 1.4426950408889634
MESH = pl.DeviceIdType.MESH
VMEM = pl.BlockSpec(memory_space=pltpu.VMEM)
ANY = pl.BlockSpec(memory_space=pl.ANY)


def mm(lhs, rhs, dims=NN):
    return lax.dot_general(lhs, rhs, dims, preferred_element_type=F32)


def norm_rows(hidden):
    wide = hidden.astype(F32)
    centred = wide - jnp.mean(wide, axis=-1, keepdims=True)
    var = jnp.mean(centred * centred, axis=-1, keepdims=True)
    return (centred * lax.rsqrt(var + 1e-6)).astype(BF)


def gelu(x):
    return 0.5 * x * (1.0 + lax.erf(x * 0.7071067811865476))


def attend_clip(tok, rows, heads, hd, k_s, vt_s, q_s, s_s, o_s):
    c2 = hd ** -0.5 * LOG2E
    group = 256 // hd
    chunk = 256
    n_chunks = tok // chunk

    def q_of(h):
        g = h // group
        qg = q_s[pl.ds(pl.multiple_of(g * 256, 256), 256), :]
        row_head = lax.broadcasted_iota(jnp.int32, (256, rows), 0) // hd
        return jnp.where(row_head == h - g * group, qg, jnp.zeros_like(qg)), pl.multiple_of(g * 256, 256)

    def scores(h, slot):
        qz, g0 = q_of(h)
        top = None
        for j in range(n_chunks):
            s = mm(k_s[j * chunk:(j + 1) * chunk, pl.ds(g0, 256)], qz)
            s_s[slot, j * chunk:(j + 1) * chunk, :] = s
            t = jnp.max(s.reshape(chunk // 8, 8, rows), axis=0)
            top = t if top is None else jnp.maximum(top, t)
        return top

    def finish(h, slot, top):
        m = jnp.max(top, axis=0, keepdims=True) * c2
        total = None
        acc = None
        v0 = pl.multiple_of(h * hd, hd)
        for j in range(n_chunks):
            e = jnp.exp2(s_s[slot, j * chunk:(j + 1) * chunk, :] * c2 - m)
            t = jnp.sum(e.reshape(chunk // 8, 8, rows), axis=0)
            total = t if total is None else total + t
            a = mm(vt_s[pl.ds(v0, hd), j * chunk:(j + 1) * chunk], e.astype(BF))
            acc = a if acc is None else acc + a
        denom = jnp.sum(total, axis=0, keepdims=True)
        o_s[pl.ds(v0, hd), :] = (acc / denom).astype(BF)

    first = scores(0, 0)

    def body(i, top0):
        h = 2 * i
        top1 = scores(h + 1, 1)
        finish(h, 0, top0)
        nxt = scores(jnp.minimum(h + 2, heads - 1), 0)
        finish(h + 1, 1, top1)
        return nxt

    lax.fori_loop(0, heads // 2, body, first)


def dec_kernel(last, n_clips, sp, a_all, u_in, wqkv, wproj, wup, wdown, wout, *rest):
    if last:
        out, k_s, vt_s, q_s, s_s, o_s = rest
    else:
        out, a_out, k_s, vt_s, q_s, s_s, o_s = rest
    rows = u_in.shape[1]
    width = u_in.shape[2]
    tok = rows * sp
    heads, hd = 16, width // 16
    me = lax.axis_index('sp')

    def clip(c, carry):
        def kv(b, cc):
            at = pl.multiple_of(b * rows, rows)
            blk = a_all[b, c]
            k_s[pl.ds(at, rows), :] = mm(blk, wqkv[width:2 * width, :], NT).astype(BF)
            vt_s[:, pl.ds(at, rows)] = mm(wqkv[2 * width:, :], blk, NT).astype(BF)
            return cc

        lax.fori_loop(0, sp, kv, 0)
        q_s[...] = mm(wqkv[:width, :], a_all[me, c], NT).astype(BF)
        attend_clip(tok, rows, heads, hd, k_s, vt_s, q_s, s_s, o_s)
        h1 = (u_in[c].astype(F32) + mm(o_s[...], wproj[...], TN)).astype(BF)
        g = gelu(mm(norm_rows(h1), wup[...])).astype(BF)
        u2 = (h1.astype(F32) + mm(g, wdown[...])).astype(BF)
        a2 = norm_rows(u2)
        if last:
            out[c] = mm(a2, wout[...])
        else:
            out[c] = u2
            a_out[c] = a2
        return carry

    lax.fori_loop(0, n_clips, clip, 0)


def dec_layer(last, sp, a_all, u_in, wqkv, wproj, wup, wdown, wout):
    n_clips, rows, width = u_in.shape
    tok = rows * sp
    if last:
        shape = jax.ShapeDtypeStruct((n_clips, rows, wout.shape[1]), F32)
        specs = VMEM
    else:
        shape = (jax.ShapeDtypeStruct(u_in.shape, BF),) * 2
        specs = (VMEM, VMEM)
    return pl.pallas_call(
        functools.partial(dec_kernel, last, n_clips, sp),
        out_shape=shape,
        in_specs=[VMEM] * 7,
        out_specs=specs,
        scratch_shapes=[
            pltpu.VMEM((tok, width), BF),
            pltpu.VMEM((width, tok), BF),
            pltpu.VMEM((width, rows), BF),
            pltpu.VMEM((2, tok, rows), F32),
            pltpu.VMEM((width, rows), BF),
        ],
        compiler_params=pltpu.CompilerParams(vmem_limit_bytes=60 << 20),
        name='dec_last' if last else 'dec_first',
    )(a_all, u_in, wqkv, wproj, wup, wdown, wout)


def gather_kernel(sp, x_ref, all_ref, send_a, recv_a, send_b, recv_b, loc):
    me = lax.axis_index('sp')
    partner = me + 1 - 2 * lax.rem(me, 2)
    barrier = pltpu.get_barrier_semaphore()
    for k in range(1, sp):
        pl.semaphore_signal(barrier, inc=1, device_id={'sp': lax.rem(me + k, sp)}, device_id_type=MESH)
    pl.semaphore_wait(barrier, sp - 1)
    own = pltpu.make_async_copy(x_ref, all_ref.at[me], loc)
    own.start()
    far = []
    near = []
    for k in range(sp // 2):
        near.append(pltpu.make_async_remote_copy(
            src_ref=x_ref if k == 0 else all_ref.at[lax.rem(me + sp - 2 * k, sp)],
            dst_ref=all_ref.at[lax.rem(me + sp - 2 * k, sp)],
            send_sem=send_b.at[k], recv_sem=recv_b.at[k], device_id={'sp': partner}, device_id_type=MESH))
        if k:
            far.append(pltpu.make_async_remote_copy(
                src_ref=x_ref, dst_ref=all_ref.at[me], send_sem=send_a.at[k], recv_sem=recv_a.at[k],
                device_id={'sp': lax.rem(me + 2 * k, sp)}, device_id_type=MESH))
            far[-1].start()
    near[0].start()
    for k in range(1, sp // 2):
        far[k - 1].wait_recv()
        near[k].start()
    for k in range(sp // 2):
        near[k].wait()
    for f in far:
        f.wait_send()
    own.wait()


def gather(sp, x):
    return pl.pallas_call(
        functools.partial(gather_kernel, sp),
        out_shape=jax.ShapeDtypeStruct((sp,) + x.shape, x.dtype),
        in_specs=[VMEM],
        out_specs=VMEM,
        scratch_shapes=[pltpu.SemaphoreType.DMA((sp // 2,))] * 4 + [pltpu.SemaphoreType.DMA],
        compiler_params=pltpu.CompilerParams(collective_id=0, has_side_effects=True),
        name='gather_rows',
    )(x)


def layer_norm(hidden):
    hid_f32 = hidden.astype(jnp.float32)
    centred = hid_f32 - jnp.mean(hid_f32, axis=-1, keepdims=True)
    row_var = jnp.mean(centred * centred, axis=-1, keepdims=True)
    return (centred * lax.rsqrt(row_var + 1e-6)).astype(jnp.bfloat16)


def attn_mlp_block(hidden, w_qkv, w_proj, w_up, w_down):
    proj_qkv = jnp.einsum('cnd,dshk->scnhk', layer_norm(hidden), w_qkv, preferred_element_type=jnp.float32).astype(jnp.bfloat16)
    kv_all = lax.all_gather(proj_qkv[1:], 'sp', axis=2, tiled=True)
    scores = jnp.einsum('cqhk,cshk->chqs', proj_qkv[0], kv_all[0], preferred_element_type=jnp.float32) * proj_qkv.shape[-1] ** -0.5
    attn_probs = jax.nn.softmax(scores, axis=-1).astype(jnp.bfloat16)
    attended = jnp.einsum('chqs,cshk->cqhk', attn_probs, kv_all[1], preferred_element_type=jnp.float32).astype(jnp.bfloat16)
    mid_state = (hidden + jnp.einsum('cqhk,hkd->cqd', attended, w_proj, preferred_element_type=jnp.float32)).astype(jnp.bfloat16)
    up_act = jax.nn.gelu(jnp.einsum('cnd,df->cnf', layer_norm(mid_state), w_up, preferred_element_type=jnp.float32), approximate=False).astype(jnp.bfloat16)
    return (mid_state + jnp.einsum('cnf,fd->cnd', up_act, w_down, preferred_element_type=jnp.float32)).astype(jnp.bfloat16)


def solution(mesh):
    group_size = mesh.shape['sp']
    to_next = [(src_dev, src_dev + 1) for src_dev in range(group_size - 1)]
    to_prev = [(src_dev + 1, src_dev) for src_dev in range(group_size - 1)]

    def local_program(patches, vis_mask, enc_pos, dec_pos, w_pe, b_pe, enc_qkv, enc_proj, enc_up, enc_down, w_ed, mask_token, dec_qkv, dec_proj, dec_up, dec_down, w_out):
        vis_shard = patches.shape[1] // KEEP_DIV
        half_rows = vis_shard // 2
        my_index = lax.axis_index('sp')
        vis_counts = lax.all_gather(jnp.sum(vis_mask, axis=1), 'sp')
        vis_before = jnp.sum(jnp.where(jnp.arange(group_size)[:, None] < my_index, vis_counts, 0), axis=0)
        local_rank = jnp.cumsum(vis_mask, axis=1) - vis_mask
        dest_row = vis_before[:, None] + local_rank - my_index * vis_shard + half_rows
        row_ids = jnp.arange(2 * vis_shard)
        select = ((dest_row[:, None, :] == row_ids[None, :, None]) & (vis_mask[:, None, :] == 1)).astype(jnp.bfloat16)
        moved_x = jnp.einsum('cqi,cip->cqp', select, patches, preferred_element_type=jnp.float32).astype(jnp.bfloat16)
        moved_pos = jnp.einsum('cqi,id->cqd', select, enc_pos, preferred_element_type=jnp.float32)
        occupied = jnp.sum(select, axis=2, dtype=jnp.float32)
        embedded = (jnp.einsum('cqp,pd->cqd', moved_x, w_pe, preferred_element_type=jnp.float32)
                    + occupied[:, :, None] * b_pe.astype(jnp.float32) + moved_pos).astype(jnp.bfloat16)
        from_prev = lax.ppermute(embedded[:, 3 * half_rows:], 'sp', to_next)
        from_next = lax.ppermute(embedded[:, :half_rows], 'sp', to_prev)
        hidden = embedded[:, half_rows:3 * half_rows] + jnp.concatenate([from_prev, from_next], axis=1)
        for layer_idx in range(enc_qkv.shape[0]):
            hidden = attn_mlp_block(hidden, enc_qkv[layer_idx], enc_proj[layer_idx], enc_up[layer_idx], enc_down[layer_idx])
        z_enc = jnp.einsum('cnd,de->cne', layer_norm(hidden), w_ed, preferred_element_type=jnp.float32).astype(jnp.bfloat16)
        z_prev = lax.ppermute(z_enc[:, half_rows:], 'sp', to_next)
        z_next = lax.ppermute(z_enc[:, :half_rows], 'sp', to_prev)
        z_rows = jnp.concatenate([z_prev, z_enc, z_next], axis=1)
        placed = jnp.einsum('cqi,cqe->cie', select, z_rows, preferred_element_type=jnp.float32)
        masked_part = (1 - vis_mask).astype(jnp.float32)[:, :, None] * mask_token.astype(jnp.float32)
        hidden = (placed + masked_part + dec_pos.astype(jnp.float32)).astype(jnp.bfloat16)
        n_layers, d_width = dec_qkv.shape[:2]
        wqkv_t = jnp.transpose(dec_qkv, (0, 2, 3, 4, 1)).reshape(n_layers, 3 * d_width, d_width)
        wproj = dec_proj.reshape(n_layers, d_width, d_width)
        acts = layer_norm(hidden)
        for layer_idx in range(n_layers):
            last = layer_idx == n_layers - 1
            a_all = gather(group_size, acts)
            res = dec_layer(last, group_size, a_all, hidden, wqkv_t[layer_idx], wproj[layer_idx], dec_up[layer_idx], dec_down[layer_idx], w_out)
            if not last:
                hidden, acts = res
        return res

    row_spec = P('dp', 'sp', None)
    pos_spec = P(('dp', 'sp'), None)
    arg_specs = (row_spec, P('dp', 'sp'), pos_spec, pos_spec) + (P(),) * 13
    return jax.shard_map(local_program, mesh=mesh, in_specs=arg_specs, out_specs=row_spec, check_vma=False)
```

```python
import functools

import jax
import jax.numpy as jnp
from jax import lax
from jax.experimental import pallas as pl
from jax.experimental.pallas import tpu as pltpu
from jax.sharding import PartitionSpec as P

KEEP_DIV = 8


BF = jnp.bfloat16
F32 = jnp.float32
NT = (((1,), (1,)), ((), ()))
TN = (((0,), (0,)), ((), ()))
NN = (((1,), (0,)), ((), ()))
LOG2E = 1.4426950408889634
MESH = pl.DeviceIdType.MESH
VMEM = pl.BlockSpec(memory_space=pltpu.VMEM)
ANY = pl.BlockSpec(memory_space=pl.ANY)


def mm(lhs, rhs, dims=NN):
    return lax.dot_general(lhs, rhs, dims, preferred_element_type=F32)


def norm_rows(hidden):
    wide = hidden.astype(F32)
    centred = wide - jnp.mean(wide, axis=-1, keepdims=True)
    var = jnp.mean(centred * centred, axis=-1, keepdims=True)
    return (centred * lax.rsqrt(var + 1e-6)).astype(BF)


def gelu(x):
    return 0.5 * x * (1.0 + lax.erf(x * 0.7071067811865476))


def attend_clip(tok, rows, heads, hd, k_s, vt_s, q_s, s_s, o_s):
    c2 = hd ** -0.5 * LOG2E
    group = 256 // hd
    chunk = 256
    n_chunks = tok // chunk

    def q_of(h):
        g = h // group
        qg = q_s[pl.ds(pl.multiple_of(g * 256, 256), 256), :]
        row_head = lax.broadcasted_iota(jnp.int32, (256, rows), 0) // hd
        return jnp.where(row_head == h - g * group, qg, jnp.zeros_like(qg)), pl.multiple_of(g * 256, 256)

    def scores(h, slot):
        qz, g0 = q_of(h)
        top = None
        for j in range(n_chunks):
            s = mm(k_s[j * chunk:(j + 1) * chunk, pl.ds(g0, 256)], qz)
            s_s[slot, j * chunk:(j + 1) * chunk, :] = s
            t = jnp.max(s.reshape(chunk // 8, 8, rows), axis=0)
            top = t if top is None else jnp.maximum(top, t)
        return top

    def finish(h, slot, top):
        m = jnp.max(top, axis=0, keepdims=True) * c2
        total = None
        acc = None
        v0 = pl.multiple_of(h * hd, hd)
        for j in range(n_chunks):
            e = jnp.exp2(s_s[slot, j * chunk:(j + 1) * chunk, :] * c2 - m)
            t = jnp.sum(e.reshape(chunk // 8, 8, rows), axis=0)
            total = t if total is None else total + t
            a = mm(vt_s[pl.ds(v0, hd), j * chunk:(j + 1) * chunk], e.astype(BF))
            acc = a if acc is None else acc + a
        denom = jnp.sum(total, axis=0, keepdims=True)
        o_s[pl.ds(v0, hd), :] = (acc / denom).astype(BF)

    first = scores(0, 0)

    def body(i, top0):
        h = 2 * i
        top1 = scores(h + 1, 1)
        finish(h, 0, top0)
        nxt = scores(jnp.minimum(h + 2, heads - 1), 0)
        finish(h + 1, 1, top1)
        return nxt

    lax.fori_loop(0, heads // 2, body, first)


def dec_kernel(last, n_clips, sp, a_all, u_in, wqkv, wproj, wup, wdown, wout, *rest):
    if last:
        out, k_s, vt_s, q_s, s_s, o_s = rest
    else:
        out, a_out, k_s, vt_s, q_s, s_s, o_s = rest
    rows = u_in.shape[1]
    width = u_in.shape[2]
    tok = rows * sp
    heads, hd = 16, width // 16
    me = lax.axis_index('sp')

    def clip(c, carry):
        def kv(b, cc):
            at = pl.multiple_of(b * rows, rows)
            blk = a_all[b, c]
            k_s[pl.ds(at, rows), :] = mm(blk, wqkv[width:2 * width, :], NT).astype(BF)
            vt_s[:, pl.ds(at, rows)] = mm(wqkv[2 * width:, :], blk, NT).astype(BF)
            return cc

        lax.fori_loop(0, sp, kv, 0)
        q_s[...] = mm(wqkv[:width, :], a_all[me, c], NT).astype(BF)
        attend_clip(tok, rows, heads, hd, k_s, vt_s, q_s, s_s, o_s)
        h1 = (u_in[c].astype(F32) + mm(o_s[...], wproj[...], TN)).astype(BF)
        g = gelu(mm(norm_rows(h1), wup[...])).astype(BF)
        u2 = (h1.astype(F32) + mm(g, wdown[...])).astype(BF)
        a2 = norm_rows(u2)
        if last:
            out[c] = mm(a2, wout[...])
        else:
            out[c] = u2
            a_out[c] = a2
        return carry

    lax.fori_loop(0, n_clips, clip, 0)


def dec_layer(last, sp, a_all, u_in, wqkv, wproj, wup, wdown, wout):
    n_clips, rows, width = u_in.shape
    tok = rows * sp
    if last:
        shape = jax.ShapeDtypeStruct((n_clips, rows, wout.shape[1]), F32)
        specs = VMEM
    else:
        shape = (jax.ShapeDtypeStruct(u_in.shape, BF),) * 2
        specs = (VMEM, VMEM)
    return pl.pallas_call(
        functools.partial(dec_kernel, last, n_clips, sp),
        out_shape=shape,
        in_specs=[VMEM] * 7,
        out_specs=specs,
        scratch_shapes=[
            pltpu.VMEM((tok, width), BF),
            pltpu.VMEM((width, tok), BF),
            pltpu.VMEM((width, rows), BF),
            pltpu.VMEM((2, tok, rows), F32),
            pltpu.VMEM((width, rows), BF),
        ],
        compiler_params=pltpu.CompilerParams(vmem_limit_bytes=60 << 20),
        name='dec_last' if last else 'dec_first',
    )(a_all, u_in, wqkv, wproj, wup, wdown, wout)


def gather_kernel(sp, x_ref, all_ref, send_a, recv_a, send_b, recv_b, loc):
    me = lax.axis_index('sp')
    partner = me + 1 - 2 * lax.rem(me, 2)
    barrier = pltpu.get_barrier_semaphore()
    for k in range(1, sp):
        pl.semaphore_signal(barrier, inc=1, device_id={'sp': lax.rem(me + k, sp)}, device_id_type=MESH)
    pl.semaphore_wait(barrier, sp - 1)
    own = pltpu.make_async_copy(x_ref, all_ref.at[me], loc)
    own.start()
    far = []
    near = []
    for k in range(sp // 2):
        near.append(pltpu.make_async_remote_copy(
            src_ref=x_ref if k == 0 else all_ref.at[lax.rem(me + sp - 2 * k, sp)],
            dst_ref=all_ref.at[lax.rem(me + sp - 2 * k, sp)],
            send_sem=send_b.at[k], recv_sem=recv_b.at[k], device_id={'sp': partner}, device_id_type=MESH))
        if k:
            far.append(pltpu.make_async_remote_copy(
                src_ref=x_ref, dst_ref=all_ref.at[me], send_sem=send_a.at[k], recv_sem=recv_a.at[k],
                device_id={'sp': lax.rem(me + 2 * k, sp)}, device_id_type=MESH))
            far[-1].start()
    near[0].start()
    for k in range(1, sp // 2):
        far[k - 1].wait_recv()
        near[k].start()
    for k in range(sp // 2):
        near[k].wait()
    for f in far:
        f.wait_send()
    own.wait()


def gather(sp, x):
    return pl.pallas_call(
        functools.partial(gather_kernel, sp),
        out_shape=jax.ShapeDtypeStruct((sp,) + x.shape, x.dtype),
        in_specs=[VMEM],
        out_specs=VMEM,
        scratch_shapes=[pltpu.SemaphoreType.DMA((sp // 2,))] * 4 + [pltpu.SemaphoreType.DMA],
        compiler_params=pltpu.CompilerParams(collective_id=0, has_side_effects=True),
        name='gather_rows',
    )(x)


def enc_kernel(sp, mask_ref, patches_h, enc_pos_h, dec_pos_h, w_pe_h, b_pe_ref, qkv_h, proj_h, up_h, down_h, w_ed_h,
               z_all, mask_all, pos_all,
               patches, enc_pos, w_pe, w_ed, wbuf, e_src, win, edge, hid, a_all, qkv_s, s_s, p_s, o_s, g_s, acc_s,
               wsem, insem, ms, mr, ws, wr, es, er, asend, arecv, zs, zr, pfs, pfr, pns, pnr, lsem):
    me = lax.axis_index('sp')
    n_clips, rows, width = patches.shape[0], patches.shape[1], hid.shape[1]
    cap = e_src.shape[1]
    share = cap // 2
    half = share // 2
    n_layers = qkv_h.shape[0]
    my_rows = hid.shape[0]
    per = sp // n_clips
    heads = 16
    hd = width // heads
    clip = me // per
    hf = lax.rem(me, 2)
    partner = me + 1 - 2 * hf
    my_half = me // per
    slot = lax.rem(me, per)

    def chunk(l, j):
        if j < 3:
            src = qkv_h.at[l, pl.ds(j * width, width), :]
        elif j == 3:
            src = proj_h.at[l]
        elif j < 8:
            src = up_h.at[l, :, pl.ds((j - 4) * width, width)]
        else:
            src = down_h.at[l, pl.ds((j - 8) * width, width), :]
        return pltpu.make_async_copy(src, wbuf.at[j], wsem.at[j])

    loads = [pltpu.make_async_copy(a, b, insem.at[i]) for i, (a, b) in enumerate(
        [(patches_h, patches), (w_pe_h, w_pe), (enc_pos_h, enc_pos), (w_ed_h, w_ed)])]
    for ld in loads:
        ld.start()
    for j in range(12):
        chunk(0, j).start()

    barrier = pltpu.get_barrier_semaphore()
    for k in range(1, sp):
        pl.semaphore_signal(barrier, inc=1, device_id={'sp': lax.rem(me + k, sp)}, device_id_type=MESH)
    pl.semaphore_wait(barrier, sp - 1)

    mask_sends = []
    for k in range(1, sp):
        mask_sends.append(pltpu.make_async_remote_copy(
            src_ref=mask_ref, dst_ref=mask_all.at[me], send_sem=ms.at[k], recv_sem=mr.at[k],
            device_id={'sp': lax.rem(me + k, sp)}, device_id_type=MESH))
        mask_sends[-1].start()
    own_mask = pltpu.make_async_copy(mask_ref, mask_all.at[me], lsem.at[0])
    own_mask.start()

    mask = mask_ref[...]
    maskf = mask.astype(F32)
    before = (lax.broadcasted_iota(jnp.int32, (rows, rows), 0) < lax.broadcasted_iota(jnp.int32, (rows, rows), 1))
    mask8 = jnp.concatenate([maskf] + [jnp.zeros_like(maskf)] * 7, axis=0).astype(BF)
    rank = mm(mask8, before.astype(BF)).astype(jnp.int32)
    b_row = b_pe_ref[...].astype(F32)
    row_id = lax.broadcasted_iota(jnp.int32, (cap, rows), 0)
    for ld in loads[:3]:
        ld.wait()
    local = []
    for c in range(n_clips):
        pick = (row_id == rank[c:c + 1, :]) & (mask[c:c + 1, :] == 1)
        pick = jnp.where(pick, 1.0, 0.0)
        used = jnp.sum(pick, axis=1, keepdims=True)
        pick = pick.astype(BF)
        x = mm(pick, patches[c]).astype(BF)
        pos = mm(pick, enc_pos[...])
        local.append((mm(x, w_pe[...]) + used * b_row + pos).astype(BF))

    for ms_ in mask_sends:
        ms_.wait_recv()
    own_mask.wait()
    total_before = [jnp.zeros((1, rows), F32) for _ in range(n_clips)]
    for s in range(sp):
        ahead = jnp.where(s < me, 1.0, 0.0)
        ms_row = mask_all[s].astype(F32)
        for c in range(n_clips):
            total_before[c] = total_before[c] + ahead * ms_row[c:c + 1, :]
    sq0 = lax.broadcasted_iota(jnp.int32, (cap, cap), 0)
    sq1 = lax.broadcasted_iota(jnp.int32, (cap, cap), 1)
    for c in range(n_clips):
        off = jnp.sum(total_before[c], axis=1, keepdims=True).astype(jnp.int32) - me * share + half
        shift = jnp.where(sq0 == sq1 + off, 1.0, 0.0).astype(BF)
        e_src[c] = mm(shift, local[c]).astype(BF)

    def to(c, x, h):
        return per * c + 2 * x + h

    for c in range(n_clips):
        for x in range(per // 2):
            dst = to(c, x, my_half)

            @pl.when(dst != me)
            def _():
                pltpu.make_async_remote_copy(
                    src_ref=e_src.at[c], dst_ref=win.at[slot], send_sem=ws.at[c, x], recv_sem=wr.at[slot],
                    device_id={'sp': dst}, device_id_type=MESH).start()

            @pl.when(dst == me)
            def _():
                pltpu.make_async_copy(e_src.at[c], win.at[slot], wr.at[slot]).start()

            for src_dev, h, r0 in ((per, 0, 0), (per - 1, 1, cap - half)):
                edst = to(c, x, h)

                @pl.when((me == src_dev) & (edst != me))
                def _():
                    pltpu.make_async_remote_copy(
                        src_ref=e_src.at[c, pl.ds(r0, half)], dst_ref=edge, send_sem=es.at[c, x], recv_sem=er,
                        device_id={'sp': edst}, device_id_type=MESH).start()

                @pl.when((me == src_dev) & (edst == me))
                def _():
                    pltpu.make_async_copy(e_src.at[c, pl.ds(r0, half)], edge, er).start()

    for b in range(per):
        pltpu.make_async_copy(e_src.at[0], win.at[b], wr.at[b]).wait()
    pltpu.make_async_copy(e_src.at[0, pl.ds(0, half)], edge, er).wait()

    pos_own = pltpu.make_async_copy(dec_pos_h, pos_all.at[me], lsem.at[1])
    pos_own.start()
    pos_far = []
    for k in range(1, sp // 2):
        pos_far.append(pltpu.make_async_remote_copy(
            src_ref=dec_pos_h, dst_ref=pos_all.at[me], send_sem=pfs.at[k], recv_sem=pfr.at[k],
            device_id={'sp': lax.rem(me + 2 * k, sp)}, device_id_type=MESH))
        pos_far[-1].start()

    zero_edge = jnp.zeros((half, width), F32)
    edge_v = edge[...].astype(F32)
    first_prev = jnp.where(hf == 1, edge_v, zero_edge)
    last_next = jnp.where(hf == 0, edge_v, zero_edge)
    for b in range(per):
        prev = first_prev if b == 0 else win[b - 1, cap - half:, :].astype(F32)
        nxt = last_next if b == per - 1 else win[b + 1, :half, :].astype(F32)
        lo = win[b, half:2 * half, :].astype(F32) + prev
        hi = win[b, 2 * half:3 * half, :].astype(F32) + nxt
        hid[b * share:b * share + half, :] = lo.astype(BF)
        hid[b * share + half:(b + 1) * share, :] = hi.astype(BF)

    scale = hd ** -0.5

    def layer(l, carry):
        def refill(j):
            @pl.when(l < n_layers - 1)
            def _():
                chunk(l + 1, j).start()

        a_all[l, 0] = norm_rows(hid[...])
        swap = pltpu.make_async_remote_copy(
            src_ref=a_all.at[l, 0], dst_ref=a_all.at[l, 1], send_sem=asend.at[l], recv_sem=arecv.at[l],
            device_id={'sp': partner}, device_id_type=MESH)
        swap.start()
        swap.wait()
        rhs = a_all[l].reshape(2 * my_rows, width)
        for j in range(3):
            chunk(l, j).wait()
            qkv_s[j] = mm(wbuf[j], rhs, NT).astype(BF)
            refill(j)
        for h in range(heads):
            s_s[h] = mm(qkv_s[0, h * hd:(h + 1) * hd, :my_rows], qkv_s[1, h * hd:(h + 1) * hd, :], TN)

        def soft(i, cc):
            s = s_s[i] * scale
            e = jnp.exp(s - jnp.max(s, axis=-1, keepdims=True))
            p_s[i] = (e / jnp.sum(e, axis=-1, keepdims=True)).astype(BF)
            return cc

        lax.fori_loop(0, heads, soft, 0, unroll=4)
        for h in range(heads):
            o_s[h * hd:(h + 1) * hd, :] = mm(qkv_s[2, h * hd:(h + 1) * hd, :], p_s[h], NT).astype(BF)
        chunk(l, 3).wait()
        h1 = (hid[...].astype(F32) + mm(o_s[...], wbuf[3], TN)).astype(BF)
        hid[...] = h1
        refill(3)
        a2 = norm_rows(h1)
        for j in range(4):
            chunk(l, 4 + j).wait()
            g_s[:, j * width:(j + 1) * width] = gelu(mm(a2, wbuf[4 + j])).astype(BF)
            refill(4 + j)
        for j in range(4):
            chunk(l, 8 + j).wait()
            part = mm(g_s[:, j * width:(j + 1) * width], wbuf[8 + j])
            acc_s[...] = part if j == 0 else acc_s[...] + part
            refill(8 + j)
        hid[...] = (hid[...].astype(F32) + acc_s[...]).astype(BF)
        return carry

    lax.fori_loop(0, n_layers, layer, 0)

    for p in pos_far:
        p.wait()
    pos_own.wait()
    pos_near = []
    for k in range(sp // 2):
        piece = lax.rem(me + 2 * k, sp)
        pos_near.append(pltpu.make_async_remote_copy(
            src_ref=pos_all.at[piece], dst_ref=pos_all.at[piece], send_sem=pns.at[k], recv_sem=pnr.at[k],
            device_id={'sp': partner}, device_id_type=MESH))
        pos_near[-1].start()

    loads[3].wait()
    mine = z_all.at[clip, pl.ds(pl.multiple_of(hf * my_rows, my_rows), my_rows), :]
    z_all[clip, pl.ds(pl.multiple_of(hf * my_rows, my_rows), my_rows), :] = mm(norm_rows(hid[...]), w_ed[...]).astype(BF)
    z_sends = []
    across = lax.rem(me + per, sp)
    for i, dst in enumerate((across, across + 1 - 2 * hf, partner)):
        z_sends.append(pltpu.make_async_remote_copy(
            src_ref=mine, dst_ref=mine, send_sem=zs.at[i], recv_sem=zr.at[i],
            device_id={'sp': dst}, device_id_type=MESH))
        z_sends[-1].start()
    for k in mask_sends:
        k.wait_send()
    for c in range(n_clips):
        for x in range(per // 2):
            @pl.when(to(c, x, my_half) != me)
            def _():
                pltpu.make_async_remote_copy(
                    src_ref=e_src.at[c], dst_ref=win.at[slot], send_sem=ws.at[c, x], recv_sem=wr.at[slot],
                    device_id={'sp': to(c, x, my_half)}, device_id_type=MESH).wait_send()

            for src_dev, h, r0 in ((per, 0, 0), (per - 1, 1, cap - half)):
                @pl.when((me == src_dev) & (to(c, x, h) != me))
                def _():
                    pltpu.make_async_remote_copy(
                        src_ref=e_src.at[c, pl.ds(r0, half)], dst_ref=edge, send_sem=es.at[c, x], recv_sem=er,
                        device_id={'sp': to(c, x, h)}, device_id_type=MESH).wait_send()
    for p in pos_near:
        p.wait()
    for s in z_sends:
        s.wait()


def encode(sp, vis_mask, patches, enc_pos, dec_pos, w_pe, b_pe, qkv_t, proj, up, down, w_ed):
    n_clips, rows, p_width = patches.shape
    width = w_pe.shape[1]
    d_width = w_ed.shape[1]
    cap = 2 * rows // KEEP_DIV
    my_rows = rows * sp // KEEP_DIV // 2
    dma = pltpu.SemaphoreType.DMA
    per = sp // n_clips
    return pl.pallas_call(
        functools.partial(enc_kernel, sp),
        out_shape=(jax.ShapeDtypeStruct((n_clips, 2 * my_rows, d_width), BF),
                   jax.ShapeDtypeStruct((sp, n_clips, rows), jnp.int32),
                   jax.ShapeDtypeStruct((sp, rows, d_width), BF)),
        in_specs=[VMEM, ANY, ANY, ANY, ANY, VMEM, ANY, ANY, ANY, ANY, ANY],
        out_specs=(VMEM, VMEM, ANY),
        scratch_shapes=[
            pltpu.VMEM(patches.shape, BF), pltpu.VMEM(enc_pos.shape, BF), pltpu.VMEM(w_pe.shape, BF), pltpu.VMEM(w_ed.shape, BF),
            pltpu.VMEM((12, width, width), BF),
            pltpu.VMEM((n_clips, cap, width), BF), pltpu.VMEM((per, cap, width), BF), pltpu.VMEM((cap // 4, width), BF),
            pltpu.VMEM((my_rows, width), BF), pltpu.VMEM((qkv_t.shape[0], 2, my_rows, width), BF),
            pltpu.VMEM((3, width, 2 * my_rows), BF),
            pltpu.VMEM((16, my_rows, 2 * my_rows), F32), pltpu.VMEM((16, my_rows, 2 * my_rows), BF),
            pltpu.VMEM((width, my_rows), BF), pltpu.VMEM((my_rows, 4 * width), BF), pltpu.VMEM((my_rows, width), F32),
            dma((12,)), dma((4,)), dma((sp,)), dma((sp,)), dma((n_clips, per // 2)), dma((per,)), dma((n_clips, per // 2)), dma,
            dma((2,)), dma((2,)), dma((3,)), dma((3,)), dma((sp // 2,)), dma((sp // 2,)), dma((sp // 2,)), dma((sp // 2,)), dma((2,)),
        ],
        compiler_params=pltpu.CompilerParams(collective_id=1, has_side_effects=True, vmem_limit_bytes=62 << 20),
        name='encode',
    )(vis_mask, patches, enc_pos, dec_pos, w_pe, b_pe.reshape(1, width), qkv_t, proj, up, down, w_ed)


def place_kernel(sp, z_ref, mask_all, pos_all, tok_ref, u_out, a_out, rank_s):
    me = lax.axis_index('sp')
    n_clips, n_vis, width = z_ref.shape
    rows = mask_all.shape[2]
    before = (lax.broadcasted_iota(jnp.int32, (rows, rows), 0) < lax.broadcasted_iota(jnp.int32, (rows, rows), 1)).astype(BF)
    pad = 16
    row_id = lax.broadcasted_iota(jnp.int32, (n_vis + pad, rows), 0)
    for c in range(n_clips):
        m = mask_all[:, c, :]
        local = mm(m.astype(F32).astype(BF), before)
        base = jnp.zeros((1, 1), F32)
        for s in range(sp):
            vis = m[s:s + 1, :]
            rank = jnp.where(vis == 1, (local[s:s + 1, :] + base).astype(jnp.int32), n_vis)
            base = base + jnp.sum(vis.astype(F32), axis=1, keepdims=True)
            rank_s[c, s:s + 1, :] = rank
        z_aug = jnp.concatenate([z_ref[c], tok_ref[...], jnp.zeros((pad - 1, width), BF)], axis=0)

        def block(b, cc):
            pick = jnp.where(row_id == rank_s[c, pl.ds(b, 1), :], 1.0, 0.0).astype(BF)
            u = (mm(pick, z_aug, TN) + pos_all[b].astype(F32)).astype(BF)
            a_out[b, c] = norm_rows(u)

            @pl.when(b == me)
            def _():
                u_out[c] = u
            return cc

        lax.fori_loop(0, sp, block, 0)


def place(sp, z_all, mask_all, pos_all, mask_token):
    n_clips, n_vis, width = z_all.shape
    rows = mask_all.shape[2]
    return pl.pallas_call(
        functools.partial(place_kernel, sp),
        out_shape=(jax.ShapeDtypeStruct((n_clips, rows, width), BF), jax.ShapeDtypeStruct((sp, n_clips, rows, width), BF)),
        in_specs=[VMEM] * 4,
        out_specs=(VMEM, VMEM),
        scratch_shapes=[pltpu.VMEM((n_clips, sp, rows), jnp.int32)],
        name='place',
    )(z_all, mask_all, pos_all, mask_token.reshape(1, width))


def solution(mesh):
    sp = mesh.shape['sp']

    def local_program(patches, vis_mask, enc_pos, dec_pos, w_pe, b_pe, enc_qkv, enc_proj, enc_up, enc_down, w_ed, mask_token, dec_qkv, dec_proj, dec_up, dec_down, w_out):
        n_layers, width = enc_qkv.shape[:2]
        d_width = dec_qkv.shape[1]
        enc_qkv_t = jnp.transpose(enc_qkv, (0, 2, 3, 4, 1)).reshape(n_layers, 3 * width, width)
        dec_qkv_t = jnp.transpose(dec_qkv, (0, 2, 3, 4, 1)).reshape(n_layers, 3 * d_width, d_width)
        z_all, mask_all, pos_all = encode(sp, vis_mask, patches, enc_pos, dec_pos, w_pe, b_pe, enc_qkv_t,
                                          enc_proj.reshape(n_layers, width, width), enc_up, enc_down, w_ed)
        hidden, a_all = place(sp, z_all, mask_all, pos_all, mask_token)
        wproj = dec_proj.reshape(n_layers, d_width, d_width)
        for layer_idx in range(n_layers):
            last = layer_idx == n_layers - 1
            if layer_idx:
                a_all = gather(sp, acts)
            res = dec_layer(last, sp, a_all, hidden, dec_qkv_t[layer_idx], wproj[layer_idx], dec_up[layer_idx], dec_down[layer_idx], w_out)
            if not last:
                hidden, acts = res
        return res

    row_spec = P('dp', 'sp', None)
    pos_spec = P(('dp', 'sp'), None)
    arg_specs = (row_spec, P('dp', 'sp'), pos_spec, pos_spec) + (P(),) * 13
    return jax.shard_map(local_program, mesh=mesh, in_specs=arg_specs, out_specs=row_spec, check_vma=False)
```

```python
import functools

import jax
import jax.numpy as jnp
from jax import lax
from jax.experimental import pallas as pl
from jax.experimental.pallas import tpu as pltpu
from jax.sharding import PartitionSpec as P

KEEP_DIV = 8


BF = jnp.bfloat16
F32 = jnp.float32
NT = (((1,), (1,)), ((), ()))
TN = (((0,), (0,)), ((), ()))
NN = (((1,), (0,)), ((), ()))
LOG2E = 1.4426950408889634
MESH = pl.DeviceIdType.MESH
VMEM = pl.BlockSpec(memory_space=pltpu.VMEM)
ANY = pl.BlockSpec(memory_space=pl.ANY)


def mm(lhs, rhs, dims=NN):
    return lax.dot_general(lhs, rhs, dims, preferred_element_type=F32)


def norm_rows(hidden):
    wide = hidden.astype(F32)
    centred = wide - jnp.mean(wide, axis=-1, keepdims=True)
    var = jnp.mean(centred * centred, axis=-1, keepdims=True)
    return (centred * lax.rsqrt(var + 1e-6)).astype(BF)


def gelu(x):
    return 0.5 * x * (1.0 + lax.erf(x * 0.7071067811865476))


def attend_clip(tok, rows, heads, hd, k_s, vt_s, q_s, s_s, o_s):
    c2 = hd ** -0.5 * LOG2E
    group = 256 // hd
    chunk = 256
    n_chunks = tok // chunk

    def q_of(h):
        g = h // group
        qg = q_s[pl.ds(pl.multiple_of(g * 256, 256), 256), :]
        row_head = lax.broadcasted_iota(jnp.int32, (256, rows), 0) // hd
        return jnp.where(row_head == h - g * group, qg, jnp.zeros_like(qg)), pl.multiple_of(g * 256, 256)

    def scores(h, slot):
        qz, g0 = q_of(h)
        top = None
        for j in range(n_chunks):
            s = mm(k_s[j * chunk:(j + 1) * chunk, pl.ds(g0, 256)], qz)
            s_s[slot, j * chunk:(j + 1) * chunk, :] = s
            t = jnp.max(s.reshape(chunk // 8, 8, rows), axis=0)
            top = t if top is None else jnp.maximum(top, t)
        return top

    def finish(h, slot, top):
        m = jnp.max(top, axis=0, keepdims=True) * c2
        total = None
        acc = None
        v0 = pl.multiple_of(h * hd, hd)
        for j in range(n_chunks):
            e = jnp.exp2(s_s[slot, j * chunk:(j + 1) * chunk, :] * c2 - m)
            t = jnp.sum(e.reshape(chunk // 8, 8, rows), axis=0)
            total = t if total is None else total + t
            a = mm(vt_s[pl.ds(v0, hd), j * chunk:(j + 1) * chunk], e.astype(BF))
            acc = a if acc is None else acc + a
        denom = jnp.sum(total, axis=0, keepdims=True)
        o_s[pl.ds(v0, hd), :] = (acc / denom).astype(BF)

    first = scores(0, 0)

    def body(i, top0):
        h = 2 * i
        top1 = scores(h + 1, 1)
        finish(h, 0, top0)
        nxt = scores(jnp.minimum(h + 2, heads - 1), 0)
        finish(h + 1, 1, top1)
        return nxt

    lax.fori_loop(0, heads // 2, body, first)


def enc_kernel(sp, mask_ref, patches_h, enc_pos_h, dec_pos_h, w_pe_h, b_pe_ref, qkv_h, proj_h, up_h, down_h, w_ed_h,
               z_all, mask_all, pos_all,
               patches, enc_pos, w_pe, w_ed, wbuf, e_src, win, edge, hid, a_all, qkv_s, s_s, p_s, o_s, g_s, acc_s,
               wsem, insem, ms, mr, ws, wr, es, er, asend, arecv, zs, zr, pfs, pfr, pns, pnr, lsem):
    me = lax.axis_index('sp')
    n_clips, rows, width = patches.shape[0], patches.shape[1], hid.shape[1]
    cap = e_src.shape[1]
    share = cap // 2
    half = share // 2
    n_layers = qkv_h.shape[0]
    my_rows = hid.shape[0]
    per = sp // n_clips
    heads = 16
    hd = width // heads
    clip = me // per
    hf = lax.rem(me, 2)
    partner = me + 1 - 2 * hf
    my_half = me // per
    slot = lax.rem(me, per)

    def chunk(l, j):
        if j < 3:
            src = qkv_h.at[l, pl.ds(j * width, width), :]
        elif j == 3:
            src = proj_h.at[l]
        elif j < 8:
            src = up_h.at[l, :, pl.ds((j - 4) * width, width)]
        else:
            src = down_h.at[l, pl.ds((j - 8) * width, width), :]
        return pltpu.make_async_copy(src, wbuf.at[j], wsem.at[j])

    loads = [pltpu.make_async_copy(a, b, insem.at[i]) for i, (a, b) in enumerate(
        [(patches_h, patches), (w_pe_h, w_pe), (enc_pos_h, enc_pos), (w_ed_h, w_ed)])]
    for ld in loads:
        ld.start()
    for j in range(12):
        chunk(0, j).start()

    barrier = pltpu.get_barrier_semaphore()
    for k in range(1, sp):
        pl.semaphore_signal(barrier, inc=1, device_id={'sp': lax.rem(me + k, sp)}, device_id_type=MESH)
    pl.semaphore_wait(barrier, sp - 1)

    mask_sends = []
    for k in range(1, sp):
        mask_sends.append(pltpu.make_async_remote_copy(
            src_ref=mask_ref, dst_ref=mask_all.at[me], send_sem=ms.at[k], recv_sem=mr.at[k],
            device_id={'sp': lax.rem(me + k, sp)}, device_id_type=MESH))
        mask_sends[-1].start()
    own_mask = pltpu.make_async_copy(mask_ref, mask_all.at[me], lsem.at[0])
    own_mask.start()

    mask = mask_ref[...]
    maskf = mask.astype(F32)
    before = (lax.broadcasted_iota(jnp.int32, (rows, rows), 0) < lax.broadcasted_iota(jnp.int32, (rows, rows), 1))
    mask8 = jnp.concatenate([maskf] + [jnp.zeros_like(maskf)] * 7, axis=0).astype(BF)
    rank = mm(mask8, before.astype(BF)).astype(jnp.int32)
    b_row = b_pe_ref[...].reshape(1, width).astype(F32)
    row_id = lax.broadcasted_iota(jnp.int32, (cap, rows), 0)
    for ld in loads[:3]:
        ld.wait()
    local = []
    for c in range(n_clips):
        pick = (row_id == rank[c:c + 1, :]) & (mask[c:c + 1, :] == 1)
        pick = jnp.where(pick, 1.0, 0.0)
        used = jnp.sum(pick, axis=1, keepdims=True)
        pick = pick.astype(BF)
        x = mm(pick, patches[c]).astype(BF)
        pos = mm(pick, enc_pos[...])
        local.append((mm(x, w_pe[...]) + used * b_row + pos).astype(BF))

    for ms_ in mask_sends:
        ms_.wait_recv()
    own_mask.wait()
    total_before = [jnp.zeros((1, rows), F32) for _ in range(n_clips)]
    for s in range(sp):
        ahead = jnp.where(s < me, 1.0, 0.0)
        ms_row = mask_all[s].astype(F32)
        for c in range(n_clips):
            total_before[c] = total_before[c] + ahead * ms_row[c:c + 1, :]
    sq0 = lax.broadcasted_iota(jnp.int32, (cap, cap), 0)
    sq1 = lax.broadcasted_iota(jnp.int32, (cap, cap), 1)
    for c in range(n_clips):
        off = jnp.sum(total_before[c], axis=1, keepdims=True).astype(jnp.int32) - me * share + half
        shift = jnp.where(sq0 == sq1 + off, 1.0, 0.0).astype(BF)
        e_src[c] = mm(shift, local[c]).astype(BF)

    def to(c, x, h):
        return per * c + 2 * x + h

    for c in range(n_clips):
        for x in range(per // 2):
            dst = to(c, x, my_half)

            @pl.when(dst != me)
            def _():
                pltpu.make_async_remote_copy(
                    src_ref=e_src.at[c], dst_ref=win.at[slot], send_sem=ws.at[c, x], recv_sem=wr.at[slot],
                    device_id={'sp': dst}, device_id_type=MESH).start()

            @pl.when(dst == me)
            def _():
                pltpu.make_async_copy(e_src.at[c], win.at[slot], wr.at[slot]).start()

            for src_dev, h, r0 in ((per, 0, 0), (per - 1, 1, cap - half)):
                edst = to(c, x, h)

                @pl.when((me == src_dev) & (edst != me))
                def _():
                    pltpu.make_async_remote_copy(
                        src_ref=e_src.at[c, pl.ds(r0, half)], dst_ref=edge, send_sem=es.at[c, x], recv_sem=er,
                        device_id={'sp': edst}, device_id_type=MESH).start()

                @pl.when((me == src_dev) & (edst == me))
                def _():
                    pltpu.make_async_copy(e_src.at[c, pl.ds(r0, half)], edge, er).start()

    for b in range(per):
        pltpu.make_async_copy(e_src.at[0], win.at[b], wr.at[b]).wait()
    pltpu.make_async_copy(e_src.at[0, pl.ds(0, half)], edge, er).wait()

    pos_own = pltpu.make_async_copy(dec_pos_h, pos_all.at[me], lsem.at[1])
    pos_own.start()
    pos_far = []
    for k in range(1, sp // 2):
        pos_far.append(pltpu.make_async_remote_copy(
            src_ref=dec_pos_h, dst_ref=pos_all.at[me], send_sem=pfs.at[k], recv_sem=pfr.at[k],
            device_id={'sp': lax.rem(me + 2 * k, sp)}, device_id_type=MESH))
        pos_far[-1].start()

    zero_edge = jnp.zeros((half, width), F32)
    edge_v = edge[...].astype(F32)
    first_prev = jnp.where(hf == 1, edge_v, zero_edge)
    last_next = jnp.where(hf == 0, edge_v, zero_edge)
    for b in range(per):
        prev = first_prev if b == 0 else win[b - 1, cap - half:, :].astype(F32)
        nxt = last_next if b == per - 1 else win[b + 1, :half, :].astype(F32)
        lo = win[b, half:2 * half, :].astype(F32) + prev
        hi = win[b, 2 * half:3 * half, :].astype(F32) + nxt
        hid[b * share:b * share + half, :] = lo.astype(BF)
        hid[b * share + half:(b + 1) * share, :] = hi.astype(BF)

    scale = hd ** -0.5

    def layer(l, carry):
        def refill(j):
            @pl.when(l < n_layers - 1)
            def _():
                chunk(l + 1, j).start()

        a_all[l, 0] = norm_rows(hid[...])
        swap = pltpu.make_async_remote_copy(
            src_ref=a_all.at[l, 0], dst_ref=a_all.at[l, 1], send_sem=asend.at[l], recv_sem=arecv.at[l],
            device_id={'sp': partner}, device_id_type=MESH)
        swap.start()
        swap.wait()
        rhs = a_all[l].reshape(2 * my_rows, width)
        for j in range(3):
            chunk(l, j).wait()
            qkv_s[j] = mm(wbuf[j], rhs, NT).astype(BF)
            refill(j)
        for h in range(heads):
            s_s[h] = mm(qkv_s[0, h * hd:(h + 1) * hd, :my_rows], qkv_s[1, h * hd:(h + 1) * hd, :], TN)

        def soft(i, cc):
            s = s_s[i] * scale
            e = jnp.exp(s - jnp.max(s, axis=-1, keepdims=True))
            p_s[i] = (e / jnp.sum(e, axis=-1, keepdims=True)).astype(BF)
            return cc

        lax.fori_loop(0, heads, soft, 0, unroll=4)
        for h in range(heads):
            o_s[h * hd:(h + 1) * hd, :] = mm(qkv_s[2, h * hd:(h + 1) * hd, :], p_s[h], NT).astype(BF)
        chunk(l, 3).wait()
        h1 = (hid[...].astype(F32) + mm(o_s[...], wbuf[3], TN)).astype(BF)
        hid[...] = h1
        refill(3)
        a2 = norm_rows(h1)
        for j in range(4):
            chunk(l, 4 + j).wait()
            g_s[:, j * width:(j + 1) * width] = gelu(mm(a2, wbuf[4 + j])).astype(BF)
            refill(4 + j)
        for j in range(4):
            chunk(l, 8 + j).wait()
            part = mm(g_s[:, j * width:(j + 1) * width], wbuf[8 + j])
            acc_s[...] = part if j == 0 else acc_s[...] + part
            refill(8 + j)
        hid[...] = (hid[...].astype(F32) + acc_s[...]).astype(BF)
        return carry

    lax.fori_loop(0, n_layers, layer, 0)

    for p in pos_far:
        p.wait()
    pos_own.wait()
    pos_near = []
    for k in range(sp // 2):
        piece = lax.rem(me + 2 * k, sp)
        pos_near.append(pltpu.make_async_remote_copy(
            src_ref=pos_all.at[piece], dst_ref=pos_all.at[piece], send_sem=pns.at[k], recv_sem=pnr.at[k],
            device_id={'sp': partner}, device_id_type=MESH))
        pos_near[-1].start()

    loads[3].wait()
    mine = z_all.at[clip, pl.ds(pl.multiple_of(hf * my_rows, my_rows), my_rows), :]
    z_all[clip, pl.ds(pl.multiple_of(hf * my_rows, my_rows), my_rows), :] = mm(norm_rows(hid[...]), w_ed[...]).astype(BF)
    z_sends = []
    across = lax.rem(me + per, sp)
    for i, dst in enumerate((across, across + 1 - 2 * hf, partner)):
        z_sends.append(pltpu.make_async_remote_copy(
            src_ref=mine, dst_ref=mine, send_sem=zs.at[i], recv_sem=zr.at[i],
            device_id={'sp': dst}, device_id_type=MESH))
        z_sends[-1].start()
    for k in mask_sends:
        k.wait_send()
    for c in range(n_clips):
        for x in range(per // 2):
            @pl.when(to(c, x, my_half) != me)
            def _():
                pltpu.make_async_remote_copy(
                    src_ref=e_src.at[c], dst_ref=win.at[slot], send_sem=ws.at[c, x], recv_sem=wr.at[slot],
                    device_id={'sp': to(c, x, my_half)}, device_id_type=MESH).wait_send()

            for src_dev, h, r0 in ((per, 0, 0), (per - 1, 1, cap - half)):
                @pl.when((me == src_dev) & (to(c, x, h) != me))
                def _():
                    pltpu.make_async_remote_copy(
                        src_ref=e_src.at[c, pl.ds(r0, half)], dst_ref=edge, send_sem=es.at[c, x], recv_sem=er,
                        device_id={'sp': to(c, x, h)}, device_id_type=MESH).wait_send()
    for p in pos_near:
        p.wait()
    for s in z_sends:
        s.wait()


def encode(sp, vis_mask, patches, enc_pos, dec_pos, w_pe, b_pe, qkv_t, proj, up, down, w_ed):
    n_clips, rows, p_width = patches.shape
    width = w_pe.shape[1]
    d_width = w_ed.shape[1]
    cap = 2 * rows // KEEP_DIV
    my_rows = rows * sp // KEEP_DIV // 2
    dma = pltpu.SemaphoreType.DMA
    per = sp // n_clips
    return pl.pallas_call(
        functools.partial(enc_kernel, sp),
        out_shape=(jax.ShapeDtypeStruct((n_clips, 2 * my_rows, d_width), BF),
                   jax.ShapeDtypeStruct((sp, n_clips, rows), jnp.int32),
                   jax.ShapeDtypeStruct((sp, rows, d_width), BF)),
        in_specs=[VMEM, ANY, ANY, ANY, ANY, VMEM, ANY, ANY, ANY, ANY, ANY],
        out_specs=(VMEM, VMEM, ANY),
        scratch_shapes=[
            pltpu.VMEM(patches.shape, BF), pltpu.VMEM(enc_pos.shape, BF), pltpu.VMEM(w_pe.shape, BF), pltpu.VMEM(w_ed.shape, BF),
            pltpu.VMEM((12, width, width), BF),
            pltpu.VMEM((n_clips, cap, width), BF), pltpu.VMEM((per, cap, width), BF), pltpu.VMEM((cap // 4, width), BF),
            pltpu.VMEM((my_rows, width), BF), pltpu.VMEM((qkv_t.shape[0], 2, my_rows, width), BF),
            pltpu.VMEM((3, width, 2 * my_rows), BF),
            pltpu.VMEM((16, my_rows, 2 * my_rows), F32), pltpu.VMEM((16, my_rows, 2 * my_rows), BF),
            pltpu.VMEM((width, my_rows), BF), pltpu.VMEM((my_rows, 4 * width), BF), pltpu.VMEM((my_rows, width), F32),
            dma((12,)), dma((4,)), dma((sp,)), dma((sp,)), dma((n_clips, per // 2)), dma((per,)), dma((n_clips, per // 2)), dma,
            dma((2,)), dma((2,)), dma((3,)), dma((3,)), dma((sp // 2,)), dma((sp // 2,)), dma((sp // 2,)), dma((sp // 2,)), dma((2,)),
        ],
        compiler_params=pltpu.CompilerParams(collective_id=1, has_side_effects=True, vmem_limit_bytes=62 << 20),
        name='encode',
    )(vis_mask, patches, enc_pos, dec_pos, w_pe, b_pe, qkv_t, proj, up, down, w_ed)


def decode_kernel(sp, z_ref, mask_all, pos_h, tok_ref, wqkv_h, wproj_h, wup_h, wdown_h, a_out,
                  pos, wqkv, wproj, wup, wdown, rank_s, u_s, a_own, a_all, k_s, vt_s, q_s, s_s, o_s,
                  insem, fs, fr, ns, nr):
    me = lax.axis_index('sp')
    partner = me + 1 - 2 * lax.rem(me, 2)
    n_clips, n_vis, width = z_ref.shape
    rows = mask_all.shape[2]
    tok = rows * sp
    heads, hd = 16, width // 16
    n_far = sp // 2

    loads = [pltpu.make_async_copy(a, b, insem.at[i]) for i, (a, b) in enumerate(
        [(pos_h, pos), (wqkv_h, wqkv), (wproj_h, wproj), (wup_h, wup), (wdown_h, wdown)])]
    for ld in loads:
        ld.start()
    barrier = pltpu.get_barrier_semaphore()
    for k in range(1, sp):
        pl.semaphore_signal(barrier, inc=1, device_id={'sp': lax.rem(me + k, sp)}, device_id_type=MESH)
    pl.semaphore_wait(barrier, sp - 1)

    before = (lax.broadcasted_iota(jnp.int32, (rows, rows), 0) < lax.broadcasted_iota(jnp.int32, (rows, rows), 1)).astype(BF)
    pad = 16
    row_id = lax.broadcasted_iota(jnp.int32, (n_vis + pad, rows), 0)
    for c in range(n_clips):
        m = mask_all[:, c, :]
        local = mm(m.astype(F32).astype(BF), before)
        base = jnp.zeros((1, 1), F32)
        for s in range(sp):
            vis = m[s:s + 1, :]
            rank_s[c, s:s + 1, :] = jnp.where(vis == 1, (local[s:s + 1, :] + base).astype(jnp.int32), n_vis)
            base = base + jnp.sum(vis.astype(F32), axis=1, keepdims=True)
    for ld in loads:
        ld.wait()

    def far(c, k):
        return pltpu.make_async_remote_copy(
            src_ref=a_own.at[c], dst_ref=a_all.at[c, me], send_sem=fs.at[c, k], recv_sem=fr.at[c, k],
            device_id={'sp': lax.rem(me + 2 * k, sp)}, device_id_type=MESH)

    def near(c, k):
        piece = lax.rem(me + 2 * k, sp)
        return pltpu.make_async_remote_copy(
            src_ref=a_all.at[c, piece] if k else a_own.at[c], dst_ref=a_all.at[c, piece],
            send_sem=ns.at[c, k], recv_sem=nr.at[c, k], device_id={'sp': partner}, device_id_type=MESH)

    def relay(c):
        for k in range(1, n_far):
            far(c, k).wait_recv()
        for k in range(n_far):
            near(c, k).start()

    def keys_values(l, b, blk):
        at = pl.multiple_of(b * rows, rows)
        k_s[pl.ds(at, rows), :] = mm(blk, wqkv[l, width:2 * width, :], NT).astype(BF)
        vt_s[:, pl.ds(at, rows)] = mm(wqkv[l, 2 * width:, :], blk, NT).astype(BF)

    def attend(l, c):
        q_s[...] = mm(wqkv[l, :width, :], a_own[c], NT).astype(BF)
        attend_clip(tok, rows, heads, hd, k_s, vt_s, q_s, s_s, o_s)

    def feed(l, c):
        h1 = (u_s[c].astype(F32) + mm(o_s[...], wproj[l], TN)).astype(BF)
        g = gelu(mm(norm_rows(h1), wup[l])).astype(BF)
        return (h1.astype(F32) + mm(g, wdown[l])).astype(BF)

    def first(c, carry):
        z_aug = jnp.concatenate([z_ref[c], tok_ref[...].reshape(1, width), jnp.zeros((pad - 1, width), BF)], axis=0)

        def block(b, cc):
            pick = jnp.where(row_id == rank_s[c, pl.ds(b, 1), :], 1.0, 0.0).astype(BF)
            u = (mm(pick, z_aug, TN) + pos[b].astype(F32)).astype(BF)
            a = norm_rows(u)
            keys_values(0, b, a)

            @pl.when(b == me)
            def _():
                u_s[c] = u
                a_own[c] = a
            return cc

        lax.fori_loop(0, sp, block, 0)
        attend(0, c)

        @pl.when(c == 1)
        def _():
            relay(0)

        u1 = feed(0, c)
        u_s[c] = u1
        a_own[c] = norm_rows(u1)
        for k in range(1, n_far):
            far(c, k).start()
        return carry

    lax.fori_loop(0, n_clips, first, 0)

    def second(c, carry):
        keys_values(1, me, a_own[c])

        def same(k, cc):
            b = lax.rem(me + 2 * k, sp)
            keys_values(1, b, a_all[c, b])
            return cc

        def other(k, cc):
            b = lax.rem(partner + 2 * k, sp)
            keys_values(1, b, a_all[c, b])
            return cc

        lax.fori_loop(1, n_far, same, 0)
        for k in range(n_far):
            near(c, k).wait_recv()
        lax.fori_loop(0, n_far, other, 0)
        attend(1, c)

        @pl.when(c == 0)
        def _():
            relay(1)

        a_out[c] = norm_rows(feed(1, c))
        return carry

    lax.fori_loop(0, n_clips, second, 0)
    for c in range(n_clips):
        for k in range(n_far):
            near(c, k).wait_send()
            if k:
                far(c, k).wait_send()


def decode(sp, z_all, mask_all, pos_all, mask_token, wqkv, wproj, wup, wdown):
    n_clips, n_vis, width = z_all.shape
    rows = mask_all.shape[2]
    tok = rows * sp
    dma = pltpu.SemaphoreType.DMA
    return pl.pallas_call(
        functools.partial(decode_kernel, sp),
        out_shape=jax.ShapeDtypeStruct((n_clips, rows, width), BF),
        in_specs=[VMEM, VMEM, ANY, VMEM, ANY, ANY, ANY, ANY],
        out_specs=VMEM,
        scratch_shapes=[
            pltpu.VMEM(pos_all.shape, BF), pltpu.VMEM(wqkv.shape, BF), pltpu.VMEM(wproj.shape, BF),
            pltpu.VMEM(wup.shape, BF), pltpu.VMEM(wdown.shape, BF),
            pltpu.VMEM((n_clips, sp, rows), jnp.int32), pltpu.VMEM((n_clips, rows, width), BF), pltpu.VMEM((n_clips, rows, width), BF),
            pltpu.VMEM((n_clips, sp, rows, width), BF),
            pltpu.VMEM((tok, width), BF), pltpu.VMEM((width, tok), BF), pltpu.VMEM((width, rows), BF),
            pltpu.VMEM((2, tok, rows), F32), pltpu.VMEM((width, rows), BF),
            dma((5,)), dma((n_clips, sp // 2)), dma((n_clips, sp // 2)), dma((n_clips, sp // 2)), dma((n_clips, sp // 2)),
        ],
        compiler_params=pltpu.CompilerParams(collective_id=2, has_side_effects=True, vmem_limit_bytes=52 << 20),
        name='decode',
    )(z_all, mask_all, pos_all, mask_token, wqkv, wproj, wup, wdown)


def solution(mesh):
    sp = mesh.shape['sp']

    def local_program(patches, vis_mask, enc_pos, dec_pos, w_pe, b_pe, enc_qkv, enc_proj, enc_up, enc_down, w_ed, mask_token, dec_qkv, dec_proj, dec_up, dec_down, w_out):
        n_layers, width = enc_qkv.shape[:2]
        d_width = dec_qkv.shape[1]
        enc_qkv_t = jnp.transpose(enc_qkv, (0, 2, 3, 4, 1)).reshape(n_layers, 3 * width, width)
        dec_qkv_t = jnp.transpose(dec_qkv, (0, 2, 3, 4, 1)).reshape(n_layers, 3 * d_width, d_width)
        z_all, mask_all, pos_all = encode(sp, vis_mask, patches, enc_pos, dec_pos, w_pe, b_pe, enc_qkv_t,
                                          enc_proj.reshape(n_layers, width, width), enc_up, enc_down, w_ed)
        acts = decode(sp, z_all, mask_all, pos_all, mask_token, dec_qkv_t,
                      dec_proj.reshape(n_layers, d_width, d_width), dec_up, dec_down)
        return jnp.einsum('cne,ep->cnp', acts, w_out, preferred_element_type=F32)

    row_spec = P('dp', 'sp', None)
    pos_spec = P(('dp', 'sp'), None)
    arg_specs = (row_spec, P('dp', 'sp'), pos_spec, pos_spec) + (P(),) * 13
    return jax.shard_map(local_program, mesh=mesh, in_specs=arg_specs, out_specs=row_spec, check_vma=False)
```

```python
import functools

import jax
import jax.numpy as jnp
from jax import lax
from jax.experimental import pallas as pl
from jax.experimental.pallas import tpu as pltpu
from jax.sharding import PartitionSpec as P

KEEP_DIV = 8


BF = jnp.bfloat16
F32 = jnp.float32
NT = (((1,), (1,)), ((), ()))
TN = (((0,), (0,)), ((), ()))
NN = (((1,), (0,)), ((), ()))
LOG2E = 1.4426950408889634
MESH = pl.DeviceIdType.MESH
VMEM = pl.BlockSpec(memory_space=pltpu.VMEM)
ANY = pl.BlockSpec(memory_space=pl.ANY)


def mm(lhs, rhs, dims=NN):
    return lax.dot_general(lhs, rhs, dims, preferred_element_type=F32)


def norm_rows(hidden):
    wide = hidden.astype(F32)
    centred = wide - jnp.mean(wide, axis=-1, keepdims=True)
    var = jnp.mean(centred * centred, axis=-1, keepdims=True)
    return (centred * lax.rsqrt(var + 1e-6)).astype(BF)


def gelu(x):
    return 0.5 * x * (1.0 + lax.erf(x * 0.7071067811865476))


def attend_clip(tok, rows, heads, hd, k_s, vt_s, q_s, s_s, o_s):
    c2 = hd ** -0.5 * LOG2E
    group = 256 // hd
    chunk = 256
    n_chunks = tok // chunk

    def q_of(h):
        g = h // group
        qg = q_s[pl.ds(pl.multiple_of(g * 256, 256), 256), :]
        row_head = lax.broadcasted_iota(jnp.int32, (256, rows), 0) // hd
        return jnp.where(row_head == h - g * group, qg, jnp.zeros_like(qg)), pl.multiple_of(g * 256, 256)

    def scores(h, slot):
        qz, g0 = q_of(h)
        top = None
        for j in range(n_chunks):
            s = mm(k_s[j * chunk:(j + 1) * chunk, pl.ds(g0, 256)], qz)
            s_s[slot, j * chunk:(j + 1) * chunk, :] = s
            t = jnp.max(s.reshape(chunk // 8, 8, rows), axis=0)
            top = t if top is None else jnp.maximum(top, t)
        return top

    def finish(h, slot, top):
        m = jnp.max(top, axis=0, keepdims=True) * c2
        total = None
        acc = None
        v0 = pl.multiple_of(h * hd, hd)
        for j in range(n_chunks):
            e = jnp.exp2(s_s[slot, j * chunk:(j + 1) * chunk, :] * c2 - m)
            t = jnp.sum(e.reshape(chunk // 8, 8, rows), axis=0)
            total = t if total is None else total + t
            a = mm(vt_s[pl.ds(v0, hd), j * chunk:(j + 1) * chunk], e.astype(BF))
            acc = a if acc is None else acc + a
        denom = jnp.sum(total, axis=0, keepdims=True)
        o_s[pl.ds(v0, hd), :] = (acc / denom).astype(BF)

    first = scores(0, 0)

    def body(i, top0):
        h = 2 * i
        top1 = scores(h + 1, 1)
        finish(h, 0, top0)
        nxt = scores(jnp.minimum(h + 2, heads - 1), 0)
        finish(h + 1, 1, top1)
        return nxt

    lax.fori_loop(0, heads // 2, body, first)


def enc_kernel(sp, mask_ref, patches_h, enc_pos_h, dec_pos_h, w_pe_h, b_pe_ref, qkv_h, proj_h, up_h, down_h, w_ed_h,
               z_all, mask_all, pos_all,
               patches, enc_pos, w_pe, w_ed, wqkv, wproj, wup, wdown, x_s, e_src, tail_s, win, hid, a_all, qkv_s, s_s, p_s, o_s, g_s,
               wsem, insem, ms, mr, ws, wr, es, er, asend, arecv, zs, zr, pfs, pfr, pns, pnr, lsem):
    me = lax.axis_index('sp')
    n_clips, rows, width = patches.shape[0], patches.shape[1], hid.shape[1]
    cap = e_src.shape[0] // n_clips
    half = tail_s.shape[0] // n_clips
    n_layers = qkv_h.shape[0]
    my_rows = hid.shape[0]
    per = sp // n_clips
    heads = 16
    hd = width // heads
    clip = me // per
    hf = lax.rem(me, 2)
    partner = me + 1 - 2 * hf
    my_half = me // per
    slot = lax.rem(me, per)

    def weight(l, i):
        src, dst = ((qkv_h, wqkv), (proj_h, wproj), (up_h, wup), (down_h, wdown))[i]
        return pltpu.make_async_copy(src.at[l], dst, wsem.at[i])

    loads = [pltpu.make_async_copy(a, b, insem.at[i]) for i, (a, b) in enumerate(
        [(patches_h, patches), (enc_pos_h, enc_pos), (w_pe_h, w_pe), (w_ed_h, w_ed)])]
    for ld in loads:
        ld.start()

    barrier = pltpu.get_barrier_semaphore()
    for k in range(1, sp):
        pl.semaphore_signal(barrier, inc=1, device_id={'sp': lax.rem(me + k, sp)}, device_id_type=MESH)

    mask = mask_ref[...]
    maskf = mask.astype(F32)
    before = (lax.broadcasted_iota(jnp.int32, (rows, rows), 0) < lax.broadcasted_iota(jnp.int32, (rows, rows), 1))
    mask8 = jnp.concatenate([maskf] + [jnp.zeros_like(maskf)] * 7, axis=0).astype(BF)
    rank = mm(mask8, before.astype(BF)).astype(jnp.int32)
    row_id = lax.broadcasted_iota(jnp.int32, (cap, rows), 0)
    picks = []
    for c in range(n_clips):
        picks.append(jnp.where((row_id == rank[c:c + 1, :]) & (mask[c:c + 1, :] == 1), 1.0, 0.0))
    pick2 = jnp.concatenate(picks, axis=0)
    used = jnp.sum(pick2, axis=1, keepdims=True)
    pick2 = pick2.astype(BF)
    for ld in loads[:2]:
        ld.wait()
    for c in range(n_clips):
        x_s[c * cap:(c + 1) * cap, :] = mm(pick2[c * cap:(c + 1) * cap], patches[c]).astype(BF)
    fixed = used * b_pe_ref[...].reshape(1, width).astype(F32) + mm(pick2, enc_pos[...])
    loads[2].wait()
    for i in range(4):
        weight(0, i).start()
    e_src[...] = (mm(x_s[...], w_pe[...]) + fixed).astype(BF)
    late = lax.broadcasted_iota(jnp.int32, (half, cap), 1) - lax.broadcasted_iota(jnp.int32, (half, cap), 0) + half
    for c in range(n_clips):
        count = jnp.sum(maskf[c:c + 1, :], axis=1, keepdims=True).astype(jnp.int32)
        pick = jnp.where(late == count, 1.0, 0.0).astype(BF)
        tail_s[c * half:(c + 1) * half, :] = mm(pick, e_src[c * cap:(c + 1) * cap, :]).astype(BF)

    pl.semaphore_wait(barrier, sp - 1)

    def to(c, x, h):
        return per * c + 2 * x + h

    def send(c, x):
        return pltpu.make_async_remote_copy(
            src_ref=e_src.at[pl.ds(c * cap, cap)], dst_ref=win.at[pl.ds(pl.multiple_of(slot * cap, cap), cap)],
            send_sem=ws.at[c, x], recv_sem=wr.at[slot], device_id={'sp': to(c, x, my_half)}, device_id_type=MESH)

    last = per * cap
    edges = ((per, 0, e_src, cap), (per - 1, 1, tail_s, half))

    def send_edge(c, x, h, buf, step):
        return pltpu.make_async_remote_copy(
            src_ref=buf.at[pl.ds(c * step, half)], dst_ref=win.at[pl.ds(last, half)], send_sem=es.at[c, x], recv_sem=er,
            device_id={'sp': to(c, x, h)}, device_id_type=MESH)

    for c in range(n_clips):
        for x in range(per // 2):
            @pl.when(to(c, x, my_half) != me)
            def _():
                send(c, x).start()

            @pl.when(to(c, x, my_half) == me)
            def _():
                pltpu.make_async_copy(
                    e_src.at[pl.ds(c * cap, cap)], win.at[pl.ds(pl.multiple_of(slot * cap, cap), cap)], wr.at[slot]).start()

            for src_dev, h, buf, step in edges:
                @pl.when((me == src_dev) & (to(c, x, h) != me))
                def _():
                    send_edge(c, x, h, buf, step).start()

                @pl.when((me == src_dev) & (to(c, x, h) == me))
                def _():
                    pltpu.make_async_copy(buf.at[pl.ds(c * step, half)], win.at[pl.ds(last, half)], er).start()

    mask_sends = []
    for k in range(1, sp):
        mask_sends.append(pltpu.make_async_remote_copy(
            src_ref=mask_ref, dst_ref=mask_all.at[me], send_sem=ms.at[k], recv_sem=mr.at[k],
            device_id={'sp': lax.rem(me + k, sp)}, device_id_type=MESH))
        mask_sends[-1].start()
    own_mask = pltpu.make_async_copy(mask_ref, mask_all.at[me], lsem.at[0])
    own_mask.start()
    for m in mask_sends:
        m.wait_recv()
    own_mask.wait()
    starts = [jnp.zeros((1, 1), F32)]
    for s in range(sp):
        both = mask_all[s].astype(F32)
        row = jnp.where(clip == 0, both[0:1, :], both[1:2, :])
        starts.append(starts[-1] + jnp.sum(row, axis=1, keepdims=True))
    out_row = lax.broadcasted_iota(jnp.int32, (my_rows, cap), 0) - lax.broadcasted_iota(jnp.int32, (my_rows, cap), 1)
    places = []
    for b in range(per):
        off = jnp.where(hf == 0, starts[b], starts[per + b] - my_rows).astype(jnp.int32)
        places.append(jnp.where(out_row == off, 1.0, 0.0))
    off = jnp.where(hf == 0, starts[per], starts[per] - half - my_rows).astype(jnp.int32)
    places.append(jnp.where(out_row[:, :half] == off, 1.0, 0.0))
    place_a = jnp.concatenate(places[:per], axis=1).astype(BF)
    place_b = places[per].astype(BF)

    for b in range(per):
        pltpu.make_async_copy(e_src.at[pl.ds(0, cap)], win.at[pl.ds(b * cap, cap)], wr.at[b]).wait()
    pltpu.make_async_copy(e_src.at[pl.ds(0, half)], win.at[pl.ds(last, half)], er).wait()
    hid[...] = (mm(place_a, win[:last, :]) + mm(place_b, win[last:, :])).astype(BF)

    scale = hd ** -0.5
    pos_own = pltpu.make_async_copy(dec_pos_h, pos_all.at[me], lsem.at[1])
    pos_own.start()

    def pos_far(k):
        return pltpu.make_async_remote_copy(
            src_ref=dec_pos_h, dst_ref=pos_all.at[me], send_sem=pfs.at[k], recv_sem=pfr.at[k],
            device_id={'sp': lax.rem(me + 2 * k, sp)}, device_id_type=MESH)

    def pos_near(k):
        piece = lax.rem(me + 2 * k, sp)
        return pltpu.make_async_remote_copy(
            src_ref=pos_all.at[piece], dst_ref=pos_all.at[piece], send_sem=pns.at[k], recv_sem=pnr.at[k],
            device_id={'sp': partner}, device_id_type=MESH)

    def layer(l, carry):
        def refill(i):
            @pl.when(l < n_layers - 1)
            def _():
                weight(l + 1, i).start()

        a_all[l, 0] = norm_rows(hid[...])
        swap = pltpu.make_async_remote_copy(
            src_ref=a_all.at[l, 0], dst_ref=a_all.at[l, 1], send_sem=asend.at[l], recv_sem=arecv.at[l],
            device_id={'sp': partner}, device_id_type=MESH)
        swap.start()
        weight(l, 0).wait()
        swap.wait()
        qkv_s[...] = mm(wqkv[...], a_all[l].reshape(2 * my_rows, width), NT).astype(BF)
        refill(0)

        @pl.when(l == 0)
        def _():
            for k in range(1, sp // 2):
                pos_far(k).start()

        for h in range(heads):
            s_s[h] = mm(qkv_s[h * hd:(h + 1) * hd, :my_rows], qkv_s[width + h * hd:width + (h + 1) * hd, :], TN)

        def soft(i, cc):
            s = s_s[i] * scale
            e = jnp.exp(s - jnp.max(s, axis=-1, keepdims=True))
            p_s[i] = (e / jnp.sum(e, axis=-1, keepdims=True)).astype(BF)
            return cc

        lax.fori_loop(0, heads, soft, 0, unroll=4)
        for h in range(heads):
            o_s[h * hd:(h + 1) * hd, :] = mm(qkv_s[2 * width + h * hd:2 * width + (h + 1) * hd, :], p_s[h], NT).astype(BF)
        weight(l, 1).wait()
        h1 = (hid[...].astype(F32) + mm(o_s[...], wproj[...], TN)).astype(BF)
        hid[...] = h1
        refill(1)
        a2 = norm_rows(h1)
        weight(l, 2).wait()
        g_s[...] = gelu(mm(a2, wup[...])).astype(BF)
        refill(2)

        @pl.when(l == n_layers - 1)
        def _():
            pos_own.wait()
            for k in range(1, sp // 2):
                pos_far(k).wait_recv()
            for k in range(sp // 2):
                pos_near(k).start()

        weight(l, 3).wait()
        hid[...] = (hid[...].astype(F32) + mm(g_s[...], wdown[...])).astype(BF)
        refill(3)
        return carry

    lax.fori_loop(0, n_layers, layer, 0)

    loads[3].wait()
    at = pl.multiple_of(hf * my_rows, my_rows)
    mine = z_all.at[clip, pl.ds(at, my_rows), :]
    other_clip = n_clips - 1 - clip
    theirs = z_all.at[other_clip, pl.ds(at, my_rows), :]
    z_all[clip, pl.ds(at, my_rows), :] = mm(norm_rows(hid[...]), w_ed[...]).astype(BF)

    def z_send(i, ref, dst):
        return pltpu.make_async_remote_copy(
            src_ref=ref, dst_ref=ref, send_sem=zs.at[i], recv_sem=zr.at[i], device_id={'sp': dst}, device_id_type=MESH)

    across = z_send(0, mine, lax.rem(me + per, sp))
    beside = z_send(1, mine, partner)
    relay = z_send(2, theirs, partner)
    across.start()
    beside.start()
    for m in mask_sends:
        m.wait_send()
    for c in range(n_clips):
        for x in range(per // 2):
            @pl.when(to(c, x, my_half) != me)
            def _():
                send(c, x).wait_send()

            for src_dev, h, buf, step in edges:
                @pl.when((me == src_dev) & (to(c, x, h) != me))
                def _():
                    send_edge(c, x, h, buf, step).wait_send()
    for k in range(1, sp // 2):
        pos_far(k).wait_send()
    across.wait_recv()
    relay.start()
    for k in range(sp // 2):
        pos_near(k).wait()
    across.wait_send()
    beside.wait()
    relay.wait()


def encode(sp, vis_mask, patches, enc_pos, dec_pos, w_pe, b_pe, qkv_t, proj, up, down, w_ed):
    n_clips, rows, p_width = patches.shape
    width = w_pe.shape[1]
    d_width = w_ed.shape[1]
    cap = 2 * rows // KEEP_DIV
    half = cap // 4
    my_rows = rows * sp // KEEP_DIV // 2
    dma = pltpu.SemaphoreType.DMA
    per = sp // n_clips
    far = sp // 2
    return pl.pallas_call(
        functools.partial(enc_kernel, sp),
        out_shape=(jax.ShapeDtypeStruct((n_clips, 2 * my_rows, d_width), BF),
                   jax.ShapeDtypeStruct((sp, n_clips, rows), jnp.int32),
                   jax.ShapeDtypeStruct((sp, rows, d_width), BF)),
        in_specs=[VMEM, ANY, ANY, ANY, ANY, VMEM, ANY, ANY, ANY, ANY, ANY],
        out_specs=(VMEM, VMEM, ANY),
        scratch_shapes=[
            pltpu.VMEM(patches.shape, BF), pltpu.VMEM(enc_pos.shape, BF), pltpu.VMEM(w_pe.shape, BF), pltpu.VMEM(w_ed.shape, BF),
            pltpu.VMEM(qkv_t.shape[1:], BF), pltpu.VMEM(proj.shape[1:], BF), pltpu.VMEM(up.shape[1:], BF), pltpu.VMEM(down.shape[1:], BF),
            pltpu.VMEM((n_clips * cap, p_width), BF), pltpu.VMEM((n_clips * cap, width), BF), pltpu.VMEM((n_clips * half, width), BF),
            pltpu.VMEM((per * cap + half, width), BF),
            pltpu.VMEM((my_rows, width), BF), pltpu.VMEM((qkv_t.shape[0], 2, my_rows, width), BF),
            pltpu.VMEM((3 * width, 2 * my_rows), BF),
            pltpu.VMEM((16, my_rows, 2 * my_rows), F32), pltpu.VMEM((16, my_rows, 2 * my_rows), BF),
            pltpu.VMEM((width, my_rows), BF), pltpu.VMEM((my_rows, 4 * width), BF),
            dma((4,)), dma((4,)), dma((sp,)), dma((sp,)), dma((n_clips, per // 2)), dma((per,)), dma((n_clips, per // 2)), dma,
            dma((2,)), dma((2,)), dma((3,)), dma((3,)), dma((far,)), dma((far,)), dma((far,)), dma((far,)), dma((2,)),
        ],
        compiler_params=pltpu.CompilerParams(collective_id=1, has_side_effects=True, vmem_limit_bytes=63 << 20),
        name='encode',
    )(vis_mask, patches, enc_pos, dec_pos, w_pe, b_pe, qkv_t, proj, up, down, w_ed)


def decode_kernel(sp, z_ref, mask_all, pos_h, tok_ref, wqkv_h, wproj_h, wup_h, wdown_h, a_out,
                  pos, wqkv, wproj, wup, wdown, rank_s, u_s, a_own, a_all, k_s, vt_s, q_s, s_s, o_s,
                  insem, fs, fr, ns, nr):
    me = lax.axis_index('sp')
    partner = me + 1 - 2 * lax.rem(me, 2)
    n_clips, n_vis, width = z_ref.shape
    rows = mask_all.shape[2]
    tok = rows * sp
    heads, hd = 16, width // 16
    n_far = sp // 2

    loads = [pltpu.make_async_copy(a, b, insem.at[i]) for i, (a, b) in enumerate(
        [(pos_h, pos), (wqkv_h, wqkv), (wproj_h, wproj), (wup_h, wup), (wdown_h, wdown)])]
    for ld in loads:
        ld.start()
    barrier = pltpu.get_barrier_semaphore()
    for k in range(1, sp):
        pl.semaphore_signal(barrier, inc=1, device_id={'sp': lax.rem(me + k, sp)}, device_id_type=MESH)
    pl.semaphore_wait(barrier, sp - 1)

    before = (lax.broadcasted_iota(jnp.int32, (rows, rows), 0) < lax.broadcasted_iota(jnp.int32, (rows, rows), 1)).astype(BF)
    pad = 16
    row_id = lax.broadcasted_iota(jnp.int32, (n_vis + pad, rows), 0)
    for c in range(n_clips):
        m = mask_all[:, c, :]
        local = mm(m.astype(F32).astype(BF), before)
        base = jnp.zeros((1, 1), F32)
        for s in range(sp):
            vis = m[s:s + 1, :]
            rank_s[c, s:s + 1, :] = jnp.where(vis == 1, (local[s:s + 1, :] + base).astype(jnp.int32), n_vis)
            base = base + jnp.sum(vis.astype(F32), axis=1, keepdims=True)
    for ld in loads[:2]:
        ld.wait()

    def far(c, k):
        return pltpu.make_async_remote_copy(
            src_ref=a_own.at[c], dst_ref=a_all.at[c, me], send_sem=fs.at[c, k], recv_sem=fr.at[c, k],
            device_id={'sp': lax.rem(me + 2 * k, sp)}, device_id_type=MESH)

    def near(c, k):
        piece = lax.rem(me + 2 * k, sp)
        return pltpu.make_async_remote_copy(
            src_ref=a_all.at[c, piece] if k else a_own.at[c], dst_ref=a_all.at[c, piece],
            send_sem=ns.at[c, k], recv_sem=nr.at[c, k], device_id={'sp': partner}, device_id_type=MESH)

    def relay(c):
        for k in range(1, n_far):
            far(c, k).wait_recv()
        for k in range(n_far):
            near(c, k).start()

    def keys_values(l, b, blk):
        at = pl.multiple_of(b * rows, rows)
        k_s[pl.ds(at, rows), :] = mm(blk, wqkv[l, width:2 * width, :], NT).astype(BF)
        vt_s[:, pl.ds(at, rows)] = mm(wqkv[l, 2 * width:, :], blk, NT).astype(BF)

    def attend(l, c):
        q_s[...] = mm(wqkv[l, :width, :], a_own[c], NT).astype(BF)
        attend_clip(tok, rows, heads, hd, k_s, vt_s, q_s, s_s, o_s)

    def feed(l, c):
        h1 = (u_s[c].astype(F32) + mm(o_s[...], wproj[l], TN)).astype(BF)
        g = gelu(mm(norm_rows(h1), wup[l])).astype(BF)
        return (h1.astype(F32) + mm(g, wdown[l])).astype(BF)

    def first(c, carry):
        z_aug = jnp.concatenate([z_ref[c], tok_ref[...].reshape(1, width), jnp.zeros((pad - 1, width), BF)], axis=0)

        def block(b, cc):
            pick = jnp.where(row_id == rank_s[c, pl.ds(b, 1), :], 1.0, 0.0).astype(BF)
            u = (mm(pick, z_aug, TN) + pos[b].astype(F32)).astype(BF)
            a = norm_rows(u)
            keys_values(0, b, a)

            @pl.when(b == me)
            def _():
                u_s[c] = u
                a_own[c] = a
            return cc

        lax.fori_loop(0, sp, block, 0)
        attend(0, c)

        @pl.when(c == 0)
        def _():
            for ld in loads[2:]:
                ld.wait()

        @pl.when(c == 1)
        def _():
            relay(0)

        u1 = feed(0, c)
        u_s[c] = u1
        a_own[c] = norm_rows(u1)
        for k in range(1, n_far):
            far(c, k).start()
        return carry

    lax.fori_loop(0, n_clips, first, 0)

    def second(c, carry):
        keys_values(1, me, a_own[c])

        def same(k, cc):
            b = lax.rem(me + 2 * k, sp)
            keys_values(1, b, a_all[c, b])
            return cc

        def other(k, cc):
            b = lax.rem(partner + 2 * k, sp)
            keys_values(1, b, a_all[c, b])
            return cc

        lax.fori_loop(1, n_far, same, 0)
        for k in range(n_far):
            near(c, k).wait_recv()
        lax.fori_loop(0, n_far, other, 0)
        attend(1, c)

        @pl.when(c == 0)
        def _():
            relay(1)

        a_out[c] = norm_rows(feed(1, c))
        return carry

    lax.fori_loop(0, n_clips, second, 0)
    for c in range(n_clips):
        for k in range(n_far):
            near(c, k).wait_send()
            if k:
                far(c, k).wait_send()


def decode(sp, z_all, mask_all, pos_all, mask_token, wqkv, wproj, wup, wdown):
    n_clips, n_vis, width = z_all.shape
    rows = mask_all.shape[2]
    tok = rows * sp
    dma = pltpu.SemaphoreType.DMA
    return pl.pallas_call(
        functools.partial(decode_kernel, sp),
        out_shape=jax.ShapeDtypeStruct((n_clips, rows, width), BF),
        in_specs=[VMEM, VMEM, ANY, VMEM, ANY, ANY, ANY, ANY],
        out_specs=VMEM,
        scratch_shapes=[
            pltpu.VMEM(pos_all.shape, BF), pltpu.VMEM(wqkv.shape, BF), pltpu.VMEM(wproj.shape, BF),
            pltpu.VMEM(wup.shape, BF), pltpu.VMEM(wdown.shape, BF),
            pltpu.VMEM((n_clips, sp, rows), jnp.int32), pltpu.VMEM((n_clips, rows, width), BF), pltpu.VMEM((n_clips, rows, width), BF),
            pltpu.VMEM((n_clips, sp, rows, width), BF),
            pltpu.VMEM((tok, width), BF), pltpu.VMEM((width, tok), BF), pltpu.VMEM((width, rows), BF),
            pltpu.VMEM((2, tok, rows), F32), pltpu.VMEM((width, rows), BF),
            dma((5,)), dma((n_clips, sp // 2)), dma((n_clips, sp // 2)), dma((n_clips, sp // 2)), dma((n_clips, sp // 2)),
        ],
        compiler_params=pltpu.CompilerParams(collective_id=2, has_side_effects=True, vmem_limit_bytes=52 << 20),
        name='decode',
    )(z_all, mask_all, pos_all, mask_token, wqkv, wproj, wup, wdown)


def solution(mesh):
    sp = mesh.shape['sp']

    def local_program(patches, vis_mask, enc_pos, dec_pos, w_pe, b_pe, enc_qkv, enc_proj, enc_up, enc_down, w_ed, mask_token, dec_qkv, dec_proj, dec_up, dec_down, w_out):
        n_layers, width = enc_qkv.shape[:2]
        d_width = dec_qkv.shape[1]
        enc_qkv_t = jnp.transpose(enc_qkv, (0, 2, 3, 4, 1)).reshape(n_layers, 3 * width, width)
        dec_qkv_t = jnp.transpose(dec_qkv, (0, 2, 3, 4, 1)).reshape(n_layers, 3 * d_width, d_width)
        z_all, mask_all, pos_all = encode(sp, vis_mask, patches, enc_pos, dec_pos, w_pe, b_pe, enc_qkv_t,
                                          enc_proj.reshape(n_layers, width, width), enc_up, enc_down, w_ed)
        acts = decode(sp, z_all, mask_all, pos_all, mask_token, dec_qkv_t,
                      dec_proj.reshape(n_layers, d_width, d_width), dec_up, dec_down)
        return jnp.einsum('cne,ep->cnp', acts, w_out, preferred_element_type=F32)

    row_spec = P('dp', 'sp', None)
    pos_spec = P(('dp', 'sp'), None)
    arg_specs = (row_spec, P('dp', 'sp'), pos_spec, pos_spec) + (P(),) * 13
    return jax.shard_map(local_program, mesh=mesh, in_specs=arg_specs, out_specs=row_spec, check_vma=False)
```

```python
import functools

import jax
import jax.numpy as jnp
from jax import lax
from jax.experimental import pallas as pl
from jax.experimental.pallas import tpu as pltpu
from jax.sharding import PartitionSpec as P

KEEP_DIV = 8


BF = jnp.bfloat16
F32 = jnp.float32
NT = (((1,), (1,)), ((), ()))
TN = (((0,), (0,)), ((), ()))
NN = (((1,), (0,)), ((), ()))
LOG2E = 1.4426950408889634
MESH = pl.DeviceIdType.MESH
VMEM = pl.BlockSpec(memory_space=pltpu.VMEM)
ANY = pl.BlockSpec(memory_space=pl.ANY)


def mm(lhs, rhs, dims=NN):
    return lax.dot_general(lhs, rhs, dims, preferred_element_type=F32)


def norm_rows(hidden):
    wide = hidden.astype(F32)
    centred = wide - jnp.mean(wide, axis=-1, keepdims=True)
    var = jnp.mean(centred * centred, axis=-1, keepdims=True)
    return (centred * lax.rsqrt(var + 1e-6)).astype(BF)


def gelu(x):
    return 0.5 * x * (1.0 + lax.erf(x * 0.7071067811865476))


def attend_clip(tok, rows, heads, hd, k_s, vt_s, q_s, s_s, o_s):
    c2 = hd ** -0.5 * LOG2E
    group = 256 // hd
    chunk = 256
    n_chunks = tok // chunk

    def q_of(h):
        g = h // group
        qg = q_s[pl.ds(pl.multiple_of(g * 256, 256), 256), :]
        row_head = lax.broadcasted_iota(jnp.int32, (256, rows), 0) // hd
        return jnp.where(row_head == h - g * group, qg, jnp.zeros_like(qg)), pl.multiple_of(g * 256, 256)

    def scores(h, slot):
        qz, g0 = q_of(h)
        top = None
        for j in range(n_chunks):
            s = mm(k_s[j * chunk:(j + 1) * chunk, pl.ds(g0, 256)], qz)
            s_s[slot, j * chunk:(j + 1) * chunk, :] = s
            t = jnp.max(s.reshape(chunk // 8, 8, rows), axis=0)
            top = t if top is None else jnp.maximum(top, t)
        return top

    def finish(h, slot, top):
        m = jnp.max(top, axis=0, keepdims=True) * c2
        total = None
        acc = None
        v0 = pl.multiple_of(h * hd, hd)
        for j in range(n_chunks):
            e = jnp.exp2(s_s[slot, j * chunk:(j + 1) * chunk, :] * c2 - m)
            t = jnp.sum(e.reshape(chunk // 8, 8, rows), axis=0)
            total = t if total is None else total + t
            a = mm(vt_s[pl.ds(v0, hd), j * chunk:(j + 1) * chunk], e.astype(BF))
            acc = a if acc is None else acc + a
        denom = jnp.sum(total, axis=0, keepdims=True)
        o_s[pl.ds(v0, hd), :] = (acc / denom).astype(BF)

    first = scores(0, 0)

    def body(i, top0):
        h = 2 * i
        top1 = scores(h + 1, 1)
        finish(h, 0, top0)
        nxt = scores(jnp.minimum(h + 2, heads - 1), 0)
        finish(h + 1, 1, top1)
        return nxt

    lax.fori_loop(0, heads // 2, body, first)


def enc_kernel(sp, mask_ref, patches_h, enc_pos_h, dec_pos_h, w_pe_h, b_pe_ref, qkv_h, proj_h, up_h, down_h,
               hid_out, mask_all, pos_all,
               patches, enc_pos, w_pe, wqkv, wproj, wup, wdown, x_s, e_src, tail_s, win, hid, a_all, qkv_s, s_s, p_s, o_s, g_s,
               wsem, insem, ms, mr, ws, wr, es, er, asend, arecv, pfs, pfr, pns, pnr, lsem):
    me = lax.axis_index('sp')
    n_clips, rows, width = patches.shape[0], patches.shape[1], hid.shape[1]
    cap = e_src.shape[0] // n_clips
    half = tail_s.shape[0] // n_clips
    n_layers = qkv_h.shape[0]
    my_rows = hid.shape[0]
    per = sp // n_clips
    heads = 16
    hd = width // heads
    clip = me // per
    hf = lax.rem(me, 2)
    partner = me + 1 - 2 * hf
    my_half = me // per
    slot = lax.rem(me, per)

    def weight(l, i):
        src, dst = ((qkv_h, wqkv), (proj_h, wproj), (up_h, wup), (down_h, wdown))[i]
        return pltpu.make_async_copy(src.at[l], dst, wsem.at[i])

    loads = [pltpu.make_async_copy(a, b, insem.at[i]) for i, (a, b) in enumerate(
        [(patches_h, patches), (enc_pos_h, enc_pos), (w_pe_h, w_pe)])]
    for ld in loads:
        ld.start()

    barrier = pltpu.get_barrier_semaphore()
    for k in range(1, sp):
        pl.semaphore_signal(barrier, inc=1, device_id={'sp': lax.rem(me + k, sp)}, device_id_type=MESH)

    mask = mask_ref[...]
    maskf = mask.astype(F32)
    before = (lax.broadcasted_iota(jnp.int32, (rows, rows), 0) < lax.broadcasted_iota(jnp.int32, (rows, rows), 1))
    mask8 = jnp.concatenate([maskf] + [jnp.zeros_like(maskf)] * 7, axis=0).astype(BF)
    rank = mm(mask8, before.astype(BF)).astype(jnp.int32)
    row_id = lax.broadcasted_iota(jnp.int32, (cap, rows), 0)
    picks = []
    for c in range(n_clips):
        picks.append(jnp.where((row_id == rank[c:c + 1, :]) & (mask[c:c + 1, :] == 1), 1.0, 0.0))
    pick2 = jnp.concatenate(picks, axis=0)
    used = jnp.sum(pick2, axis=1, keepdims=True)
    pick2 = pick2.astype(BF)
    for ld in loads[:2]:
        ld.wait()
    for c in range(n_clips):
        x_s[c * cap:(c + 1) * cap, :] = mm(pick2[c * cap:(c + 1) * cap], patches[c]).astype(BF)
    fixed = used * b_pe_ref[...].reshape(1, width).astype(F32) + mm(pick2, enc_pos[...])
    loads[2].wait()
    for i in range(4):
        weight(0, i).start()
    e_src[...] = (mm(x_s[...], w_pe[...]) + fixed).astype(BF)
    late = lax.broadcasted_iota(jnp.int32, (half, cap), 1) - lax.broadcasted_iota(jnp.int32, (half, cap), 0) + half
    for c in range(n_clips):
        count = jnp.sum(maskf[c:c + 1, :], axis=1, keepdims=True).astype(jnp.int32)
        pick = jnp.where(late == count, 1.0, 0.0).astype(BF)
        tail_s[c * half:(c + 1) * half, :] = mm(pick, e_src[c * cap:(c + 1) * cap, :]).astype(BF)

    pl.semaphore_wait(barrier, sp - 1)

    def to(c, x, h):
        return per * c + 2 * x + h

    def send(c, x):
        return pltpu.make_async_remote_copy(
            src_ref=e_src.at[pl.ds(c * cap, cap)], dst_ref=win.at[pl.ds(pl.multiple_of(slot * cap, cap), cap)],
            send_sem=ws.at[c, x], recv_sem=wr.at[slot], device_id={'sp': to(c, x, my_half)}, device_id_type=MESH)

    last = per * cap
    edges = ((per, 0, e_src, cap), (per - 1, 1, tail_s, half))

    def send_edge(c, x, h, buf, step):
        return pltpu.make_async_remote_copy(
            src_ref=buf.at[pl.ds(c * step, half)], dst_ref=win.at[pl.ds(last, half)], send_sem=es.at[c, x], recv_sem=er,
            device_id={'sp': to(c, x, h)}, device_id_type=MESH)

    for c in range(n_clips):
        for x in range(per // 2):
            @pl.when(to(c, x, my_half) != me)
            def _():
                send(c, x).start()

            @pl.when(to(c, x, my_half) == me)
            def _():
                pltpu.make_async_copy(
                    e_src.at[pl.ds(c * cap, cap)], win.at[pl.ds(pl.multiple_of(slot * cap, cap), cap)], wr.at[slot]).start()

            for src_dev, h, buf, step in edges:
                @pl.when((me == src_dev) & (to(c, x, h) != me))
                def _():
                    send_edge(c, x, h, buf, step).start()

                @pl.when((me == src_dev) & (to(c, x, h) == me))
                def _():
                    pltpu.make_async_copy(buf.at[pl.ds(c * step, half)], win.at[pl.ds(last, half)], er).start()

    mask_sends = []
    for k in range(1, sp):
        mask_sends.append(pltpu.make_async_remote_copy(
            src_ref=mask_ref, dst_ref=mask_all.at[me], send_sem=ms.at[k], recv_sem=mr.at[k],
            device_id={'sp': lax.rem(me + k, sp)}, device_id_type=MESH))
        mask_sends[-1].start()
    own_mask = pltpu.make_async_copy(mask_ref, mask_all.at[me], lsem.at[0])
    own_mask.start()
    for m in mask_sends:
        m.wait_recv()
    own_mask.wait()
    starts = [jnp.zeros((1, 1), F32)]
    for s in range(sp):
        both = mask_all[s].astype(F32)
        row = jnp.where(clip == 0, both[0:1, :], both[1:2, :])
        starts.append(starts[-1] + jnp.sum(row, axis=1, keepdims=True))
    out_row = lax.broadcasted_iota(jnp.int32, (my_rows, cap), 0) - lax.broadcasted_iota(jnp.int32, (my_rows, cap), 1)
    places = []
    for b in range(per):
        off = jnp.where(hf == 0, starts[b], starts[per + b] - my_rows).astype(jnp.int32)
        places.append(jnp.where(out_row == off, 1.0, 0.0))
    off = jnp.where(hf == 0, starts[per], starts[per] - half - my_rows).astype(jnp.int32)
    places.append(jnp.where(out_row[:, :half] == off, 1.0, 0.0))
    place_a = jnp.concatenate(places[:per], axis=1).astype(BF)
    place_b = places[per].astype(BF)

    for b in range(per):
        pltpu.make_async_copy(e_src.at[pl.ds(0, cap)], win.at[pl.ds(b * cap, cap)], wr.at[b]).wait()
    pltpu.make_async_copy(e_src.at[pl.ds(0, half)], win.at[pl.ds(last, half)], er).wait()
    hid[...] = (mm(place_a, win[:last, :]) + mm(place_b, win[last:, :])).astype(BF)

    scale = hd ** -0.5
    pos_own = pltpu.make_async_copy(dec_pos_h, pos_all.at[me], lsem.at[1])
    pos_own.start()

    def pos_far(k):
        return pltpu.make_async_remote_copy(
            src_ref=dec_pos_h, dst_ref=pos_all.at[me], send_sem=pfs.at[k], recv_sem=pfr.at[k],
            device_id={'sp': lax.rem(me + 2 * k, sp)}, device_id_type=MESH)

    def pos_near(k):
        piece = lax.rem(me + 2 * k, sp)
        return pltpu.make_async_remote_copy(
            src_ref=pos_all.at[piece], dst_ref=pos_all.at[piece], send_sem=pns.at[k], recv_sem=pnr.at[k],
            device_id={'sp': partner}, device_id_type=MESH)

    def layer(l, carry):
        def refill(i):
            @pl.when(l < n_layers - 1)
            def _():
                weight(l + 1, i).start()

        a_all[l, 0] = norm_rows(hid[...])
        swap = pltpu.make_async_remote_copy(
            src_ref=a_all.at[l, 0], dst_ref=a_all.at[l, 1], send_sem=asend.at[l], recv_sem=arecv.at[l],
            device_id={'sp': partner}, device_id_type=MESH)
        swap.start()
        weight(l, 0).wait()
        qkv_s[:width, :my_rows] = mm(wqkv[:width, :], a_all[l, 0], NT).astype(BF)
        swap.wait()
        qkv_s[width:, :] = mm(wqkv[width:, :], a_all[l].reshape(2 * my_rows, width), NT).astype(BF)
        refill(0)

        @pl.when(l == 0)
        def _():
            for k in range(1, sp // 2):
                pos_far(k).start()

        for h in range(heads):
            s_s[h] = mm(qkv_s[h * hd:(h + 1) * hd, :my_rows], qkv_s[width + h * hd:width + (h + 1) * hd, :], TN)

        def soft(i, cc):
            s = s_s[i] * scale
            e = jnp.exp(s - jnp.max(s, axis=-1, keepdims=True))
            p_s[i] = (e / jnp.sum(e, axis=-1, keepdims=True)).astype(BF)
            return cc

        lax.fori_loop(0, heads, soft, 0, unroll=4)
        for h in range(heads):
            o_s[h * hd:(h + 1) * hd, :] = mm(qkv_s[2 * width + h * hd:2 * width + (h + 1) * hd, :], p_s[h], NT).astype(BF)
        weight(l, 1).wait()
        h1 = (hid[...].astype(F32) + mm(o_s[...], wproj[...], TN)).astype(BF)
        hid[...] = h1
        refill(1)
        a2 = norm_rows(h1)
        weight(l, 2).wait()
        g_s[...] = gelu(mm(a2, wup[...])).astype(BF)
        refill(2)

        @pl.when(l == n_layers - 1)
        def _():
            pos_own.wait()
            for k in range(1, sp // 2):
                pos_far(k).wait_recv()
            for k in range(sp // 2):
                pos_near(k).start()

        weight(l, 3).wait()
        hid[...] = (hid[...].astype(F32) + mm(g_s[...], wdown[...])).astype(BF)
        refill(3)
        return carry

    lax.fori_loop(0, n_layers, layer, 0)

    hid_out[...] = hid[...]
    for m in mask_sends:
        m.wait_send()
    for c in range(n_clips):
        for x in range(per // 2):
            @pl.when(to(c, x, my_half) != me)
            def _():
                send(c, x).wait_send()

            for src_dev, h, buf, step in edges:
                @pl.when((me == src_dev) & (to(c, x, h) != me))
                def _():
                    send_edge(c, x, h, buf, step).wait_send()
    for k in range(1, sp // 2):
        pos_far(k).wait_send()
    for k in range(sp // 2):
        pos_near(k).wait()


def encode(sp, vis_mask, patches, enc_pos, dec_pos, w_pe, b_pe, qkv_t, proj, up, down):
    n_clips, rows, p_width = patches.shape
    width = w_pe.shape[1]
    d_width = dec_pos.shape[1]
    cap = 2 * rows // KEEP_DIV
    half = cap // 4
    my_rows = rows * sp // KEEP_DIV // 2
    dma = pltpu.SemaphoreType.DMA
    per = sp // n_clips
    far = sp // 2
    return pl.pallas_call(
        functools.partial(enc_kernel, sp),
        out_shape=(jax.ShapeDtypeStruct((my_rows, width), BF),
                   jax.ShapeDtypeStruct((sp, n_clips, rows), jnp.int32),
                   jax.ShapeDtypeStruct((sp, rows, d_width), BF)),
        in_specs=[VMEM, ANY, ANY, ANY, ANY, VMEM, ANY, ANY, ANY, ANY],
        out_specs=(VMEM, VMEM, ANY),
        scratch_shapes=[
            pltpu.VMEM(patches.shape, BF), pltpu.VMEM(enc_pos.shape, BF), pltpu.VMEM(w_pe.shape, BF),
            pltpu.VMEM(qkv_t.shape[1:], BF), pltpu.VMEM(proj.shape[1:], BF), pltpu.VMEM(up.shape[1:], BF), pltpu.VMEM(down.shape[1:], BF),
            pltpu.VMEM((n_clips * cap, p_width), BF), pltpu.VMEM((n_clips * cap, width), BF), pltpu.VMEM((n_clips * half, width), BF),
            pltpu.VMEM((per * cap + half, width), BF),
            pltpu.VMEM((my_rows, width), BF), pltpu.VMEM((qkv_t.shape[0], 2, my_rows, width), BF),
            pltpu.VMEM((3 * width, 2 * my_rows), BF),
            pltpu.VMEM((16, my_rows, 2 * my_rows), F32), pltpu.VMEM((16, my_rows, 2 * my_rows), BF),
            pltpu.VMEM((width, my_rows), BF), pltpu.VMEM((my_rows, 4 * width), BF),
            dma((4,)), dma((4,)), dma((sp,)), dma((sp,)), dma((n_clips, per // 2)), dma((per,)), dma((n_clips, per // 2)), dma,
            dma((2,)), dma((2,)), dma((far,)), dma((far,)), dma((far,)), dma((far,)), dma((2,)),
        ],
        compiler_params=pltpu.CompilerParams(collective_id=1, has_side_effects=True, vmem_limit_bytes=63 << 20),
        name='encode',
    )(vis_mask, patches, enc_pos, dec_pos, w_pe, b_pe, qkv_t, proj, up, down)


def decode_kernel(sp, hid_h, w_ed_h, mask_h, pos_h, tok_ref, wqkv_h, wproj_h, wup_h, wdown_h, a_out,
                  hid, w_ed, mask_all, pos, wqkv, wproj, wup, wdown, z_s, rank_s, u_s, a_own, a_all, km_s, vm_s, pv_s, k_s, vt_s, q_s, s_s, o_s,
                  insem, zs, zr, fs, fr, ns, nr):
    me = lax.axis_index('sp')
    hf = lax.rem(me, 2)
    partner = me + 1 - 2 * hf
    n_clips, n_vis, width = z_s.shape
    rows = mask_all.shape[2]
    my_rows = hid.shape[0]
    per = sp // n_clips
    clip_of = me // per
    tok = rows * sp
    heads, hd = 16, width // 16
    n_far = sp // 2

    loads = [pltpu.make_async_copy(a, b, insem.at[i]) for i, (a, b) in enumerate(
        [(hid_h, hid), (w_ed_h, w_ed), (mask_h, mask_all), (pos_h, pos), (wqkv_h, wqkv), (wproj_h, wproj), (wup_h, wup), (wdown_h, wdown)])]
    for ld in loads:
        ld.start()
    barrier = pltpu.get_barrier_semaphore()
    for k in range(1, sp):
        pl.semaphore_signal(barrier, inc=1, device_id={'sp': lax.rem(me + k, sp)}, device_id_type=MESH)

    at = pl.multiple_of(hf * my_rows, my_rows)
    mine = z_s.at[clip_of, pl.ds(at, my_rows), :]
    theirs = z_s.at[n_clips - 1 - clip_of, pl.ds(at, my_rows), :]
    for ld in loads[:2]:
        ld.wait()
    z_s[clip_of, pl.ds(at, my_rows), :] = mm(norm_rows(hid[...]), w_ed[...]).astype(BF)
    pl.semaphore_wait(barrier, sp - 1)

    def z_send(i, ref, dst):
        return pltpu.make_async_remote_copy(
            src_ref=ref, dst_ref=ref, send_sem=zs.at[i], recv_sem=zr.at[i], device_id={'sp': dst}, device_id_type=MESH)

    across = z_send(0, mine, lax.rem(me + per, sp))
    beside = z_send(1, mine, partner)
    relayed = z_send(2, theirs, partner)
    across.start()
    beside.start()

    before = (lax.broadcasted_iota(jnp.int32, (rows, rows), 0) < lax.broadcasted_iota(jnp.int32, (rows, rows), 1)).astype(BF)
    row_id = lax.broadcasted_iota(jnp.int32, (n_vis, rows), 0)
    loads[2].wait()
    for c in range(n_clips):
        m = mask_all[:, c, :]
        local = mm(m.astype(F32).astype(BF), before)
        base = jnp.zeros((1, 1), F32)
        for s in range(sp):
            vis = m[s:s + 1, :]
            rank_s[c, s:s + 1, :] = jnp.where(vis == 1, (local[s:s + 1, :] + base).astype(jnp.int32), n_vis)
            base = base + jnp.sum(vis.astype(F32), axis=1, keepdims=True)
    for ld in loads[3:5]:
        ld.wait()

    def pick_of(c, b):
        return jnp.where(row_id == rank_s[c, pl.ds(b, 1), :], 1.0, 0.0).astype(BF)

    def keys_values(l, b, blk, k_to, vt_to):
        here = pl.ds(pl.multiple_of(b * rows, rows), rows)
        k_to[here, :] = mm(blk, wqkv[l, width:2 * width, :], NT).astype(BF)
        vt_to[:, here] = mm(wqkv[l, 2 * width:, :], blk, NT).astype(BF)

    token = tok_ref[...].reshape(1, width).astype(F32)
    pv_s[...] = jnp.zeros_like(pv_s)

    def plain(b, cc):
        keys_values(0, b, norm_rows((token + pos[b].astype(F32)).astype(BF)), km_s, vm_s)
        for c in range(n_clips):
            pv_s[c] += mm(pick_of(c, b), pos[b])
        return cc

    lax.fori_loop(0, sp, plain, 0)

    def far(c, k):
        return pltpu.make_async_remote_copy(
            src_ref=a_own.at[c], dst_ref=a_all.at[c, me], send_sem=fs.at[c, k], recv_sem=fr.at[c, k],
            device_id={'sp': lax.rem(me + 2 * k, sp)}, device_id_type=MESH)

    def near(c, k):
        piece = lax.rem(me + 2 * k, sp)
        return pltpu.make_async_remote_copy(
            src_ref=a_all.at[c, piece] if k else a_own.at[c], dst_ref=a_all.at[c, piece],
            send_sem=ns.at[c, k], recv_sem=nr.at[c, k], device_id={'sp': partner}, device_id_type=MESH)

    def relay(c):
        for k in range(1, n_far):
            far(c, k).wait_recv()
        for k in range(n_far):
            near(c, k).start()

    def attend(l, c):
        q_s[...] = mm(wqkv[l, :width, :], a_own[c], NT).astype(BF)
        attend_clip(tok, rows, heads, hd, k_s, vt_s, q_s, s_s, o_s)

    def feed(l, c):
        h1 = (u_s[c].astype(F32) + mm(o_s[...], wproj[l], TN)).astype(BF)
        g = gelu(mm(norm_rows(h1), wup[l])).astype(BF)
        return (h1.astype(F32) + mm(g, wdown[l])).astype(BF)

    across.wait_recv()
    relayed.start()
    beside.wait_recv()
    relayed.wait_recv()

    def first(c, carry):
        u_vis = (z_s[c].astype(F32) + pv_s[c]).astype(BF)
        a_vis = norm_rows(u_vis)
        k_vis = mm(a_vis, wqkv[0, width:2 * width, :], NT).astype(BF)
        vt_vis = mm(wqkv[0, 2 * width:, :], a_vis, NT).astype(BF)
        k_aug = jnp.concatenate([k_vis, jnp.ones((n_vis, 128), BF)], axis=1)
        u_aug = jnp.concatenate([u_vis, jnp.ones((n_vis, 128), BF)], axis=1)

        def put(pick, aug, plain_rows):
            got = mm(pick, aug, TN)
            seen = jnp.concatenate([got[:, width:]] * (width // 128), axis=1)
            return jnp.where(seen > 0.5, got[:, :width], plain_rows.astype(F32)).astype(BF)

        def block(b, cc):
            here = pl.ds(pl.multiple_of(b * rows, rows), rows)
            pick = pick_of(c, b)
            k_s[here, :] = put(pick, k_aug, km_s[here, :])
            seen = rank_s[c, pl.ds(b, 1), :] < n_vis
            vt_s[:, here] = jnp.where(seen, mm(vt_vis, pick), vm_s[:, here].astype(F32)).astype(BF)
            return cc

        lax.fori_loop(0, sp, block, 0)
        u = put(pick_of(c, me), u_aug, (token + pos[me].astype(F32)).astype(BF))
        u_s[c] = u
        a_own[c] = norm_rows(u)
        attend(0, c)

        @pl.when(c == 0)
        def _():
            for ld in loads[5:]:
                ld.wait()

        @pl.when(c == 1)
        def _():
            relay(0)

        u1 = feed(0, c)
        u_s[c] = u1
        a_own[c] = norm_rows(u1)
        for k in range(1, n_far):
            far(c, k).start()
        return carry

    lax.fori_loop(0, n_clips, first, 0)

    def second(c, carry):
        keys_values(1, me, a_own[c], k_s, vt_s)

        def same(k, cc):
            b = lax.rem(me + 2 * k, sp)
            keys_values(1, b, a_all[c, b], k_s, vt_s)
            return cc

        def other(k, cc):
            b = lax.rem(partner + 2 * k, sp)
            keys_values(1, b, a_all[c, b], k_s, vt_s)
            return cc

        lax.fori_loop(1, n_far, same, 0)
        for k in range(n_far):
            near(c, k).wait_recv()
        lax.fori_loop(0, n_far, other, 0)
        attend(1, c)

        @pl.when(c == 0)
        def _():
            relay(1)

        a_out[c] = norm_rows(feed(1, c))
        return carry

    lax.fori_loop(0, n_clips, second, 0)
    for c in range(n_clips):
        for k in range(n_far):
            near(c, k).wait_send()
            if k:
                far(c, k).wait_send()
    across.wait_send()
    beside.wait_send()
    relayed.wait_send()


def decode(sp, hid, w_ed, mask_all, pos_all, mask_token, wqkv, wproj, wup, wdown):
    _, n_clips, rows = mask_all.shape
    width = w_ed.shape[1]
    tok = rows * sp
    n_vis = tok // KEEP_DIV
    dma = pltpu.SemaphoreType.DMA
    return pl.pallas_call(
        functools.partial(decode_kernel, sp),
        out_shape=jax.ShapeDtypeStruct((n_clips, rows, width), BF),
        in_specs=[ANY, ANY, ANY, ANY, VMEM, ANY, ANY, ANY, ANY],
        out_specs=VMEM,
        scratch_shapes=[
            pltpu.VMEM(hid.shape, BF), pltpu.VMEM(w_ed.shape, BF), pltpu.VMEM(mask_all.shape, jnp.int32),
            pltpu.VMEM(pos_all.shape, BF), pltpu.VMEM(wqkv.shape, BF), pltpu.VMEM(wproj.shape, BF),
            pltpu.VMEM(wup.shape, BF), pltpu.VMEM(wdown.shape, BF),
            pltpu.VMEM((n_clips, n_vis, width), BF),
            pltpu.VMEM((n_clips, sp, rows), jnp.int32), pltpu.VMEM((n_clips, rows, width), BF), pltpu.VMEM((n_clips, rows, width), BF),
            pltpu.VMEM((n_clips, sp, rows, width), BF),
            pltpu.VMEM((tok, width), BF), pltpu.VMEM((width, tok), BF), pltpu.VMEM((n_clips, n_vis, width), F32),
            pltpu.VMEM((tok, width), BF), pltpu.VMEM((width, tok), BF), pltpu.VMEM((width, rows), BF),
            pltpu.VMEM((2, tok, rows), F32), pltpu.VMEM((width, rows), BF),
            dma((8,)), dma((3,)), dma((3,)), dma((n_clips, sp // 2)), dma((n_clips, sp // 2)), dma((n_clips, sp // 2)), dma((n_clips, sp // 2)),
        ],
        compiler_params=pltpu.CompilerParams(collective_id=2, has_side_effects=True, vmem_limit_bytes=56 << 20),
        name='decode',
    )(hid, w_ed, mask_all, pos_all, mask_token, wqkv, wproj, wup, wdown)


def solution(mesh):
    sp = mesh.shape['sp']

    def local_program(patches, vis_mask, enc_pos, dec_pos, w_pe, b_pe, enc_qkv, enc_proj, enc_up, enc_down, w_ed, mask_token, dec_qkv, dec_proj, dec_up, dec_down, w_out):
        n_layers, width = enc_qkv.shape[:2]
        d_width = dec_qkv.shape[1]
        enc_qkv_t = jnp.transpose(enc_qkv, (0, 2, 3, 4, 1)).reshape(n_layers, 3 * width, width)
        dec_qkv_t = jnp.transpose(dec_qkv, (0, 2, 3, 4, 1)).reshape(n_layers, 3 * d_width, d_width)
        hid, mask_all, pos_all = encode(sp, vis_mask, patches, enc_pos, dec_pos, w_pe, b_pe, enc_qkv_t,
                                          enc_proj.reshape(n_layers, width, width), enc_up, enc_down)
        acts = decode(sp, hid, w_ed, mask_all, pos_all, mask_token, dec_qkv_t,
                      dec_proj.reshape(n_layers, d_width, d_width), dec_up, dec_down)
        return jnp.einsum('cne,ep->cnp', acts, w_out, preferred_element_type=F32)

    row_spec = P('dp', 'sp', None)
    pos_spec = P(('dp', 'sp'), None)
    arg_specs = (row_spec, P('dp', 'sp'), pos_spec, pos_spec) + (P(),) * 13
    return jax.shard_map(local_program, mesh=mesh, in_specs=arg_specs, out_specs=row_spec, check_vma=False)
```

```python
import functools

import jax
import jax.numpy as jnp
from jax import lax
from jax.experimental import pallas as pl
from jax.experimental.pallas import tpu as pltpu
from jax.sharding import PartitionSpec as P

KEEP_DIV = 8


BF = jnp.bfloat16
F32 = jnp.float32
NT = (((1,), (1,)), ((), ()))
TN = (((0,), (0,)), ((), ()))
NN = (((1,), (0,)), ((), ()))
LOG2E = 1.4426950408889634
MESH = pl.DeviceIdType.MESH
VMEM = pl.BlockSpec(memory_space=pltpu.VMEM)
ANY = pl.BlockSpec(memory_space=pl.ANY)


def mm(lhs, rhs, dims=NN):
    return lax.dot_general(lhs, rhs, dims, preferred_element_type=F32)


def norm_rows(hidden):
    wide = hidden.astype(F32)
    centred = wide - jnp.mean(wide, axis=-1, keepdims=True)
    var = jnp.mean(centred * centred, axis=-1, keepdims=True)
    return (centred * lax.rsqrt(var + 1e-6)).astype(BF)


def gelu(x):
    return 0.5 * x * (1.0 + lax.erf(x * 0.7071067811865476))


def attend_clip(tok, rows, heads, hd, k_s, vt_s, q_s, s_s, o_s):
    c2 = hd ** -0.5 * LOG2E
    group = 256 // hd
    chunk = 256
    n_chunks = tok // chunk

    def q_of(h):
        g = h // group
        qg = q_s[pl.ds(pl.multiple_of(g * 256, 256), 256), :]
        row_head = lax.broadcasted_iota(jnp.int32, (256, rows), 0) // hd
        return jnp.where(row_head == h - g * group, qg, jnp.zeros_like(qg)), pl.multiple_of(g * 256, 256)

    def scores(h, slot):
        qz, g0 = q_of(h)
        top = None
        for j in range(n_chunks):
            s = mm(k_s[j * chunk:(j + 1) * chunk, pl.ds(g0, 256)], qz)
            s_s[slot, j * chunk:(j + 1) * chunk, :] = s
            t = jnp.max(s.reshape(chunk // 8, 8, rows), axis=0)
            top = t if top is None else jnp.maximum(top, t)
        return top

    def finish(h, slot, top):
        m = jnp.max(top, axis=0, keepdims=True) * c2
        total = None
        acc = None
        v0 = pl.multiple_of(h * hd, hd)
        for j in range(n_chunks):
            e = jnp.exp2(s_s[slot, j * chunk:(j + 1) * chunk, :] * c2 - m)
            t = jnp.sum(e.reshape(chunk // 8, 8, rows), axis=0)
            total = t if total is None else total + t
            a = mm(vt_s[pl.ds(v0, hd), j * chunk:(j + 1) * chunk], e.astype(BF))
            acc = a if acc is None else acc + a
        denom = jnp.sum(total, axis=0, keepdims=True)
        o_s[pl.ds(v0, hd), :] = (acc / denom).astype(BF)

    first = scores(0, 0)

    def body(i, top0):
        h = 2 * i
        top1 = scores(h + 1, 1)
        finish(h, 0, top0)
        nxt = scores(jnp.minimum(h + 2, heads - 1), 0)
        finish(h + 1, 1, top1)
        return nxt

    lax.fori_loop(0, heads // 2, body, first)


def enc_kernel(sp, mask_ref, patches_h, enc_pos_h, dec_pos_h, w_pe_h, b_pe_ref, qkv_h, proj_h, up_h, down_h,
               hid_out, mask_all, pos_all,
               patches, enc_pos, w_pe, wqkv, wproj, wup, wdown, x_s, e_src, tail_s, win, hid, a_all, qkv_s, s_s, p_s, o_s, g_s,
               wsem, insem, ms, mr, ws, wr, es, er, asend, arecv, pfs, pfr, pns, pnr, lsem):
    me = lax.axis_index('sp')
    n_clips, rows, width = patches.shape[0], patches.shape[1], hid.shape[1]
    cap = e_src.shape[0] // n_clips
    half = tail_s.shape[0] // n_clips
    n_layers = qkv_h.shape[0]
    my_rows = hid.shape[0]
    per = sp // n_clips
    heads = 16
    hd = width // heads
    clip = me // per
    hf = lax.rem(me, 2)
    partner = me + 1 - 2 * hf
    my_half = me // per
    slot = lax.rem(me, per)

    def weight(l, i):
        src, dst = ((qkv_h, wqkv), (proj_h, wproj), (up_h, wup), (down_h, wdown))[i]
        return pltpu.make_async_copy(src.at[l], dst, wsem.at[i])

    loads = [pltpu.make_async_copy(a, b, insem.at[i]) for i, (a, b) in enumerate(
        [(patches_h, patches), (enc_pos_h, enc_pos), (w_pe_h, w_pe)])]
    for ld in loads:
        ld.start()

    barrier = pltpu.get_barrier_semaphore()
    for k in range(1, sp):
        pl.semaphore_signal(barrier, inc=1, device_id={'sp': lax.rem(me + k, sp)}, device_id_type=MESH)

    mask = mask_ref[...]
    maskf = mask.astype(F32)
    before = (lax.broadcasted_iota(jnp.int32, (rows, rows), 0) < lax.broadcasted_iota(jnp.int32, (rows, rows), 1))
    mask8 = jnp.concatenate([maskf] + [jnp.zeros_like(maskf)] * 7, axis=0).astype(BF)
    rank = mm(mask8, before.astype(BF)).astype(jnp.int32)
    row_id = lax.broadcasted_iota(jnp.int32, (cap, rows), 0)
    picks = []
    for c in range(n_clips):
        picks.append(jnp.where((row_id == rank[c:c + 1, :]) & (mask[c:c + 1, :] == 1), 1.0, 0.0))
    pick2 = jnp.concatenate(picks, axis=0)
    used = jnp.sum(pick2, axis=1, keepdims=True)
    pick2 = pick2.astype(BF)
    for ld in loads[:2]:
        ld.wait()
    for c in range(n_clips):
        x_s[c * cap:(c + 1) * cap, :] = mm(pick2[c * cap:(c + 1) * cap], patches[c]).astype(BF)
    fixed = used * b_pe_ref[...].reshape(1, width).astype(F32) + mm(pick2, enc_pos[...])
    loads[2].wait()
    weight(0, 0).start()
    e_src[...] = (mm(x_s[...], w_pe[...]) + fixed).astype(BF)
    late = lax.broadcasted_iota(jnp.int32, (half, cap), 1) - lax.broadcasted_iota(jnp.int32, (half, cap), 0) + half
    for c in range(n_clips):
        count = jnp.sum(maskf[c:c + 1, :], axis=1, keepdims=True).astype(jnp.int32)
        pick = jnp.where(late == count, 1.0, 0.0).astype(BF)
        tail_s[c * half:(c + 1) * half, :] = mm(pick, e_src[c * cap:(c + 1) * cap, :]).astype(BF)

    pl.semaphore_wait(barrier, sp - 1)

    def to(c, x, h):
        return per * c + 2 * x + h

    def send(c, x):
        return pltpu.make_async_remote_copy(
            src_ref=e_src.at[pl.ds(c * cap, cap)], dst_ref=win.at[pl.ds(pl.multiple_of(slot * cap, cap), cap)],
            send_sem=ws.at[c, x], recv_sem=wr.at[slot], device_id={'sp': to(c, x, my_half)}, device_id_type=MESH)

    last = per * cap
    edges = ((per, 0, e_src, cap), (per - 1, 1, tail_s, half))

    def send_edge(c, x, h, buf, step):
        return pltpu.make_async_remote_copy(
            src_ref=buf.at[pl.ds(c * step, half)], dst_ref=win.at[pl.ds(last, half)], send_sem=es.at[c, x], recv_sem=er,
            device_id={'sp': to(c, x, h)}, device_id_type=MESH)

    for c in range(n_clips):
        for x in range(per // 2):
            @pl.when(to(c, x, my_half) != me)
            def _():
                send(c, x).start()

            @pl.when(to(c, x, my_half) == me)
            def _():
                pltpu.make_async_copy(
                    e_src.at[pl.ds(c * cap, cap)], win.at[pl.ds(pl.multiple_of(slot * cap, cap), cap)], wr.at[slot]).start()

            for src_dev, h, buf, step in edges:
                @pl.when((me == src_dev) & (to(c, x, h) != me))
                def _():
                    send_edge(c, x, h, buf, step).start()

                @pl.when((me == src_dev) & (to(c, x, h) == me))
                def _():
                    pltpu.make_async_copy(buf.at[pl.ds(c * step, half)], win.at[pl.ds(last, half)], er).start()

    for i in range(1, 4):
        weight(0, i).start()
    mask_sends = []
    for k in range(1, sp):
        mask_sends.append(pltpu.make_async_remote_copy(
            src_ref=mask_ref, dst_ref=mask_all.at[me], send_sem=ms.at[k], recv_sem=mr.at[k],
            device_id={'sp': lax.rem(me + k, sp)}, device_id_type=MESH))
        mask_sends[-1].start()
    own_mask = pltpu.make_async_copy(mask_ref, mask_all.at[me], lsem.at[0])
    own_mask.start()
    for m in mask_sends:
        m.wait_recv()
    own_mask.wait()
    starts = [jnp.zeros((1, 1), F32)]
    for s in range(sp):
        both = mask_all[s].astype(F32)
        row = jnp.where(clip == 0, both[0:1, :], both[1:2, :])
        starts.append(starts[-1] + jnp.sum(row, axis=1, keepdims=True))
    out_row = lax.broadcasted_iota(jnp.int32, (my_rows, cap), 0) - lax.broadcasted_iota(jnp.int32, (my_rows, cap), 1)
    places = []
    for b in range(per):
        off = jnp.where(hf == 0, starts[b], starts[per + b] - my_rows).astype(jnp.int32)
        places.append(jnp.where(out_row == off, 1.0, 0.0))
    off = jnp.where(hf == 0, starts[per], starts[per] - half - my_rows).astype(jnp.int32)
    places.append(jnp.where(out_row[:, :half] == off, 1.0, 0.0))
    place_a = jnp.concatenate(places[:per], axis=1).astype(BF)
    place_b = places[per].astype(BF)

    for b in range(per):
        pltpu.make_async_copy(e_src.at[pl.ds(0, cap)], win.at[pl.ds(b * cap, cap)], wr.at[b]).wait()
    pltpu.make_async_copy(e_src.at[pl.ds(0, half)], win.at[pl.ds(last, half)], er).wait()
    hid[...] = (mm(place_a, win[:last, :]) + mm(place_b, win[last:, :])).astype(BF)

    scale = hd ** -0.5
    pos_own = pltpu.make_async_copy(dec_pos_h, pos_all.at[me], lsem.at[1])
    pos_own.start()

    def pos_far(k):
        return pltpu.make_async_remote_copy(
            src_ref=dec_pos_h, dst_ref=pos_all.at[me], send_sem=pfs.at[k], recv_sem=pfr.at[k],
            device_id={'sp': lax.rem(me + 2 * k, sp)}, device_id_type=MESH)

    def pos_near(k):
        piece = lax.rem(me + 2 * k, sp)
        return pltpu.make_async_remote_copy(
            src_ref=pos_all.at[piece], dst_ref=pos_all.at[piece], send_sem=pns.at[k], recv_sem=pnr.at[k],
            device_id={'sp': partner}, device_id_type=MESH)

    def layer(l, carry):
        def refill(i):
            @pl.when(l < n_layers - 1)
            def _():
                weight(l + 1, i).start()

        a_all[l, 0] = norm_rows(hid[...])
        swap = pltpu.make_async_remote_copy(
            src_ref=a_all.at[l, 0], dst_ref=a_all.at[l, 1], send_sem=asend.at[l], recv_sem=arecv.at[l],
            device_id={'sp': partner}, device_id_type=MESH)
        swap.start()
        weight(l, 0).wait()
        qkv_s[:width, :my_rows] = mm(wqkv[:width, :], a_all[l, 0], NT).astype(BF)
        swap.wait()
        qkv_s[width:, :] = mm(wqkv[width:, :], a_all[l].reshape(2 * my_rows, width), NT).astype(BF)
        refill(0)

        @pl.when(l == 0)
        def _():
            for k in range(1, sp // 2):
                pos_far(k).start()

        for h in range(heads):
            s_s[h] = mm(qkv_s[h * hd:(h + 1) * hd, :my_rows], qkv_s[width + h * hd:width + (h + 1) * hd, :], TN)

        def soft(i, cc):
            s = s_s[i] * scale
            e = jnp.exp(s - jnp.max(s, axis=-1, keepdims=True))
            p_s[i] = (e / jnp.sum(e, axis=-1, keepdims=True)).astype(BF)
            return cc

        lax.fori_loop(0, heads, soft, 0, unroll=4)
        for h in range(heads):
            o_s[h * hd:(h + 1) * hd, :] = mm(qkv_s[2 * width + h * hd:2 * width + (h + 1) * hd, :], p_s[h], NT).astype(BF)
        weight(l, 1).wait()
        h1 = (hid[...].astype(F32) + mm(o_s[...], wproj[...], TN)).astype(BF)
        hid[...] = h1
        refill(1)
        a2 = norm_rows(h1)
        weight(l, 2).wait()
        g_s[...] = gelu(mm(a2, wup[...])).astype(BF)
        refill(2)

        @pl.when(l == n_layers - 1)
        def _():
            pos_own.wait()
            for k in range(1, sp // 2):
                pos_far(k).wait_recv()
            for k in range(sp // 2):
                pos_near(k).start()

        weight(l, 3).wait()
        hid[...] = (hid[...].astype(F32) + mm(g_s[...], wdown[...])).astype(BF)
        refill(3)
        return carry

    lax.fori_loop(0, n_layers, layer, 0)

    hid_out[...] = hid[...]
    for m in mask_sends:
        m.wait_send()
    for c in range(n_clips):
        for x in range(per // 2):
            @pl.when(to(c, x, my_half) != me)
            def _():
                send(c, x).wait_send()

            for src_dev, h, buf, step in edges:
                @pl.when((me == src_dev) & (to(c, x, h) != me))
                def _():
                    send_edge(c, x, h, buf, step).wait_send()
    for k in range(1, sp // 2):
        pos_far(k).wait_send()
    for k in range(sp // 2):
        pos_near(k).wait()


def encode(sp, vis_mask, patches, enc_pos, dec_pos, w_pe, b_pe, qkv_t, proj, up, down):
    n_clips, rows, p_width = patches.shape
    width = w_pe.shape[1]
    d_width = dec_pos.shape[1]
    cap = 2 * rows // KEEP_DIV
    half = cap // 4
    my_rows = rows * sp // KEEP_DIV // 2
    dma = pltpu.SemaphoreType.DMA
    per = sp // n_clips
    far = sp // 2
    return pl.pallas_call(
        functools.partial(enc_kernel, sp),
        out_shape=(jax.ShapeDtypeStruct((my_rows, width), BF),
                   jax.ShapeDtypeStruct((sp, n_clips, rows), jnp.int32),
                   jax.ShapeDtypeStruct((sp, rows, d_width), BF)),
        in_specs=[VMEM, ANY, ANY, ANY, ANY, VMEM, ANY, ANY, ANY, ANY],
        out_specs=(VMEM, VMEM, ANY),
        scratch_shapes=[
            pltpu.VMEM(patches.shape, BF), pltpu.VMEM(enc_pos.shape, BF), pltpu.VMEM(w_pe.shape, BF),
            pltpu.VMEM(qkv_t.shape[1:], BF), pltpu.VMEM(proj.shape[1:], BF), pltpu.VMEM(up.shape[1:], BF), pltpu.VMEM(down.shape[1:], BF),
            pltpu.VMEM((n_clips * cap, p_width), BF), pltpu.VMEM((n_clips * cap, width), BF), pltpu.VMEM((n_clips * half, width), BF),
            pltpu.VMEM((per * cap + half, width), BF),
            pltpu.VMEM((my_rows, width), BF), pltpu.VMEM((qkv_t.shape[0], 2, my_rows, width), BF),
            pltpu.VMEM((3 * width, 2 * my_rows), BF),
            pltpu.VMEM((16, my_rows, 2 * my_rows), F32), pltpu.VMEM((16, my_rows, 2 * my_rows), BF),
            pltpu.VMEM((width, my_rows), BF), pltpu.VMEM((my_rows, 4 * width), BF),
            dma((4,)), dma((4,)), dma((sp,)), dma((sp,)), dma((n_clips, per // 2)), dma((per,)), dma((n_clips, per // 2)), dma,
            dma((2,)), dma((2,)), dma((far,)), dma((far,)), dma((far,)), dma((far,)), dma((2,)),
        ],
        compiler_params=pltpu.CompilerParams(collective_id=1, has_side_effects=True, vmem_limit_bytes=63 << 20),
        name='encode',
    )(vis_mask, patches, enc_pos, dec_pos, w_pe, b_pe, qkv_t, proj, up, down)


def decode_kernel(sp, hid_h, w_ed_h, mask_h, pos_h, tok_ref, wqkv_h, wproj_h, wup_h, wdown_h, a_out,
                  hid, w_ed, mask_all, pos, wqkv, wproj, wup, wdown, z_s, rank_s, u_s, a_own, a_all, km_s, vm_s, pv_s, k_s, vt_s, q_s, s_s, o_s,
                  insem, zs, zr, fs, fr, ns, nr):
    me = lax.axis_index('sp')
    hf = lax.rem(me, 2)
    partner = me + 1 - 2 * hf
    n_clips, n_vis, width = z_s.shape
    rows = mask_all.shape[2]
    my_rows = hid.shape[0]
    per = sp // n_clips
    clip_of = me // per
    tok = rows * sp
    heads, hd = 16, width // 16
    n_far = sp // 2

    loads = [pltpu.make_async_copy(a, b, insem.at[i]) for i, (a, b) in enumerate(
        [(hid_h, hid), (w_ed_h, w_ed), (mask_h, mask_all), (pos_h, pos), (wqkv_h, wqkv), (wproj_h, wproj), (wup_h, wup), (wdown_h, wdown)])]
    for ld in loads:
        ld.start()
    barrier = pltpu.get_barrier_semaphore()
    for k in range(1, sp):
        pl.semaphore_signal(barrier, inc=1, device_id={'sp': lax.rem(me + k, sp)}, device_id_type=MESH)

    at = pl.multiple_of(hf * my_rows, my_rows)
    mine = z_s.at[clip_of, pl.ds(at, my_rows), :]
    theirs = z_s.at[n_clips - 1 - clip_of, pl.ds(at, my_rows), :]
    for ld in loads[:2]:
        ld.wait()
    z_s[clip_of, pl.ds(at, my_rows), :] = mm(norm_rows(hid[...]), w_ed[...]).astype(BF)
    pl.semaphore_wait(barrier, sp - 1)

    def z_send(i, ref, dst):
        return pltpu.make_async_remote_copy(
            src_ref=ref, dst_ref=ref, send_sem=zs.at[i], recv_sem=zr.at[i], device_id={'sp': dst}, device_id_type=MESH)

    across = z_send(0, mine, lax.rem(me + per, sp))
    beside = z_send(1, mine, partner)
    relayed = z_send(2, theirs, partner)
    across.start()
    beside.start()

    before = (lax.broadcasted_iota(jnp.int32, (rows, rows), 0) < lax.broadcasted_iota(jnp.int32, (rows, rows), 1)).astype(BF)
    row_id = lax.broadcasted_iota(jnp.int32, (n_vis, rows), 0)
    loads[2].wait()
    for c in range(n_clips):
        m = mask_all[:, c, :]
        local = mm(m.astype(F32).astype(BF), before)
        base = jnp.zeros((1, 1), F32)
        for s in range(sp):
            vis = m[s:s + 1, :]
            rank_s[c, s:s + 1, :] = jnp.where(vis == 1, (local[s:s + 1, :] + base).astype(jnp.int32), n_vis)
            base = base + jnp.sum(vis.astype(F32), axis=1, keepdims=True)
    for ld in loads[3:5]:
        ld.wait()

    def pick_of(c, b):
        return jnp.where(row_id == rank_s[c, pl.ds(b, 1), :], 1.0, 0.0).astype(BF)

    def keys_values(l, b, blk, k_to, vt_to):
        here = pl.ds(pl.multiple_of(b * rows, rows), rows)
        k_to[here, :] = mm(blk, wqkv[l, width:2 * width, :], NT).astype(BF)
        vt_to[:, here] = mm(wqkv[l, 2 * width:, :], blk, NT).astype(BF)

    token = tok_ref[...].reshape(1, width).astype(F32)
    pv_s[...] = jnp.zeros_like(pv_s)

    def plain(b, cc):
        keys_values(0, b, norm_rows((token + pos[b].astype(F32)).astype(BF)), km_s, vm_s)
        for c in range(n_clips):
            pv_s[c] += mm(pick_of(c, b), pos[b])
        return cc

    lax.fori_loop(0, sp, plain, 0, unroll=4)

    def far(c, k):
        return pltpu.make_async_remote_copy(
            src_ref=a_own.at[c], dst_ref=a_all.at[c, me], send_sem=fs.at[c, k], recv_sem=fr.at[c, k],
            device_id={'sp': lax.rem(me + 2 * k, sp)}, device_id_type=MESH)

    def near(c, k):
        piece = lax.rem(me + 2 * k, sp)
        return pltpu.make_async_remote_copy(
            src_ref=a_all.at[c, piece] if k else a_own.at[c], dst_ref=a_all.at[c, piece],
            send_sem=ns.at[c, k], recv_sem=nr.at[c, k], device_id={'sp': partner}, device_id_type=MESH)

    def relay(c):
        for k in range(1, n_far):
            far(c, k).wait_recv()
        for k in range(n_far):
            near(c, k).start()

    def attend(l, c):
        q_s[...] = mm(wqkv[l, :width, :], a_own[c], NT).astype(BF)
        attend_clip(tok, rows, heads, hd, k_s, vt_s, q_s, s_s, o_s)

    def feed(l, c):
        h1 = (u_s[c].astype(F32) + mm(o_s[...], wproj[l], TN)).astype(BF)
        g = gelu(mm(norm_rows(h1), wup[l])).astype(BF)
        return (h1.astype(F32) + mm(g, wdown[l])).astype(BF)

    across.wait_recv()
    relayed.start()
    beside.wait_recv()
    relayed.wait_recv()

    def first(c, carry):
        u_vis = (z_s[c].astype(F32) + pv_s[c]).astype(BF)
        a_vis = norm_rows(u_vis)
        k_vis = mm(a_vis, wqkv[0, width:2 * width, :], NT).astype(BF)
        vt_vis = mm(wqkv[0, 2 * width:, :], a_vis, NT).astype(BF)
        k_aug = jnp.concatenate([k_vis, jnp.ones((n_vis, 128), BF)], axis=1)
        u_aug = jnp.concatenate([u_vis, jnp.ones((n_vis, 128), BF)], axis=1)

        def put(pick, aug, plain_rows):
            got = mm(pick, aug, TN)
            seen = jnp.concatenate([got[:, width:]] * (width // 128), axis=1)
            return jnp.where(seen > 0.5, got[:, :width], plain_rows.astype(F32)).astype(BF)

        def block(b, cc):
            here = pl.ds(pl.multiple_of(b * rows, rows), rows)
            pick = pick_of(c, b)
            k_s[here, :] = put(pick, k_aug, km_s[here, :])
            seen = rank_s[c, pl.ds(b, 1), :] < n_vis
            vt_s[:, here] = jnp.where(seen, mm(vt_vis, pick), vm_s[:, here].astype(F32)).astype(BF)
            return cc

        lax.fori_loop(0, sp, block, 0, unroll=8)
        u = put(pick_of(c, me), u_aug, (token + pos[me].astype(F32)).astype(BF))
        u_s[c] = u
        a_own[c] = norm_rows(u)
        attend(0, c)

        @pl.when(c == 0)
        def _():
            for ld in loads[5:]:
                ld.wait()

        @pl.when(c == 1)
        def _():
            relay(0)

        u1 = feed(0, c)
        u_s[c] = u1
        a_own[c] = norm_rows(u1)
        for k in range(1, n_far):
            far(c, k).start()
        return carry

    lax.fori_loop(0, n_clips, first, 0)

    def second(c, carry):
        keys_values(1, me, a_own[c], k_s, vt_s)

        def same(k, cc):
            b = lax.rem(me + 2 * k, sp)
            keys_values(1, b, a_all[c, b], k_s, vt_s)
            return cc

        def other(k, cc):
            b = lax.rem(partner + 2 * k, sp)
            keys_values(1, b, a_all[c, b], k_s, vt_s)
            return cc

        lax.fori_loop(1, n_far, same, 0, unroll=True)
        for k in range(n_far):
            near(c, k).wait_recv()
        lax.fori_loop(0, n_far, other, 0, unroll=True)
        attend(1, c)

        @pl.when(c == 0)
        def _():
            relay(1)

        a_out[c] = norm_rows(feed(1, c))
        return carry

    lax.fori_loop(0, n_clips, second, 0)
    for c in range(n_clips):
        for k in range(n_far):
            near(c, k).wait_send()
            if k:
                far(c, k).wait_send()
    across.wait_send()
    beside.wait_send()
    relayed.wait_send()


def decode(sp, hid, w_ed, mask_all, pos_all, mask_token, wqkv, wproj, wup, wdown):
    _, n_clips, rows = mask_all.shape
    width = w_ed.shape[1]
    tok = rows * sp
    n_vis = tok // KEEP_DIV
    dma = pltpu.SemaphoreType.DMA
    return pl.pallas_call(
        functools.partial(decode_kernel, sp),
        out_shape=jax.ShapeDtypeStruct((n_clips, rows, width), BF),
        in_specs=[ANY, ANY, ANY, ANY, VMEM, ANY, ANY, ANY, ANY],
        out_specs=VMEM,
        scratch_shapes=[
            pltpu.VMEM(hid.shape, BF), pltpu.VMEM(w_ed.shape, BF), pltpu.VMEM(mask_all.shape, jnp.int32),
            pltpu.VMEM(pos_all.shape, BF), pltpu.VMEM(wqkv.shape, BF), pltpu.VMEM(wproj.shape, BF),
            pltpu.VMEM(wup.shape, BF), pltpu.VMEM(wdown.shape, BF),
            pltpu.VMEM((n_clips, n_vis, width), BF),
            pltpu.VMEM((n_clips, sp, rows), jnp.int32), pltpu.VMEM((n_clips, rows, width), BF), pltpu.VMEM((n_clips, rows, width), BF),
            pltpu.VMEM((n_clips, sp, rows, width), BF),
            pltpu.VMEM((tok, width), BF), pltpu.VMEM((width, tok), BF), pltpu.VMEM((n_clips, n_vis, width), F32),
            pltpu.VMEM((tok, width), BF), pltpu.VMEM((width, tok), BF), pltpu.VMEM((width, rows), BF),
            pltpu.VMEM((2, tok, rows), F32), pltpu.VMEM((width, rows), BF),
            dma((8,)), dma((3,)), dma((3,)), dma((n_clips, sp // 2)), dma((n_clips, sp // 2)), dma((n_clips, sp // 2)), dma((n_clips, sp // 2)),
        ],
        compiler_params=pltpu.CompilerParams(collective_id=2, has_side_effects=True, vmem_limit_bytes=56 << 20),
        name='decode',
    )(hid, w_ed, mask_all, pos_all, mask_token, wqkv, wproj, wup, wdown)


def solution(mesh):
    sp = mesh.shape['sp']

    def local_program(patches, vis_mask, enc_pos, dec_pos, w_pe, b_pe, enc_qkv, enc_proj, enc_up, enc_down, w_ed, mask_token, dec_qkv, dec_proj, dec_up, dec_down, w_out):
        n_layers, width = enc_qkv.shape[:2]
        d_width = dec_qkv.shape[1]
        enc_qkv_t = jnp.transpose(enc_qkv, (0, 2, 3, 4, 1)).reshape(n_layers, 3 * width, width)
        dec_qkv_t = jnp.transpose(dec_qkv, (0, 2, 3, 4, 1)).reshape(n_layers, 3 * d_width, d_width)
        hid, mask_all, pos_all = encode(sp, vis_mask, patches, enc_pos, dec_pos, w_pe, b_pe, enc_qkv_t,
                                          enc_proj.reshape(n_layers, width, width), enc_up, enc_down)
        acts = decode(sp, hid, w_ed, mask_all, pos_all, mask_token, dec_qkv_t,
                      dec_proj.reshape(n_layers, d_width, d_width), dec_up, dec_down)
        return jnp.einsum('cne,ep->cnp', acts, w_out, preferred_element_type=F32)

    row_spec = P('dp', 'sp', None)
    pos_spec = P(('dp', 'sp'), None)
    arg_specs = (row_spec, P('dp', 'sp'), pos_spec, pos_spec) + (P(),) * 13
    return jax.shard_map(local_program, mesh=mesh, in_specs=arg_specs, out_specs=row_spec, check_vma=False)
```

```python
import functools

import jax
import jax.numpy as jnp
from jax import lax
from jax.experimental import pallas as pl
from jax.experimental.pallas import tpu as pltpu
from jax.sharding import PartitionSpec as P

KEEP_DIV = 8
HEADS_PER_STEP = 8


BF = jnp.bfloat16
F32 = jnp.float32
NT = (((1,), (1,)), ((), ()))
TN = (((0,), (0,)), ((), ()))
NN = (((1,), (0,)), ((), ()))
LOG2E = 1.4426950408889634
MESH = pl.DeviceIdType.MESH
VMEM = pl.BlockSpec(memory_space=pltpu.VMEM)
ANY = pl.BlockSpec(memory_space=pl.ANY)


def mm(lhs, rhs, dims=NN):
    return lax.dot_general(lhs, rhs, dims, preferred_element_type=F32)


def norm_rows(hidden):
    wide = hidden.astype(F32)
    centred = wide - jnp.mean(wide, axis=-1, keepdims=True)
    var = jnp.mean(centred * centred, axis=-1, keepdims=True)
    return (centred * lax.rsqrt(var + 1e-6)).astype(BF)


def gelu(x):
    return 0.5 * x * (1.0 + lax.erf(x * 0.7071067811865476))


def attend_clip(tok, rows, heads, hd, k_s, vt_s, q_s, s_s, o_s):
    c2 = hd ** -0.5 * LOG2E
    group = 256 // hd
    chunk = 256
    n_chunks = tok // chunk

    def q_of(h):
        g = h // group
        qg = q_s[pl.ds(pl.multiple_of(g * 256, 256), 256), :]
        row_head = lax.broadcasted_iota(jnp.int32, (256, rows), 0) // hd
        return jnp.where(row_head == h - g * group, qg, jnp.zeros_like(qg)), pl.multiple_of(g * 256, 256)

    def turn(nxt, nxt_slot, h, slot, top):
        qz, g0 = q_of(nxt)
        next_top = total = acc = None
        if h is not None:
            m = jnp.max(top, axis=0, keepdims=True) * c2
            v0 = pl.multiple_of(h * hd, hd)
        for j in range(n_chunks):
            at = slice(j * chunk, (j + 1) * chunk)
            s = mm(k_s[at, pl.ds(g0, 256)], qz)
            s_s[nxt_slot, at, :] = s
            t = jnp.max(s.reshape(chunk // 8, 8, rows), axis=0)
            next_top = t if next_top is None else jnp.maximum(next_top, t)
            if h is not None:
                e = jnp.exp2(s_s[slot, at, :] * c2 - m)
                t = jnp.sum(e.reshape(chunk // 8, 8, rows), axis=0)
                total = t if total is None else total + t
                a = mm(vt_s[pl.ds(v0, hd), at], e.astype(BF))
                acc = a if acc is None else acc + a
        if h is not None:
            o_s[pl.ds(v0, hd), :] = (acc / jnp.sum(total, axis=0, keepdims=True)).astype(BF)
        return next_top

    def body(i, top):
        for u in range(HEADS_PER_STEP):
            h = HEADS_PER_STEP * i + u
            top = turn(jnp.minimum(h + 1, heads - 1), (u + 1) % 2, h, u % 2, top)
        return top

    lax.fori_loop(0, heads // HEADS_PER_STEP, body, turn(0, 0, None, None, None))


def enc_kernel(sp, mask_ref, patches_h, enc_pos_h, dec_pos_h, w_pe_h, b_pe_ref, qkv_h, proj_h, up_h, down_h,
               hid_out, mask_all, pos_all,
               patches, enc_pos, w_pe, wqkv, wproj, wup, wdown, x_s, e_src, tail_s, win, hid, a_all, qkv_s, s_s, p_s, o_s, g_s,
               wsem, insem, ms, mr, ws, wr, es, er, asend, arecv, pfs, pfr, pns, pnr, lsem):
    me = lax.axis_index('sp')
    n_clips, rows, width = patches.shape[0], patches.shape[1], hid.shape[1]
    cap = e_src.shape[0] // n_clips
    half = tail_s.shape[0] // n_clips
    n_layers = qkv_h.shape[0]
    my_rows = hid.shape[0]
    per = sp // n_clips
    heads = 16
    hd = width // heads
    clip = me // per
    hf = lax.rem(me, 2)
    partner = me + 1 - 2 * hf
    my_half = me // per
    slot = lax.rem(me, per)

    def weight(l, i):
        src, dst = ((qkv_h, wqkv), (proj_h, wproj), (up_h, wup), (down_h, wdown))[i]
        return pltpu.make_async_copy(src.at[l], dst, wsem.at[i])

    loads = [pltpu.make_async_copy(a, b, insem.at[i]) for i, (a, b) in enumerate(
        [(patches_h, patches), (enc_pos_h, enc_pos), (w_pe_h, w_pe)])]
    for ld in loads:
        ld.start()

    barrier = pltpu.get_barrier_semaphore()
    for k in range(1, sp):
        pl.semaphore_signal(barrier, inc=1, device_id={'sp': lax.rem(me + k, sp)}, device_id_type=MESH)

    mask = mask_ref[...]
    maskf = mask.astype(F32)
    before = (lax.broadcasted_iota(jnp.int32, (rows, rows), 0) < lax.broadcasted_iota(jnp.int32, (rows, rows), 1))
    mask8 = jnp.concatenate([maskf] + [jnp.zeros_like(maskf)] * 7, axis=0).astype(BF)
    rank = mm(mask8, before.astype(BF)).astype(jnp.int32)
    row_id = lax.broadcasted_iota(jnp.int32, (cap, rows), 0)
    picks = []
    for c in range(n_clips):
        picks.append(jnp.where((row_id == rank[c:c + 1, :]) & (mask[c:c + 1, :] == 1), 1.0, 0.0))
    pick2 = jnp.concatenate(picks, axis=0)
    used = jnp.sum(pick2, axis=1, keepdims=True)
    pick2 = pick2.astype(BF)
    for ld in loads[:2]:
        ld.wait()
    for c in range(n_clips):
        x_s[c * cap:(c + 1) * cap, :] = mm(pick2[c * cap:(c + 1) * cap], patches[c]).astype(BF)
    fixed = used * b_pe_ref[...].reshape(1, width).astype(F32) + mm(pick2, enc_pos[...])
    loads[2].wait()
    weight(0, 0).start()
    e_src[...] = (mm(x_s[...], w_pe[...]) + fixed).astype(BF)
    late = lax.broadcasted_iota(jnp.int32, (half, cap), 1) - lax.broadcasted_iota(jnp.int32, (half, cap), 0) + half
    for c in range(n_clips):
        count = jnp.sum(maskf[c:c + 1, :], axis=1, keepdims=True).astype(jnp.int32)
        pick = jnp.where(late == count, 1.0, 0.0).astype(BF)
        tail_s[c * half:(c + 1) * half, :] = mm(pick, e_src[c * cap:(c + 1) * cap, :]).astype(BF)

    pl.semaphore_wait(barrier, sp - 1)

    def to(c, x, h):
        return per * c + 2 * x + h

    def send(c, x):
        return pltpu.make_async_remote_copy(
            src_ref=e_src.at[pl.ds(c * cap, cap)], dst_ref=win.at[pl.ds(pl.multiple_of(slot * cap, cap), cap)],
            send_sem=ws.at[c, x], recv_sem=wr.at[slot], device_id={'sp': to(c, x, my_half)}, device_id_type=MESH)

    last = per * cap
    edges = ((per, 0, e_src, cap), (per - 1, 1, tail_s, half))

    def send_edge(c, x, h, buf, step):
        return pltpu.make_async_remote_copy(
            src_ref=buf.at[pl.ds(c * step, half)], dst_ref=win.at[pl.ds(last, half)], send_sem=es.at[c, x], recv_sem=er,
            device_id={'sp': to(c, x, h)}, device_id_type=MESH)

    for c in range(n_clips):
        for x in range(per // 2):
            @pl.when(to(c, x, my_half) != me)
            def _():
                send(c, x).start()

            @pl.when(to(c, x, my_half) == me)
            def _():
                pltpu.make_async_copy(
                    e_src.at[pl.ds(c * cap, cap)], win.at[pl.ds(pl.multiple_of(slot * cap, cap), cap)], wr.at[slot]).start()

            for src_dev, h, buf, step in edges:
                @pl.when((me == src_dev) & (to(c, x, h) != me))
                def _():
                    send_edge(c, x, h, buf, step).start()

                @pl.when((me == src_dev) & (to(c, x, h) == me))
                def _():
                    pltpu.make_async_copy(buf.at[pl.ds(c * step, half)], win.at[pl.ds(last, half)], er).start()

    for i in range(1, 4):
        weight(0, i).start()
    mask_sends = []
    for k in range(1, sp):
        mask_sends.append(pltpu.make_async_remote_copy(
            src_ref=mask_ref, dst_ref=mask_all.at[me], send_sem=ms.at[k], recv_sem=mr.at[k],
            device_id={'sp': lax.rem(me + k, sp)}, device_id_type=MESH))
        mask_sends[-1].start()
    own_mask = pltpu.make_async_copy(mask_ref, mask_all.at[me], lsem.at[0])
    own_mask.start()
    for m in mask_sends:
        m.wait_recv()
    own_mask.wait()
    starts = [jnp.zeros((1, 1), F32)]
    for s in range(sp):
        both = mask_all[s].astype(F32)
        row = jnp.where(clip == 0, both[0:1, :], both[1:2, :])
        starts.append(starts[-1] + jnp.sum(row, axis=1, keepdims=True))
    out_row = lax.broadcasted_iota(jnp.int32, (my_rows, cap), 0) - lax.broadcasted_iota(jnp.int32, (my_rows, cap), 1)
    places = []
    for b in range(per):
        off = jnp.where(hf == 0, starts[b], starts[per + b] - my_rows).astype(jnp.int32)
        places.append(jnp.where(out_row == off, 1.0, 0.0))
    off = jnp.where(hf == 0, starts[per], starts[per] - half - my_rows).astype(jnp.int32)
    places.append(jnp.where(out_row[:, :half] == off, 1.0, 0.0))
    place_a = jnp.concatenate(places[:per], axis=1).astype(BF)
    place_b = places[per].astype(BF)

    for b in range(per):
        pltpu.make_async_copy(e_src.at[pl.ds(0, cap)], win.at[pl.ds(b * cap, cap)], wr.at[b]).wait()
    pltpu.make_async_copy(e_src.at[pl.ds(0, half)], win.at[pl.ds(last, half)], er).wait()
    hid[...] = (mm(place_a, win[:last, :]) + mm(place_b, win[last:, :])).astype(BF)

    scale = hd ** -0.5
    pos_own = pltpu.make_async_copy(dec_pos_h, pos_all.at[me], lsem.at[1])
    pos_own.start()

    def pos_far(k):
        return pltpu.make_async_remote_copy(
            src_ref=dec_pos_h, dst_ref=pos_all.at[me], send_sem=pfs.at[k], recv_sem=pfr.at[k],
            device_id={'sp': lax.rem(me + 2 * k, sp)}, device_id_type=MESH)

    def pos_near(k):
        piece = lax.rem(me + 2 * k, sp)
        return pltpu.make_async_remote_copy(
            src_ref=pos_all.at[piece], dst_ref=pos_all.at[piece], send_sem=pns.at[k], recv_sem=pnr.at[k],
            device_id={'sp': partner}, device_id_type=MESH)

    def layer(l, carry):
        def refill(i):
            @pl.when(l < n_layers - 1)
            def _():
                weight(l + 1, i).start()

        a_all[l, 0] = norm_rows(hid[...])
        swap = pltpu.make_async_remote_copy(
            src_ref=a_all.at[l, 0], dst_ref=a_all.at[l, 1], send_sem=asend.at[l], recv_sem=arecv.at[l],
            device_id={'sp': partner}, device_id_type=MESH)
        swap.start()
        weight(l, 0).wait()
        qkv_s[:width, :my_rows] = mm(wqkv[:width, :], a_all[l, 0], NT).astype(BF)
        swap.wait()
        qkv_s[width:, :] = mm(wqkv[width:, :], a_all[l].reshape(2 * my_rows, width), NT).astype(BF)
        refill(0)

        @pl.when(l == 0)
        def _():
            for k in range(1, sp // 2):
                pos_far(k).start()

        for h in range(heads):
            s_s[h] = mm(qkv_s[h * hd:(h + 1) * hd, :my_rows], qkv_s[width + h * hd:width + (h + 1) * hd, :], TN)

        def soft(i, cc):
            s = s_s[i] * scale
            e = jnp.exp(s - jnp.max(s, axis=-1, keepdims=True))
            p_s[i] = (e / jnp.sum(e, axis=-1, keepdims=True)).astype(BF)
            return cc

        lax.fori_loop(0, heads, soft, 0, unroll=4)
        for h in range(heads):
            o_s[h * hd:(h + 1) * hd, :] = mm(qkv_s[2 * width + h * hd:2 * width + (h + 1) * hd, :], p_s[h], NT).astype(BF)
        weight(l, 1).wait()
        h1 = (hid[...].astype(F32) + mm(o_s[...], wproj[...], TN)).astype(BF)
        hid[...] = h1
        refill(1)
        a2 = norm_rows(h1)
        weight(l, 2).wait()
        g_s[...] = gelu(mm(a2, wup[...])).astype(BF)
        refill(2)

        @pl.when(l == n_layers - 1)
        def _():
            pos_own.wait()
            for k in range(1, sp // 2):
                pos_far(k).wait_recv()
            for k in range(sp // 2):
                pos_near(k).start()

        weight(l, 3).wait()
        hid[...] = (hid[...].astype(F32) + mm(g_s[...], wdown[...])).astype(BF)
        refill(3)
        return carry

    lax.fori_loop(0, n_layers, layer, 0)

    hid_out[...] = hid[...]
    for m in mask_sends:
        m.wait_send()
    for c in range(n_clips):
        for x in range(per // 2):
            @pl.when(to(c, x, my_half) != me)
            def _():
                send(c, x).wait_send()

            for src_dev, h, buf, step in edges:
                @pl.when((me == src_dev) & (to(c, x, h) != me))
                def _():
                    send_edge(c, x, h, buf, step).wait_send()
    for k in range(1, sp // 2):
        pos_far(k).wait_send()
    for k in range(sp // 2):
        pos_near(k).wait()


def encode(sp, vis_mask, patches, enc_pos, dec_pos, w_pe, b_pe, qkv_t, proj, up, down):
    n_clips, rows, p_width = patches.shape
    width = w_pe.shape[1]
    d_width = dec_pos.shape[1]
    cap = 2 * rows // KEEP_DIV
    half = cap // 4
    my_rows = rows * sp // KEEP_DIV // 2
    dma = pltpu.SemaphoreType.DMA
    per = sp // n_clips
    far = sp // 2
    return pl.pallas_call(
        functools.partial(enc_kernel, sp),
        out_shape=(jax.ShapeDtypeStruct((my_rows, width), BF),
                   jax.ShapeDtypeStruct((sp, n_clips, rows), jnp.int32),
                   jax.ShapeDtypeStruct((sp, rows, d_width), BF)),
        in_specs=[VMEM, ANY, ANY, ANY, ANY, VMEM, ANY, ANY, ANY, ANY],
        out_specs=(VMEM, VMEM, ANY),
        scratch_shapes=[
            pltpu.VMEM(patches.shape, BF), pltpu.VMEM(enc_pos.shape, BF), pltpu.VMEM(w_pe.shape, BF),
            pltpu.VMEM(qkv_t.shape[1:], BF), pltpu.VMEM(proj.shape[1:], BF), pltpu.VMEM(up.shape[1:], BF), pltpu.VMEM(down.shape[1:], BF),
            pltpu.VMEM((n_clips * cap, p_width), BF), pltpu.VMEM((n_clips * cap, width), BF), pltpu.VMEM((n_clips * half, width), BF),
            pltpu.VMEM((per * cap + half, width), BF),
            pltpu.VMEM((my_rows, width), BF), pltpu.VMEM((qkv_t.shape[0], 2, my_rows, width), BF),
            pltpu.VMEM((3 * width, 2 * my_rows), BF),
            pltpu.VMEM((16, my_rows, 2 * my_rows), F32), pltpu.VMEM((16, my_rows, 2 * my_rows), BF),
            pltpu.VMEM((width, my_rows), BF), pltpu.VMEM((my_rows, 4 * width), BF),
            dma((4,)), dma((4,)), dma((sp,)), dma((sp,)), dma((n_clips, per // 2)), dma((per,)), dma((n_clips, per // 2)), dma,
            dma((2,)), dma((2,)), dma((far,)), dma((far,)), dma((far,)), dma((far,)), dma((2,)),
        ],
        compiler_params=pltpu.CompilerParams(collective_id=1, has_side_effects=True, vmem_limit_bytes=63 << 20),
        name='encode',
    )(vis_mask, patches, enc_pos, dec_pos, w_pe, b_pe, qkv_t, proj, up, down)


def decode_kernel(sp, hid_h, w_ed_h, mask_h, pos_h, tok_ref, wqkv_h, wproj_h, wup_h, wdown_h, a_out,
                  hid, w_ed, mask_all, pos, wqkv, wproj, wup, wdown, z_s, rank_s, u_s, a_own, a_all, km_s, vm_s, pv_s, k_s, vt_s, q_s, s_s, o_s,
                  insem, zs, zr, fs, fr, ns, nr):
    me = lax.axis_index('sp')
    hf = lax.rem(me, 2)
    partner = me + 1 - 2 * hf
    n_clips, n_vis, width = z_s.shape
    rows = mask_all.shape[2]
    my_rows = hid.shape[0]
    per = sp // n_clips
    clip_of = me // per
    tok = rows * sp
    heads, hd = 16, width // 16
    n_far = sp // 2

    loads = [pltpu.make_async_copy(a, b, insem.at[i]) for i, (a, b) in enumerate(
        [(hid_h, hid), (w_ed_h, w_ed), (mask_h, mask_all), (pos_h, pos), (wqkv_h, wqkv), (wproj_h, wproj), (wup_h, wup), (wdown_h, wdown)])]
    for ld in loads:
        ld.start()
    barrier = pltpu.get_barrier_semaphore()
    for k in range(1, sp):
        pl.semaphore_signal(barrier, inc=1, device_id={'sp': lax.rem(me + k, sp)}, device_id_type=MESH)

    at = pl.multiple_of(hf * my_rows, my_rows)
    mine = z_s.at[clip_of, pl.ds(at, my_rows), :]
    theirs = z_s.at[n_clips - 1 - clip_of, pl.ds(at, my_rows), :]
    for ld in loads[:2]:
        ld.wait()
    z_s[clip_of, pl.ds(at, my_rows), :] = mm(norm_rows(hid[...]), w_ed[...]).astype(BF)
    pl.semaphore_wait(barrier, sp - 1)

    def z_send(i, ref, dst):
        return pltpu.make_async_remote_copy(
            src_ref=ref, dst_ref=ref, send_sem=zs.at[i], recv_sem=zr.at[i], device_id={'sp': dst}, device_id_type=MESH)

    across = z_send(0, mine, lax.rem(me + per, sp))
    beside = z_send(1, mine, partner)
    relayed = z_send(2, theirs, partner)
    across.start()
    beside.start()

    before = (lax.broadcasted_iota(jnp.int32, (rows, rows), 0) < lax.broadcasted_iota(jnp.int32, (rows, rows), 1)).astype(BF)
    row_id = lax.broadcasted_iota(jnp.int32, (n_vis, rows), 0)
    loads[2].wait()
    for c in range(n_clips):
        m = mask_all[:, c, :]
        local = mm(m.astype(F32).astype(BF), before)
        base = jnp.zeros((1, 1), F32)
        for s in range(sp):
            vis = m[s:s + 1, :]
            rank_s[c, s:s + 1, :] = jnp.where(vis == 1, (local[s:s + 1, :] + base).astype(jnp.int32), n_vis)
            base = base + jnp.sum(vis.astype(F32), axis=1, keepdims=True)
    for ld in loads[3:5]:
        ld.wait()

    def pick_of(c, b):
        return jnp.where(row_id == rank_s[c, pl.ds(b, 1), :], 1.0, 0.0).astype(BF)

    def keys_values(l, b, blk, k_to, vt_to):
        here = pl.ds(pl.multiple_of(b * rows, rows), rows)
        k_to[here, :] = mm(blk, wqkv[l, width:2 * width, :], NT).astype(BF)
        vt_to[:, here] = mm(wqkv[l, 2 * width:, :], blk, NT).astype(BF)

    token = tok_ref[...].reshape(1, width).astype(F32)
    pv_s[...] = jnp.zeros_like(pv_s)

    def plain(b, cc):
        keys_values(0, b, norm_rows((token + pos[b].astype(F32)).astype(BF)), km_s, vm_s)
        for c in range(n_clips):
            pv_s[c] += mm(pick_of(c, b), pos[b])
        return cc

    lax.fori_loop(0, sp, plain, 0, unroll=4)

    def far(c, k):
        return pltpu.make_async_remote_copy(
            src_ref=a_own.at[c], dst_ref=a_all.at[c, me], send_sem=fs.at[c, k], recv_sem=fr.at[c, k],
            device_id={'sp': lax.rem(me + 2 * k, sp)}, device_id_type=MESH)

    def near(c, k):
        piece = lax.rem(me + 2 * k, sp)
        return pltpu.make_async_remote_copy(
            src_ref=a_all.at[c, piece] if k else a_own.at[c], dst_ref=a_all.at[c, piece],
            send_sem=ns.at[c, k], recv_sem=nr.at[c, k], device_id={'sp': partner}, device_id_type=MESH)

    def relay(c):
        for k in range(1, n_far):
            far(c, k).wait_recv()
        for k in range(n_far):
            near(c, k).start()

    def attend(l, c):
        q_s[...] = mm(wqkv[l, :width, :], a_own[c], NT).astype(BF)
        attend_clip(tok, rows, heads, hd, k_s, vt_s, q_s, s_s, o_s)

    def feed(l, c):
        h1 = (u_s[c].astype(F32) + mm(o_s[...], wproj[l], TN)).astype(BF)
        g = gelu(mm(norm_rows(h1), wup[l])).astype(BF)
        return (h1.astype(F32) + mm(g, wdown[l])).astype(BF)

    across.wait_recv()
    relayed.start()
    beside.wait_recv()
    relayed.wait_recv()

    def first(c, carry):
        u_vis = (z_s[c].astype(F32) + pv_s[c]).astype(BF)
        a_vis = norm_rows(u_vis)
        k_vis = mm(a_vis, wqkv[0, width:2 * width, :], NT).astype(BF)
        vt_vis = mm(wqkv[0, 2 * width:, :], a_vis, NT).astype(BF)
        k_aug = jnp.concatenate([k_vis, jnp.ones((n_vis, 128), BF)], axis=1)
        u_aug = jnp.concatenate([u_vis, jnp.ones((n_vis, 128), BF)], axis=1)

        def put(pick, aug, plain_rows):
            got = mm(pick, aug, TN)
            seen = jnp.concatenate([got[:, width:]] * (width // 128), axis=1)
            return jnp.where(seen > 0.5, got[:, :width], plain_rows.astype(F32)).astype(BF)

        def block(b, cc):
            here = pl.ds(pl.multiple_of(b * rows, rows), rows)
            pick = pick_of(c, b)
            k_s[here, :] = put(pick, k_aug, km_s[here, :])
            seen = rank_s[c, pl.ds(b, 1), :] < n_vis
            vt_s[:, here] = jnp.where(seen, mm(vt_vis, pick), vm_s[:, here].astype(F32)).astype(BF)
            return cc

        lax.fori_loop(0, sp, block, 0, unroll=8)
        u = put(pick_of(c, me), u_aug, (token + pos[me].astype(F32)).astype(BF))
        u_s[c] = u
        a_own[c] = norm_rows(u)
        attend(0, c)

        @pl.when(c == 0)
        def _():
            for ld in loads[5:]:
                ld.wait()

        @pl.when(c == 1)
        def _():
            relay(0)

        u1 = feed(0, c)
        u_s[c] = u1
        a_own[c] = norm_rows(u1)
        for k in range(1, n_far):
            far(c, k).start()
        return carry

    lax.fori_loop(0, n_clips, first, 0)

    def second(c, carry):
        keys_values(1, me, a_own[c], k_s, vt_s)

        def same(k, cc):
            b = lax.rem(me + 2 * k, sp)
            keys_values(1, b, a_all[c, b], k_s, vt_s)
            return cc

        def other(k, cc):
            b = lax.rem(partner + 2 * k, sp)
            keys_values(1, b, a_all[c, b], k_s, vt_s)
            return cc

        lax.fori_loop(1, n_far, same, 0, unroll=True)
        for k in range(n_far):
            near(c, k).wait_recv()
        lax.fori_loop(0, n_far, other, 0, unroll=True)
        attend(1, c)

        @pl.when(c == 0)
        def _():
            relay(1)

        a_out[c] = norm_rows(feed(1, c))
        return carry

    lax.fori_loop(0, n_clips, second, 0)
    for c in range(n_clips):
        for k in range(n_far):
            near(c, k).wait_send()
            if k:
                far(c, k).wait_send()
    across.wait_send()
    beside.wait_send()
    relayed.wait_send()


def decode(sp, hid, w_ed, mask_all, pos_all, mask_token, wqkv, wproj, wup, wdown):
    _, n_clips, rows = mask_all.shape
    width = w_ed.shape[1]
    tok = rows * sp
    n_vis = tok // KEEP_DIV
    dma = pltpu.SemaphoreType.DMA
    return pl.pallas_call(
        functools.partial(decode_kernel, sp),
        out_shape=jax.ShapeDtypeStruct((n_clips, rows, width), BF),
        in_specs=[ANY, ANY, ANY, ANY, VMEM, ANY, ANY, ANY, ANY],
        out_specs=VMEM,
        scratch_shapes=[
            pltpu.VMEM(hid.shape, BF), pltpu.VMEM(w_ed.shape, BF), pltpu.VMEM(mask_all.shape, jnp.int32),
            pltpu.VMEM(pos_all.shape, BF), pltpu.VMEM(wqkv.shape, BF), pltpu.VMEM(wproj.shape, BF),
            pltpu.VMEM(wup.shape, BF), pltpu.VMEM(wdown.shape, BF),
            pltpu.VMEM((n_clips, n_vis, width), BF),
            pltpu.VMEM((n_clips, sp, rows), jnp.int32), pltpu.VMEM((n_clips, rows, width), BF), pltpu.VMEM((n_clips, rows, width), BF),
            pltpu.VMEM((n_clips, sp, rows, width), BF),
            pltpu.VMEM((tok, width), BF), pltpu.VMEM((width, tok), BF), pltpu.VMEM((n_clips, n_vis, width), F32),
            pltpu.VMEM((tok, width), BF), pltpu.VMEM((width, tok), BF), pltpu.VMEM((width, rows), BF),
            pltpu.VMEM((2, tok, rows), F32), pltpu.VMEM((width, rows), BF),
            dma((8,)), dma((3,)), dma((3,)), dma((n_clips, sp // 2)), dma((n_clips, sp // 2)), dma((n_clips, sp // 2)), dma((n_clips, sp // 2)),
        ],
        compiler_params=pltpu.CompilerParams(collective_id=2, has_side_effects=True, vmem_limit_bytes=56 << 20),
        name='decode',
    )(hid, w_ed, mask_all, pos_all, mask_token, wqkv, wproj, wup, wdown)


def solution(mesh):
    sp = mesh.shape['sp']

    def local_program(patches, vis_mask, enc_pos, dec_pos, w_pe, b_pe, enc_qkv, enc_proj, enc_up, enc_down, w_ed, mask_token, dec_qkv, dec_proj, dec_up, dec_down, w_out):
        n_layers, width = enc_qkv.shape[:2]
        d_width = dec_qkv.shape[1]
        enc_qkv_t = jnp.transpose(enc_qkv, (0, 2, 3, 4, 1)).reshape(n_layers, 3 * width, width)
        dec_qkv_t = jnp.transpose(dec_qkv, (0, 2, 3, 4, 1)).reshape(n_layers, 3 * d_width, d_width)
        hid, mask_all, pos_all = encode(sp, vis_mask, patches, enc_pos, dec_pos, w_pe, b_pe, enc_qkv_t,
                                          enc_proj.reshape(n_layers, width, width), enc_up, enc_down)
        acts = decode(sp, hid, w_ed, mask_all, pos_all, mask_token, dec_qkv_t,
                      dec_proj.reshape(n_layers, d_width, d_width), dec_up, dec_down)
        return jnp.einsum('cne,ep->cnp', acts, w_out, preferred_element_type=F32)

    row_spec = P('dp', 'sp', None)
    pos_spec = P(('dp', 'sp'), None)
    arg_specs = (row_spec, P('dp', 'sp'), pos_spec, pos_spec) + (P(),) * 13
    return jax.shard_map(local_program, mesh=mesh, in_specs=arg_specs, out_specs=row_spec, check_vma=False)
```

```python
import functools

import jax
import jax.numpy as jnp
from jax import lax
from jax.experimental import pallas as pl
from jax.experimental.pallas import tpu as pltpu
from jax.sharding import PartitionSpec as P

KEEP_DIV = 8
HEADS_PER_STEP = 8


BF = jnp.bfloat16
F32 = jnp.float32
NT = (((1,), (1,)), ((), ()))
TN = (((0,), (0,)), ((), ()))
NN = (((1,), (0,)), ((), ()))
LOG2E = 1.4426950408889634
MESH = pl.DeviceIdType.MESH
VMEM = pl.BlockSpec(memory_space=pltpu.VMEM)
ANY = pl.BlockSpec(memory_space=pl.ANY)


def mm(lhs, rhs, dims=NN):
    return lax.dot_general(lhs, rhs, dims, preferred_element_type=F32)


def norm_rows(hidden):
    wide = hidden.astype(F32)
    centred = wide - jnp.mean(wide, axis=-1, keepdims=True)
    var = jnp.mean(centred * centred, axis=-1, keepdims=True)
    return (centred * lax.rsqrt(var + 1e-6)).astype(BF)


def gelu(x):
    return 0.5 * x * (1.0 + lax.erf(x * 0.7071067811865476))


def attend_clip(tok, rows, heads, hd, k_s, vt_s, q_s, s_s, o_s):
    c2 = hd ** -0.5 * LOG2E
    group = 256 // hd
    chunk = 256
    n_chunks = tok // chunk

    def q_of(h):
        g = h // group
        qg = q_s[pl.ds(pl.multiple_of(g * 256, 256), 256), :]
        row_head = lax.broadcasted_iota(jnp.int32, (256, rows), 0) // hd
        return jnp.where(row_head == h - g * group, qg, jnp.zeros_like(qg)), pl.multiple_of(g * 256, 256)

    def turn(nxt, nxt_slot, h, slot, top):
        qz, g0 = q_of(nxt)
        next_top = total = acc = None
        if h is not None:
            m = jnp.max(top, axis=0, keepdims=True) * c2
            v0 = pl.multiple_of(h * hd, hd)
        for j in range(n_chunks):
            at = slice(j * chunk, (j + 1) * chunk)
            s = mm(k_s[at, pl.ds(g0, 256)], qz)
            s_s[nxt_slot, at, :] = s
            t = jnp.max(s.reshape(chunk // 8, 8, rows), axis=0)
            next_top = t if next_top is None else jnp.maximum(next_top, t)
            if h is not None:
                e = jnp.exp2(s_s[slot, at, :] * c2 - m)
                t = jnp.sum(e.reshape(chunk // 8, 8, rows), axis=0)
                total = t if total is None else total + t
                a = mm(vt_s[pl.ds(v0, hd), at], e.astype(BF))
                acc = a if acc is None else acc + a
        if h is not None:
            o_s[pl.ds(v0, hd), :] = (acc / jnp.sum(total, axis=0, keepdims=True)).astype(BF)
        return next_top

    def body(i, top):
        for u in range(HEADS_PER_STEP):
            h = HEADS_PER_STEP * i + u
            top = turn(jnp.minimum(h + 1, heads - 1), (u + 1) % 2, h, u % 2, top)
        return top

    lax.fori_loop(0, heads // HEADS_PER_STEP, body, turn(0, 0, None, None, None))


def enc_kernel(sp, mask_ref, patches_h, enc_pos_h, dec_pos_h, w_pe_h, b_pe_ref, qkv_h, proj_h, up_h, down_h,
               hid_out, mask_all, pos_all,
               patches, enc_pos, w_pe, wqkv, wproj, wup, wdown, x_s, e_src, tail_s, win, hid, a_all, qkv_s, s_s, p_s, o_s, g_s,
               wsem, insem, ms, mr, ws, wr, es, er, asend, arecv, pfs, pfr, pns, pnr, lsem):
    me = lax.axis_index('sp')
    n_clips, rows, width = patches.shape[0], patches.shape[1], hid.shape[1]
    cap = e_src.shape[0] // n_clips
    half = tail_s.shape[0] // n_clips
    n_layers = qkv_h.shape[0]
    my_rows = hid.shape[0]
    per = sp // n_clips
    heads = 16
    hd = width // heads
    clip = me // per
    hf = lax.rem(me, 2)
    partner = me + 1 - 2 * hf
    my_half = me // per
    slot = lax.rem(me, per)

    def weight(l, i):
        src, dst = ((qkv_h, wqkv), (proj_h, wproj), (up_h, wup), (down_h, wdown))[i]
        return pltpu.make_async_copy(src.at[l], dst, wsem.at[i])

    loads = [pltpu.make_async_copy(a, b, insem.at[i]) for i, (a, b) in enumerate(
        [(patches_h, patches), (enc_pos_h, enc_pos), (w_pe_h, w_pe)])]
    for ld in loads:
        ld.start()

    barrier = pltpu.get_barrier_semaphore()
    for k in range(1, sp):
        pl.semaphore_signal(barrier, inc=1, device_id={'sp': lax.rem(me + k, sp)}, device_id_type=MESH)

    mask = mask_ref[...]
    maskf = mask.astype(F32)
    before = (lax.broadcasted_iota(jnp.int32, (rows, rows), 0) < lax.broadcasted_iota(jnp.int32, (rows, rows), 1))
    mask8 = jnp.concatenate([maskf] + [jnp.zeros_like(maskf)] * 7, axis=0).astype(BF)
    rank = mm(mask8, before.astype(BF)).astype(jnp.int32)
    row_id = lax.broadcasted_iota(jnp.int32, (cap, rows), 0)
    picks = []
    for c in range(n_clips):
        picks.append(jnp.where((row_id == rank[c:c + 1, :]) & (mask[c:c + 1, :] == 1), 1.0, 0.0))
    pick2 = jnp.concatenate(picks, axis=0)
    used = jnp.sum(pick2, axis=1, keepdims=True)
    pick2 = pick2.astype(BF)
    for ld in loads[:2]:
        ld.wait()
    for c in range(n_clips):
        x_s[c * cap:(c + 1) * cap, :] = mm(pick2[c * cap:(c + 1) * cap], patches[c]).astype(BF)
    fixed = used * b_pe_ref[...].reshape(1, width).astype(F32) + mm(pick2, enc_pos[...])
    loads[2].wait()
    weight(0, 0).start()
    e_src[...] = (mm(x_s[...], w_pe[...]) + fixed).astype(BF)
    late = lax.broadcasted_iota(jnp.int32, (half, cap), 1) - lax.broadcasted_iota(jnp.int32, (half, cap), 0) + half
    for c in range(n_clips):
        count = jnp.sum(maskf[c:c + 1, :], axis=1, keepdims=True).astype(jnp.int32)
        pick = jnp.where(late == count, 1.0, 0.0).astype(BF)
        tail_s[c * half:(c + 1) * half, :] = mm(pick, e_src[c * cap:(c + 1) * cap, :]).astype(BF)

    pl.semaphore_wait(barrier, sp - 1)

    def to(c, x, h):
        return per * c + 2 * x + h

    def send(c, x):
        return pltpu.make_async_remote_copy(
            src_ref=e_src.at[pl.ds(c * cap, cap)], dst_ref=win.at[pl.ds(pl.multiple_of(slot * cap, cap), cap)],
            send_sem=ws.at[c, x], recv_sem=wr.at[slot], device_id={'sp': to(c, x, my_half)}, device_id_type=MESH)

    last = per * cap
    edges = ((per, 0, e_src, cap), (per - 1, 1, tail_s, half))

    def send_edge(c, x, h, buf, step):
        return pltpu.make_async_remote_copy(
            src_ref=buf.at[pl.ds(c * step, half)], dst_ref=win.at[pl.ds(last, half)], send_sem=es.at[c, x], recv_sem=er,
            device_id={'sp': to(c, x, h)}, device_id_type=MESH)

    for c in range(n_clips):
        for x in range(per // 2):
            @pl.when(to(c, x, my_half) != me)
            def _():
                send(c, x).start()

            @pl.when(to(c, x, my_half) == me)
            def _():
                pltpu.make_async_copy(
                    e_src.at[pl.ds(c * cap, cap)], win.at[pl.ds(pl.multiple_of(slot * cap, cap), cap)], wr.at[slot]).start()

            for src_dev, h, buf, step in edges:
                @pl.when((me == src_dev) & (to(c, x, h) != me))
                def _():
                    send_edge(c, x, h, buf, step).start()

                @pl.when((me == src_dev) & (to(c, x, h) == me))
                def _():
                    pltpu.make_async_copy(buf.at[pl.ds(c * step, half)], win.at[pl.ds(last, half)], er).start()

    for i in range(1, 4):
        weight(0, i).start()
    mask_sends = []
    for k in range(1, sp):
        mask_sends.append(pltpu.make_async_remote_copy(
            src_ref=mask_ref, dst_ref=mask_all.at[me], send_sem=ms.at[k], recv_sem=mr.at[k],
            device_id={'sp': lax.rem(me + k, sp)}, device_id_type=MESH))
        mask_sends[-1].start()
    own_mask = pltpu.make_async_copy(mask_ref, mask_all.at[me], lsem.at[0])
    own_mask.start()
    for m in mask_sends:
        m.wait_recv()
    own_mask.wait()
    starts = [jnp.zeros((1, 1), F32)]
    for s in range(sp):
        both = mask_all[s].astype(F32)
        row = jnp.where(clip == 0, both[0:1, :], both[1:2, :])
        starts.append(starts[-1] + jnp.sum(row, axis=1, keepdims=True))
    out_row = lax.broadcasted_iota(jnp.int32, (my_rows, cap), 0) - lax.broadcasted_iota(jnp.int32, (my_rows, cap), 1)
    places = []
    for b in range(per):
        off = jnp.where(hf == 0, starts[b], starts[per + b] - my_rows).astype(jnp.int32)
        places.append(jnp.where(out_row == off, 1.0, 0.0))
    off = jnp.where(hf == 0, starts[per], starts[per] - half - my_rows).astype(jnp.int32)
    places.append(jnp.where(out_row[:, :half] == off, 1.0, 0.0))
    place_a = jnp.concatenate(places[:per], axis=1).astype(BF)
    place_b = places[per].astype(BF)

    for b in range(per):
        pltpu.make_async_copy(e_src.at[pl.ds(0, cap)], win.at[pl.ds(b * cap, cap)], wr.at[b]).wait()
    pltpu.make_async_copy(e_src.at[pl.ds(0, half)], win.at[pl.ds(last, half)], er).wait()
    hid[...] = (mm(place_a, win[:last, :]) + mm(place_b, win[last:, :])).astype(BF)

    scale = hd ** -0.5
    pos_own = pltpu.make_async_copy(dec_pos_h, pos_all.at[me], lsem.at[1])
    pos_own.start()

    def pos_far(k):
        return pltpu.make_async_remote_copy(
            src_ref=dec_pos_h, dst_ref=pos_all.at[me], send_sem=pfs.at[k], recv_sem=pfr.at[k],
            device_id={'sp': lax.rem(me + 2 * k, sp)}, device_id_type=MESH)

    def pos_near(k):
        piece = lax.rem(me + 2 * k, sp)
        return pltpu.make_async_remote_copy(
            src_ref=pos_all.at[piece], dst_ref=pos_all.at[piece], send_sem=pns.at[k], recv_sem=pnr.at[k],
            device_id={'sp': partner}, device_id_type=MESH)

    def layer(l, carry):
        def refill(i):
            @pl.when(l < n_layers - 1)
            def _():
                weight(l + 1, i).start()

        a_all[l, 0] = norm_rows(hid[...])
        swap = pltpu.make_async_remote_copy(
            src_ref=a_all.at[l, 0], dst_ref=a_all.at[l, 1], send_sem=asend.at[l], recv_sem=arecv.at[l],
            device_id={'sp': partner}, device_id_type=MESH)
        swap.start()
        weight(l, 0).wait()
        qkv_s[:width, :my_rows] = mm(wqkv[:width, :], a_all[l, 0], NT).astype(BF)
        swap.wait()
        qkv_s[width:, :] = mm(wqkv[width:, :], a_all[l].reshape(2 * my_rows, width), NT).astype(BF)
        refill(0)

        @pl.when(l == 0)
        def _():
            for k in range(1, sp // 2):
                pos_far(k).start()

        for h in range(heads):
            s_s[h] = mm(qkv_s[h * hd:(h + 1) * hd, :my_rows], qkv_s[width + h * hd:width + (h + 1) * hd, :], TN)

        def soft(i, cc):
            s = s_s[i] * scale
            e = jnp.exp(s - jnp.max(s, axis=-1, keepdims=True))
            p_s[i] = (e / jnp.sum(e, axis=-1, keepdims=True)).astype(BF)
            return cc

        lax.fori_loop(0, heads, soft, 0, unroll=16)
        for h in range(heads):
            o_s[h * hd:(h + 1) * hd, :] = mm(qkv_s[2 * width + h * hd:2 * width + (h + 1) * hd, :], p_s[h], NT).astype(BF)
        weight(l, 1).wait()
        h1 = (hid[...].astype(F32) + mm(o_s[...], wproj[...], TN)).astype(BF)
        hid[...] = h1
        refill(1)
        a2 = norm_rows(h1)
        weight(l, 2).wait()
        g_s[...] = gelu(mm(a2, wup[...])).astype(BF)
        refill(2)

        @pl.when(l == n_layers - 1)
        def _():
            pos_own.wait()
            for k in range(1, sp // 2):
                pos_far(k).wait_recv()
            for k in range(sp // 2):
                pos_near(k).start()

        weight(l, 3).wait()
        hid[...] = (hid[...].astype(F32) + mm(g_s[...], wdown[...])).astype(BF)
        refill(3)
        return carry

    lax.fori_loop(0, n_layers, layer, 0)

    hid_out[...] = hid[...]
    for m in mask_sends:
        m.wait_send()
    for c in range(n_clips):
        for x in range(per // 2):
            @pl.when(to(c, x, my_half) != me)
            def _():
                send(c, x).wait_send()

            for src_dev, h, buf, step in edges:
                @pl.when((me == src_dev) & (to(c, x, h) != me))
                def _():
                    send_edge(c, x, h, buf, step).wait_send()
    for k in range(1, sp // 2):
        pos_far(k).wait_send()
    for k in range(sp // 2):
        pos_near(k).wait()


def encode(sp, vis_mask, patches, enc_pos, dec_pos, w_pe, b_pe, qkv_t, proj, up, down):
    n_clips, rows, p_width = patches.shape
    width = w_pe.shape[1]
    d_width = dec_pos.shape[1]
    cap = 2 * rows // KEEP_DIV
    half = cap // 4
    my_rows = rows * sp // KEEP_DIV // 2
    dma = pltpu.SemaphoreType.DMA
    per = sp // n_clips
    far = sp // 2
    return pl.pallas_call(
        functools.partial(enc_kernel, sp),
        out_shape=(jax.ShapeDtypeStruct((my_rows, width), BF),
                   jax.ShapeDtypeStruct((sp, n_clips, rows), jnp.int32),
                   jax.ShapeDtypeStruct((sp, rows, d_width), BF)),
        in_specs=[VMEM, ANY, ANY, ANY, ANY, VMEM, ANY, ANY, ANY, ANY],
        out_specs=(VMEM, VMEM, ANY),
        scratch_shapes=[
            pltpu.VMEM(patches.shape, BF), pltpu.VMEM(enc_pos.shape, BF), pltpu.VMEM(w_pe.shape, BF),
            pltpu.VMEM(qkv_t.shape[1:], BF), pltpu.VMEM(proj.shape[1:], BF), pltpu.VMEM(up.shape[1:], BF), pltpu.VMEM(down.shape[1:], BF),
            pltpu.VMEM((n_clips * cap, p_width), BF), pltpu.VMEM((n_clips * cap, width), BF), pltpu.VMEM((n_clips * half, width), BF),
            pltpu.VMEM((per * cap + half, width), BF),
            pltpu.VMEM((my_rows, width), BF), pltpu.VMEM((qkv_t.shape[0], 2, my_rows, width), BF),
            pltpu.VMEM((3 * width, 2 * my_rows), BF),
            pltpu.VMEM((16, my_rows, 2 * my_rows), F32), pltpu.VMEM((16, my_rows, 2 * my_rows), BF),
            pltpu.VMEM((width, my_rows), BF), pltpu.VMEM((my_rows, 4 * width), BF),
            dma((4,)), dma((4,)), dma((sp,)), dma((sp,)), dma((n_clips, per // 2)), dma((per,)), dma((n_clips, per // 2)), dma,
            dma((2,)), dma((2,)), dma((far,)), dma((far,)), dma((far,)), dma((far,)), dma((2,)),
        ],
        compiler_params=pltpu.CompilerParams(collective_id=1, has_side_effects=True, vmem_limit_bytes=63 << 20),
        name='encode',
    )(vis_mask, patches, enc_pos, dec_pos, w_pe, b_pe, qkv_t, proj, up, down)


def decode_kernel(sp, hid_h, w_ed_h, mask_h, pos_h, tok_ref, wqkv_h, wproj_h, wup_h, wdown_h, a_out,
                  hid, w_ed, mask_all, pos, wqkv, wproj, wup, wdown, z_s, rank_s, u_s, a_own, a_all, km_s, vm_s, pv_s, k_s, vt_s, q_s, s_s, o_s,
                  insem, zs, zr, fs, fr, ns, nr):
    me = lax.axis_index('sp')
    hf = lax.rem(me, 2)
    partner = me + 1 - 2 * hf
    n_clips, n_vis, width = z_s.shape
    rows = mask_all.shape[2]
    my_rows = hid.shape[0]
    per = sp // n_clips
    clip_of = me // per
    tok = rows * sp
    heads, hd = 16, width // 16
    n_far = sp // 2

    loads = [pltpu.make_async_copy(a, b, insem.at[i]) for i, (a, b) in enumerate(
        [(hid_h, hid), (w_ed_h, w_ed), (mask_h, mask_all), (pos_h, pos), (wqkv_h, wqkv), (wproj_h, wproj), (wup_h, wup), (wdown_h, wdown)])]
    for ld in loads:
        ld.start()
    barrier = pltpu.get_barrier_semaphore()
    for k in range(1, sp):
        pl.semaphore_signal(barrier, inc=1, device_id={'sp': lax.rem(me + k, sp)}, device_id_type=MESH)

    at = pl.multiple_of(hf * my_rows, my_rows)
    mine = z_s.at[clip_of, pl.ds(at, my_rows), :]
    theirs = z_s.at[n_clips - 1 - clip_of, pl.ds(at, my_rows), :]
    for ld in loads[:2]:
        ld.wait()
    z_s[clip_of, pl.ds(at, my_rows), :] = mm(norm_rows(hid[...]), w_ed[...]).astype(BF)
    pl.semaphore_wait(barrier, sp - 1)

    def z_send(i, ref, dst):
        return pltpu.make_async_remote_copy(
            src_ref=ref, dst_ref=ref, send_sem=zs.at[i], recv_sem=zr.at[i], device_id={'sp': dst}, device_id_type=MESH)

    across = z_send(0, mine, lax.rem(me + per, sp))
    beside = z_send(1, mine, partner)
    relayed = z_send(2, theirs, partner)
    across.start()
    beside.start()

    before = (lax.broadcasted_iota(jnp.int32, (rows, rows), 0) < lax.broadcasted_iota(jnp.int32, (rows, rows), 1)).astype(BF)
    row_id = lax.broadcasted_iota(jnp.int32, (n_vis, rows), 0)
    loads[2].wait()
    for c in range(n_clips):
        m = mask_all[:, c, :]
        local = mm(m.astype(F32).astype(BF), before)
        base = jnp.zeros((1, 1), F32)
        for s in range(sp):
            vis = m[s:s + 1, :]
            rank_s[c, s:s + 1, :] = jnp.where(vis == 1, (local[s:s + 1, :] + base).astype(jnp.int32), n_vis)
            base = base + jnp.sum(vis.astype(F32), axis=1, keepdims=True)
    for ld in loads[3:5]:
        ld.wait()

    def pick_of(c, b):
        return jnp.where(row_id == rank_s[c, pl.ds(b, 1), :], 1.0, 0.0).astype(BF)

    def keys_values(l, b, blk, k_to, vt_to):
        here = pl.ds(pl.multiple_of(b * rows, rows), rows)
        k_to[here, :] = mm(blk, wqkv[l, width:2 * width, :], NT).astype(BF)
        vt_to[:, here] = mm(wqkv[l, 2 * width:, :], blk, NT).astype(BF)

    token = tok_ref[...].reshape(1, width).astype(F32)
    pv_s[...] = jnp.zeros_like(pv_s)

    def plain(b, cc):
        keys_values(0, b, norm_rows((token + pos[b].astype(F32)).astype(BF)), km_s, vm_s)
        for c in range(n_clips):
            pv_s[c] += mm(pick_of(c, b), pos[b])
        return cc

    lax.fori_loop(0, sp, plain, 0, unroll=4)

    def far(c, k):
        return pltpu.make_async_remote_copy(
            src_ref=a_own.at[c], dst_ref=a_all.at[c, me], send_sem=fs.at[c, k], recv_sem=fr.at[c, k],
            device_id={'sp': lax.rem(me + 2 * k, sp)}, device_id_type=MESH)

    def near(c, k):
        piece = lax.rem(me + 2 * k, sp)
        return pltpu.make_async_remote_copy(
            src_ref=a_all.at[c, piece] if k else a_own.at[c], dst_ref=a_all.at[c, piece],
            send_sem=ns.at[c, k], recv_sem=nr.at[c, k], device_id={'sp': partner}, device_id_type=MESH)

    def relay(c):
        for k in range(1, n_far):
            far(c, k).wait_recv()
        for k in range(n_far):
            near(c, k).start()

    def attend(l, c):
        q_s[...] = mm(wqkv[l, :width, :], a_own[c], NT).astype(BF)
        attend_clip(tok, rows, heads, hd, k_s, vt_s, q_s, s_s, o_s)

    def feed(l, c):
        h1 = (u_s[c].astype(F32) + mm(o_s[...], wproj[l], TN)).astype(BF)
        g = gelu(mm(norm_rows(h1), wup[l])).astype(BF)
        return (h1.astype(F32) + mm(g, wdown[l])).astype(BF)

    across.wait_recv()
    relayed.start()
    beside.wait_recv()
    relayed.wait_recv()

    def first(c, carry):
        u_vis = (z_s[c].astype(F32) + pv_s[c]).astype(BF)
        a_vis = norm_rows(u_vis)
        k_vis = mm(a_vis, wqkv[0, width:2 * width, :], NT).astype(BF)
        vt_vis = mm(wqkv[0, 2 * width:, :], a_vis, NT).astype(BF)
        k_aug = jnp.concatenate([k_vis, jnp.ones((n_vis, 128), BF)], axis=1)
        u_aug = jnp.concatenate([u_vis, jnp.ones((n_vis, 128), BF)], axis=1)

        def put(pick, aug, plain_rows):
            got = mm(pick, aug, TN)
            seen = jnp.concatenate([got[:, width:]] * (width // 128), axis=1)
            return jnp.where(seen > 0.5, got[:, :width], plain_rows.astype(F32)).astype(BF)

        def block(b, cc):
            here = pl.ds(pl.multiple_of(b * rows, rows), rows)
            pick = pick_of(c, b)
            k_s[here, :] = put(pick, k_aug, km_s[here, :])
            seen = rank_s[c, pl.ds(b, 1), :] < n_vis
            vt_s[:, here] = jnp.where(seen, mm(vt_vis, pick), vm_s[:, here].astype(F32)).astype(BF)
            return cc

        lax.fori_loop(0, sp, block, 0, unroll=8)
        u = put(pick_of(c, me), u_aug, (token + pos[me].astype(F32)).astype(BF))
        u_s[c] = u
        a_own[c] = norm_rows(u)
        attend(0, c)

        @pl.when(c == 0)
        def _():
            for ld in loads[5:]:
                ld.wait()

        @pl.when(c == 1)
        def _():
            relay(0)

        u1 = feed(0, c)
        u_s[c] = u1
        a_own[c] = norm_rows(u1)
        for k in range(1, n_far):
            far(c, k).start()
        return carry

    lax.fori_loop(0, n_clips, first, 0)

    def second(c, carry):
        keys_values(1, me, a_own[c], k_s, vt_s)

        def same(k, cc):
            b = lax.rem(me + 2 * k, sp)
            keys_values(1, b, a_all[c, b], k_s, vt_s)
            return cc

        def other(k, cc):
            b = lax.rem(partner + 2 * k, sp)
            keys_values(1, b, a_all[c, b], k_s, vt_s)
            return cc

        lax.fori_loop(1, n_far, same, 0, unroll=True)
        for k in range(n_far):
            near(c, k).wait_recv()
        lax.fori_loop(0, n_far, other, 0, unroll=True)
        attend(1, c)

        @pl.when(c == 0)
        def _():
            relay(1)

        a_out[c] = norm_rows(feed(1, c))
        return carry

    lax.fori_loop(0, n_clips, second, 0)
    for c in range(n_clips):
        for k in range(n_far):
            near(c, k).wait_send()
            if k:
                far(c, k).wait_send()
    across.wait_send()
    beside.wait_send()
    relayed.wait_send()


def decode(sp, hid, w_ed, mask_all, pos_all, mask_token, wqkv, wproj, wup, wdown):
    _, n_clips, rows = mask_all.shape
    width = w_ed.shape[1]
    tok = rows * sp
    n_vis = tok // KEEP_DIV
    dma = pltpu.SemaphoreType.DMA
    return pl.pallas_call(
        functools.partial(decode_kernel, sp),
        out_shape=jax.ShapeDtypeStruct((n_clips, rows, width), BF),
        in_specs=[ANY, ANY, ANY, ANY, VMEM, ANY, ANY, ANY, ANY],
        out_specs=VMEM,
        scratch_shapes=[
            pltpu.VMEM(hid.shape, BF), pltpu.VMEM(w_ed.shape, BF), pltpu.VMEM(mask_all.shape, jnp.int32),
            pltpu.VMEM(pos_all.shape, BF), pltpu.VMEM(wqkv.shape, BF), pltpu.VMEM(wproj.shape, BF),
            pltpu.VMEM(wup.shape, BF), pltpu.VMEM(wdown.shape, BF),
            pltpu.VMEM((n_clips, n_vis, width), BF),
            pltpu.VMEM((n_clips, sp, rows), jnp.int32), pltpu.VMEM((n_clips, rows, width), BF), pltpu.VMEM((n_clips, rows, width), BF),
            pltpu.VMEM((n_clips, sp, rows, width), BF),
            pltpu.VMEM((tok, width), BF), pltpu.VMEM((width, tok), BF), pltpu.VMEM((n_clips, n_vis, width), F32),
            pltpu.VMEM((tok, width), BF), pltpu.VMEM((width, tok), BF), pltpu.VMEM((width, rows), BF),
            pltpu.VMEM((2, tok, rows), F32), pltpu.VMEM((width, rows), BF),
            dma((8,)), dma((3,)), dma((3,)), dma((n_clips, sp // 2)), dma((n_clips, sp // 2)), dma((n_clips, sp // 2)), dma((n_clips, sp // 2)),
        ],
        compiler_params=pltpu.CompilerParams(collective_id=2, has_side_effects=True, vmem_limit_bytes=56 << 20),
        name='decode',
    )(hid, w_ed, mask_all, pos_all, mask_token, wqkv, wproj, wup, wdown)


def solution(mesh):
    sp = mesh.shape['sp']

    def local_program(patches, vis_mask, enc_pos, dec_pos, w_pe, b_pe, enc_qkv, enc_proj, enc_up, enc_down, w_ed, mask_token, dec_qkv, dec_proj, dec_up, dec_down, w_out):
        n_layers, width = enc_qkv.shape[:2]
        d_width = dec_qkv.shape[1]
        enc_qkv_t = jnp.transpose(enc_qkv, (0, 2, 3, 4, 1)).reshape(n_layers, 3 * width, width)
        dec_qkv_t = jnp.transpose(dec_qkv, (0, 2, 3, 4, 1)).reshape(n_layers, 3 * d_width, d_width)
        hid, mask_all, pos_all = encode(sp, vis_mask, patches, enc_pos, dec_pos, w_pe, b_pe, enc_qkv_t,
                                          enc_proj.reshape(n_layers, width, width), enc_up, enc_down)
        acts = decode(sp, hid, w_ed, mask_all, pos_all, mask_token, dec_qkv_t,
                      dec_proj.reshape(n_layers, d_width, d_width), dec_up, dec_down)
        return jnp.einsum('cne,ep->cnp', acts, w_out, preferred_element_type=F32)

    row_spec = P('dp', 'sp', None)
    pos_spec = P(('dp', 'sp'), None)
    arg_specs = (row_spec, P('dp', 'sp'), pos_spec, pos_spec) + (P(),) * 13
    return jax.shard_map(local_program, mesh=mesh, in_specs=arg_specs, out_specs=row_spec, check_vma=False)
```

```python
import functools

import jax
import jax.numpy as jnp
from jax import lax
from jax.experimental import pallas as pl
from jax.experimental.pallas import tpu as pltpu
from jax.sharding import PartitionSpec as P

KEEP_DIV = 8
HEADS_PER_STEP = 8


BF = jnp.bfloat16
F32 = jnp.float32
NT = (((1,), (1,)), ((), ()))
TN = (((0,), (0,)), ((), ()))
NN = (((1,), (0,)), ((), ()))
LOG2E = 1.4426950408889634
MESH = pl.DeviceIdType.MESH
VMEM = pl.BlockSpec(memory_space=pltpu.VMEM)
ANY = pl.BlockSpec(memory_space=pl.ANY)


def mm(lhs, rhs, dims=NN):
    return lax.dot_general(lhs, rhs, dims, preferred_element_type=F32)


def norm_rows(hidden):
    wide = hidden.astype(F32)
    centred = wide - jnp.mean(wide, axis=-1, keepdims=True)
    var = jnp.mean(centred * centred, axis=-1, keepdims=True)
    return (centred * lax.rsqrt(var + 1e-6)).astype(BF)


def gelu(x):
    return 0.5 * x * (1.0 + lax.erf(x * 0.7071067811865476))


def attend_clip(tok, rows, heads, hd, k_s, vt_s, q_s, s_s, o_s):
    c2 = hd ** -0.5 * LOG2E
    group = 256 // hd
    chunk = 256
    n_chunks = tok // chunk

    def q_of(h):
        g = h // group
        qg = q_s[pl.ds(pl.multiple_of(g * 256, 256), 256), :]
        row_head = lax.broadcasted_iota(jnp.int32, (256, rows), 0) // hd
        return jnp.where(row_head == h - g * group, qg, jnp.zeros_like(qg)), pl.multiple_of(g * 256, 256)

    def turn(nxt, nxt_slot, h, slot, top):
        qz, g0 = q_of(nxt)
        next_top = total = acc = None
        if h is not None:
            m = jnp.max(top, axis=0, keepdims=True) * c2
            v0 = pl.multiple_of(h * hd, hd)
        for j in range(n_chunks):
            at = slice(j * chunk, (j + 1) * chunk)
            s = mm(k_s[at, pl.ds(g0, 256)], qz)
            s_s[nxt_slot, at, :] = s
            for r in range(0, chunk, 64):
                t = jnp.max(s[r:r + 64].reshape(8, 8, rows), axis=0)
                next_top = t if next_top is None else jnp.maximum(next_top, t)
            if h is not None:
                weights = []
                for r in range(j * chunk, (j + 1) * chunk, 64):
                    e = jnp.exp2(s_s[slot, r:r + 64, :] * c2 - m)
                    t = jnp.sum(e.reshape(8, 8, rows), axis=0)
                    total = t if total is None else total + t
                    weights.append(e.astype(BF))
                a = mm(vt_s[pl.ds(v0, hd), at], jnp.concatenate(weights, axis=0))
                acc = a if acc is None else acc + a
        if h is not None:
            o_s[pl.ds(v0, hd), :] = (acc / jnp.sum(total, axis=0, keepdims=True)).astype(BF)
        return next_top

    def body(i, top):
        for u in range(HEADS_PER_STEP):
            h = HEADS_PER_STEP * i + u
            top = turn(jnp.minimum(h + 1, heads - 1), (u + 1) % 2, h, u % 2, top)
        return top

    lax.fori_loop(0, heads // HEADS_PER_STEP, body, turn(0, 0, None, None, None))


def enc_kernel(sp, mask_ref, patches_h, enc_pos_h, dec_pos_h, w_pe_h, b_pe_ref, qkv_h, proj_h, up_h, down_h,
               hid_out, mask_all, pos_all,
               patches, enc_pos, w_pe, wqkv, wproj, wup, wdown, x_s, e_src, tail_s, win, hid, a_all, qkv_s, s_s, p_s, o_s, g_s,
               wsem, insem, ms, mr, ws, wr, es, er, asend, arecv, pfs, pfr, pns, pnr, lsem):
    me = lax.axis_index('sp')
    n_clips, rows, width = patches.shape[0], patches.shape[1], hid.shape[1]
    cap = e_src.shape[0] // n_clips
    half = tail_s.shape[0] // n_clips
    n_layers = qkv_h.shape[0]
    my_rows = hid.shape[0]
    per = sp // n_clips
    heads = 16
    hd = width // heads
    clip = me // per
    hf = lax.rem(me, 2)
    partner = me + 1 - 2 * hf
    my_half = me // per
    slot = lax.rem(me, per)

    def weight(l, i):
        src, dst = ((qkv_h, wqkv), (proj_h, wproj), (up_h, wup), (down_h, wdown))[i]
        return pltpu.make_async_copy(src.at[l], dst, wsem.at[i])

    loads = [pltpu.make_async_copy(a, b, insem.at[i]) for i, (a, b) in enumerate(
        [(patches_h, patches), (enc_pos_h, enc_pos), (w_pe_h, w_pe)])]
    for ld in loads:
        ld.start()

    barrier = pltpu.get_barrier_semaphore()
    for k in range(1, sp):
        pl.semaphore_signal(barrier, inc=1, device_id={'sp': lax.rem(me + k, sp)}, device_id_type=MESH)

    mask = mask_ref[...]
    maskf = mask.astype(F32)
    before = (lax.broadcasted_iota(jnp.int32, (rows, rows), 0) < lax.broadcasted_iota(jnp.int32, (rows, rows), 1))
    mask8 = jnp.concatenate([maskf] + [jnp.zeros_like(maskf)] * 7, axis=0).astype(BF)
    rank = mm(mask8, before.astype(BF)).astype(jnp.int32)
    row_id = lax.broadcasted_iota(jnp.int32, (cap, rows), 0)
    picks = []
    for c in range(n_clips):
        picks.append(jnp.where((row_id == rank[c:c + 1, :]) & (mask[c:c + 1, :] == 1), 1.0, 0.0))
    pick2 = jnp.concatenate(picks, axis=0)
    used = jnp.sum(pick2, axis=1, keepdims=True)
    pick2 = pick2.astype(BF)
    for ld in loads[:2]:
        ld.wait()
    for c in range(n_clips):
        x_s[c * cap:(c + 1) * cap, :] = mm(pick2[c * cap:(c + 1) * cap], patches[c]).astype(BF)
    fixed = used * b_pe_ref[...].reshape(1, width).astype(F32) + mm(pick2, enc_pos[...])
    loads[2].wait()
    weight(0, 0).start()
    e_src[...] = (mm(x_s[...], w_pe[...]) + fixed).astype(BF)
    late = lax.broadcasted_iota(jnp.int32, (half, cap), 1) - lax.broadcasted_iota(jnp.int32, (half, cap), 0) + half
    for c in range(n_clips):
        count = jnp.sum(maskf[c:c + 1, :], axis=1, keepdims=True).astype(jnp.int32)
        pick = jnp.where(late == count, 1.0, 0.0).astype(BF)
        tail_s[c * half:(c + 1) * half, :] = mm(pick, e_src[c * cap:(c + 1) * cap, :]).astype(BF)

    pl.semaphore_wait(barrier, sp - 1)

    def to(c, x, h):
        return per * c + 2 * x + h

    def send(c, x):
        return pltpu.make_async_remote_copy(
            src_ref=e_src.at[pl.ds(c * cap, cap)], dst_ref=win.at[pl.ds(pl.multiple_of(slot * cap, cap), cap)],
            send_sem=ws.at[c, x], recv_sem=wr.at[slot], device_id={'sp': to(c, x, my_half)}, device_id_type=MESH)

    last = per * cap
    edges = ((per, 0, e_src, cap), (per - 1, 1, tail_s, half))

    def send_edge(c, x, h, buf, step):
        return pltpu.make_async_remote_copy(
            src_ref=buf.at[pl.ds(c * step, half)], dst_ref=win.at[pl.ds(last, half)], send_sem=es.at[c, x], recv_sem=er,
            device_id={'sp': to(c, x, h)}, device_id_type=MESH)

    for c in range(n_clips):
        for x in range(per // 2):
            @pl.when(to(c, x, my_half) != me)
            def _():
                send(c, x).start()

            @pl.when(to(c, x, my_half) == me)
            def _():
                pltpu.make_async_copy(
                    e_src.at[pl.ds(c * cap, cap)], win.at[pl.ds(pl.multiple_of(slot * cap, cap), cap)], wr.at[slot]).start()

            for src_dev, h, buf, step in edges:
                @pl.when((me == src_dev) & (to(c, x, h) != me))
                def _():
                    send_edge(c, x, h, buf, step).start()

                @pl.when((me == src_dev) & (to(c, x, h) == me))
                def _():
                    pltpu.make_async_copy(buf.at[pl.ds(c * step, half)], win.at[pl.ds(last, half)], er).start()

    for i in range(1, 4):
        weight(0, i).start()
    mask_sends = []
    for k in range(1, sp):
        mask_sends.append(pltpu.make_async_remote_copy(
            src_ref=mask_ref, dst_ref=mask_all.at[me], send_sem=ms.at[k], recv_sem=mr.at[k],
            device_id={'sp': lax.rem(me + k, sp)}, device_id_type=MESH))
        mask_sends[-1].start()
    own_mask = pltpu.make_async_copy(mask_ref, mask_all.at[me], lsem.at[0])
    own_mask.start()
    for m in mask_sends:
        m.wait_recv()
    own_mask.wait()
    starts = [jnp.zeros((1, 1), F32)]
    for s in range(sp):
        both = mask_all[s].astype(F32)
        row = jnp.where(clip == 0, both[0:1, :], both[1:2, :])
        starts.append(starts[-1] + jnp.sum(row, axis=1, keepdims=True))
    out_row = lax.broadcasted_iota(jnp.int32, (my_rows, cap), 0) - lax.broadcasted_iota(jnp.int32, (my_rows, cap), 1)
    places = []
    for b in range(per):
        off = jnp.where(hf == 0, starts[b], starts[per + b] - my_rows).astype(jnp.int32)
        places.append(jnp.where(out_row == off, 1.0, 0.0))
    off = jnp.where(hf == 0, starts[per], starts[per] - half - my_rows).astype(jnp.int32)
    places.append(jnp.where(out_row[:, :half] == off, 1.0, 0.0))
    place_a = jnp.concatenate(places[:per], axis=1).astype(BF)
    place_b = places[per].astype(BF)

    for b in range(per):
        pltpu.make_async_copy(e_src.at[pl.ds(0, cap)], win.at[pl.ds(b * cap, cap)], wr.at[b]).wait()
    pltpu.make_async_copy(e_src.at[pl.ds(0, half)], win.at[pl.ds(last, half)], er).wait()
    hid[...] = (mm(place_a, win[:last, :]) + mm(place_b, win[last:, :])).astype(BF)

    scale = hd ** -0.5
    pos_own = pltpu.make_async_copy(dec_pos_h, pos_all.at[me], lsem.at[1])
    pos_own.start()

    def pos_far(k):
        return pltpu.make_async_remote_copy(
            src_ref=dec_pos_h, dst_ref=pos_all.at[me], send_sem=pfs.at[k], recv_sem=pfr.at[k],
            device_id={'sp': lax.rem(me + 2 * k, sp)}, device_id_type=MESH)

    def pos_near(k):
        piece = lax.rem(me + 2 * k, sp)
        return pltpu.make_async_remote_copy(
            src_ref=pos_all.at[piece], dst_ref=pos_all.at[piece], send_sem=pns.at[k], recv_sem=pnr.at[k],
            device_id={'sp': partner}, device_id_type=MESH)

    def layer(l, carry):
        def refill(i):
            @pl.when(l < n_layers - 1)
            def _():
                weight(l + 1, i).start()

        a_all[l, 0] = norm_rows(hid[...])
        swap = pltpu.make_async_remote_copy(
            src_ref=a_all.at[l, 0], dst_ref=a_all.at[l, 1], send_sem=asend.at[l], recv_sem=arecv.at[l],
            device_id={'sp': partner}, device_id_type=MESH)
        swap.start()
        weight(l, 0).wait()
        qkv_s[:width, :my_rows] = mm(wqkv[:width, :], a_all[l, 0], NT).astype(BF)
        swap.wait()
        qkv_s[width:, :] = mm(wqkv[width:, :], a_all[l].reshape(2 * my_rows, width), NT).astype(BF)
        refill(0)

        @pl.when(l == 0)
        def _():
            for k in range(1, sp // 2):
                pos_far(k).start()

        for h in range(heads):
            s_s[h] = mm(qkv_s[h * hd:(h + 1) * hd, :my_rows], qkv_s[width + h * hd:width + (h + 1) * hd, :], TN)

        def soft(i, cc):
            s = s_s[i] * scale
            e = jnp.exp(s - jnp.max(s, axis=-1, keepdims=True))
            p_s[i] = (e / jnp.sum(e, axis=-1, keepdims=True)).astype(BF)
            return cc

        lax.fori_loop(0, heads, soft, 0, unroll=16)
        for h in range(heads):
            o_s[h * hd:(h + 1) * hd, :] = mm(qkv_s[2 * width + h * hd:2 * width + (h + 1) * hd, :], p_s[h], NT).astype(BF)
        weight(l, 1).wait()
        h1 = (hid[...].astype(F32) + mm(o_s[...], wproj[...], TN)).astype(BF)
        hid[...] = h1
        refill(1)
        a2 = norm_rows(h1)
        weight(l, 2).wait()
        g_s[...] = gelu(mm(a2, wup[...])).astype(BF)
        refill(2)

        @pl.when(l == n_layers - 1)
        def _():
            pos_own.wait()
            for k in range(1, sp // 2):
                pos_far(k).wait_recv()
            for k in range(sp // 2):
                pos_near(k).start()

        weight(l, 3).wait()
        hid[...] = (hid[...].astype(F32) + mm(g_s[...], wdown[...])).astype(BF)
        refill(3)
        return carry

    lax.fori_loop(0, n_layers, layer, 0)

    hid_out[...] = hid[...]
    for m in mask_sends:
        m.wait_send()
    for c in range(n_clips):
        for x in range(per // 2):
            @pl.when(to(c, x, my_half) != me)
            def _():
                send(c, x).wait_send()

            for src_dev, h, buf, step in edges:
                @pl.when((me == src_dev) & (to(c, x, h) != me))
                def _():
                    send_edge(c, x, h, buf, step).wait_send()
    for k in range(1, sp // 2):
        pos_far(k).wait_send()
    for k in range(sp // 2):
        pos_near(k).wait()


def encode(sp, vis_mask, patches, enc_pos, dec_pos, w_pe, b_pe, qkv_t, proj, up, down):
    n_clips, rows, p_width = patches.shape
    width = w_pe.shape[1]
    d_width = dec_pos.shape[1]
    cap = 2 * rows // KEEP_DIV
    half = cap // 4
    my_rows = rows * sp // KEEP_DIV // 2
    dma = pltpu.SemaphoreType.DMA
    per = sp // n_clips
    far = sp // 2
    return pl.pallas_call(
        functools.partial(enc_kernel, sp),
        out_shape=(jax.ShapeDtypeStruct((my_rows, width), BF),
                   jax.ShapeDtypeStruct((sp, n_clips, rows), jnp.int32),
                   jax.ShapeDtypeStruct((sp, rows, d_width), BF)),
        in_specs=[VMEM, ANY, ANY, ANY, ANY, VMEM, ANY, ANY, ANY, ANY],
        out_specs=(VMEM, VMEM, ANY),
        scratch_shapes=[
            pltpu.VMEM(patches.shape, BF), pltpu.VMEM(enc_pos.shape, BF), pltpu.VMEM(w_pe.shape, BF),
            pltpu.VMEM(qkv_t.shape[1:], BF), pltpu.VMEM(proj.shape[1:], BF), pltpu.VMEM(up.shape[1:], BF), pltpu.VMEM(down.shape[1:], BF),
            pltpu.VMEM((n_clips * cap, p_width), BF), pltpu.VMEM((n_clips * cap, width), BF), pltpu.VMEM((n_clips * half, width), BF),
            pltpu.VMEM((per * cap + half, width), BF),
            pltpu.VMEM((my_rows, width), BF), pltpu.VMEM((qkv_t.shape[0], 2, my_rows, width), BF),
            pltpu.VMEM((3 * width, 2 * my_rows), BF),
            pltpu.VMEM((16, my_rows, 2 * my_rows), F32), pltpu.VMEM((16, my_rows, 2 * my_rows), BF),
            pltpu.VMEM((width, my_rows), BF), pltpu.VMEM((my_rows, 4 * width), BF),
            dma((4,)), dma((4,)), dma((sp,)), dma((sp,)), dma((n_clips, per // 2)), dma((per,)), dma((n_clips, per // 2)), dma,
            dma((2,)), dma((2,)), dma((far,)), dma((far,)), dma((far,)), dma((far,)), dma((2,)),
        ],
        compiler_params=pltpu.CompilerParams(collective_id=1, has_side_effects=True, vmem_limit_bytes=63 << 20),
        name='encode',
    )(vis_mask, patches, enc_pos, dec_pos, w_pe, b_pe, qkv_t, proj, up, down)


def decode_kernel(sp, hid_h, w_ed_h, mask_h, pos_h, tok_ref, wqkv_h, wproj_h, wup_h, wdown_h, a_out,
                  hid, w_ed, mask_all, pos, wqkv, wproj, wup, wdown, z_s, rank_s, u_s, a_own, a_all, km_s, vm_s, pv_s, k_s, vt_s, q_s, s_s, o_s,
                  insem, zs, zr, fs, fr, ns, nr):
    me = lax.axis_index('sp')
    hf = lax.rem(me, 2)
    partner = me + 1 - 2 * hf
    n_clips, n_vis, width = z_s.shape
    rows = mask_all.shape[2]
    my_rows = hid.shape[0]
    per = sp // n_clips
    clip_of = me // per
    tok = rows * sp
    heads, hd = 16, width // 16
    n_far = sp // 2

    loads = [pltpu.make_async_copy(a, b, insem.at[i]) for i, (a, b) in enumerate(
        [(hid_h, hid), (w_ed_h, w_ed), (mask_h, mask_all), (pos_h, pos), (wqkv_h, wqkv), (wproj_h, wproj), (wup_h, wup), (wdown_h, wdown)])]
    for ld in loads:
        ld.start()
    barrier = pltpu.get_barrier_semaphore()
    for k in range(1, sp):
        pl.semaphore_signal(barrier, inc=1, device_id={'sp': lax.rem(me + k, sp)}, device_id_type=MESH)

    at = pl.multiple_of(hf * my_rows, my_rows)
    mine = z_s.at[clip_of, pl.ds(at, my_rows), :]
    theirs = z_s.at[n_clips - 1 - clip_of, pl.ds(at, my_rows), :]
    for ld in loads[:2]:
        ld.wait()
    z_s[clip_of, pl.ds(at, my_rows), :] = mm(norm_rows(hid[...]), w_ed[...]).astype(BF)
    pl.semaphore_wait(barrier, sp - 1)

    def z_send(i, ref, dst):
        return pltpu.make_async_remote_copy(
            src_ref=ref, dst_ref=ref, send_sem=zs.at[i], recv_sem=zr.at[i], device_id={'sp': dst}, device_id_type=MESH)

    across = z_send(0, mine, lax.rem(me + per, sp))
    beside = z_send(1, mine, partner)
    relayed = z_send(2, theirs, partner)
    across.start()
    beside.start()

    before = (lax.broadcasted_iota(jnp.int32, (rows, rows), 0) < lax.broadcasted_iota(jnp.int32, (rows, rows), 1)).astype(BF)
    row_id = lax.broadcasted_iota(jnp.int32, (n_vis, rows), 0)
    loads[2].wait()
    for c in range(n_clips):
        m = mask_all[:, c, :]
        local = mm(m.astype(F32).astype(BF), before)
        base = jnp.zeros((1, 1), F32)
        for s in range(sp):
            vis = m[s:s + 1, :]
            rank_s[c, s:s + 1, :] = jnp.where(vis == 1, (local[s:s + 1, :] + base).astype(jnp.int32), n_vis)
            base = base + jnp.sum(vis.astype(F32), axis=1, keepdims=True)
    for ld in loads[3:5]:
        ld.wait()

    def pick_of(c, b):
        return jnp.where(row_id == rank_s[c, pl.ds(b, 1), :], 1.0, 0.0).astype(BF)

    def keys_values(l, b, blk, k_to, vt_to):
        here = pl.ds(pl.multiple_of(b * rows, rows), rows)
        k_to[here, :] = mm(blk, wqkv[l, width:2 * width, :], NT).astype(BF)
        vt_to[:, here] = mm(wqkv[l, 2 * width:, :], blk, NT).astype(BF)

    token = tok_ref[...].reshape(1, width).astype(F32)
    pv_s[...] = jnp.zeros_like(pv_s)

    def plain(b, cc):
        keys_values(0, b, norm_rows((token + pos[b].astype(F32)).astype(BF)), km_s, vm_s)
        for c in range(n_clips):
            pv_s[c] += mm(pick_of(c, b), pos[b])
        return cc

    lax.fori_loop(0, sp, plain, 0, unroll=8)

    def far(c, k):
        return pltpu.make_async_remote_copy(
            src_ref=a_own.at[c], dst_ref=a_all.at[c, me], send_sem=fs.at[c, k], recv_sem=fr.at[c, k],
            device_id={'sp': lax.rem(me + 2 * k, sp)}, device_id_type=MESH)

    def near(c, k):
        piece = lax.rem(me + 2 * k, sp)
        return pltpu.make_async_remote_copy(
            src_ref=a_all.at[c, piece] if k else a_own.at[c], dst_ref=a_all.at[c, piece],
            send_sem=ns.at[c, k], recv_sem=nr.at[c, k], device_id={'sp': partner}, device_id_type=MESH)

    def relay(c):
        for k in range(1, n_far):
            far(c, k).wait_recv()
        for k in range(n_far):
            near(c, k).start()

    def attend(l, c):
        q_s[...] = mm(wqkv[l, :width, :], a_own[c], NT).astype(BF)
        attend_clip(tok, rows, heads, hd, k_s, vt_s, q_s, s_s, o_s)

    def feed(l, c):
        h1 = (u_s[c].astype(F32) + mm(o_s[...], wproj[l], TN)).astype(BF)
        g = gelu(mm(norm_rows(h1), wup[l])).astype(BF)
        return (h1.astype(F32) + mm(g, wdown[l])).astype(BF)

    across.wait_recv()
    relayed.start()
    beside.wait_recv()
    relayed.wait_recv()

    def first(c, carry):
        u_vis = (z_s[c].astype(F32) + pv_s[c]).astype(BF)
        a_vis = norm_rows(u_vis)
        k_vis = mm(a_vis, wqkv[0, width:2 * width, :], NT).astype(BF)
        vt_vis = mm(wqkv[0, 2 * width:, :], a_vis, NT).astype(BF)
        k_aug = jnp.concatenate([k_vis, jnp.ones((n_vis, 128), BF)], axis=1)
        u_aug = jnp.concatenate([u_vis, jnp.ones((n_vis, 128), BF)], axis=1)

        def put(pick, aug, plain_rows):
            got = mm(pick, aug, TN)
            seen = jnp.concatenate([got[:, width:]] * (width // 128), axis=1)
            return jnp.where(seen > 0.5, got[:, :width], plain_rows.astype(F32)).astype(BF)

        def block(b, cc):
            here = pl.ds(pl.multiple_of(b * rows, rows), rows)
            pick = pick_of(c, b)
            k_s[here, :] = put(pick, k_aug, km_s[here, :])
            seen = rank_s[c, pl.ds(b, 1), :] < n_vis
            vt_s[:, here] = jnp.where(seen, mm(vt_vis, pick), vm_s[:, here].astype(F32)).astype(BF)
            return cc

        lax.fori_loop(0, sp, block, 0, unroll=8)
        u = put(pick_of(c, me), u_aug, (token + pos[me].astype(F32)).astype(BF))
        u_s[c] = u
        a_own[c] = norm_rows(u)
        attend(0, c)

        @pl.when(c == 0)
        def _():
            for ld in loads[5:]:
                ld.wait()

        @pl.when(c == 1)
        def _():
            relay(0)

        u1 = feed(0, c)
        u_s[c] = u1
        a_own[c] = norm_rows(u1)
        for k in range(1, n_far):
            far(c, k).start()
        return carry

    lax.fori_loop(0, n_clips, first, 0)

    def second(c, carry):
        keys_values(1, me, a_own[c], k_s, vt_s)

        def same(k, cc):
            b = lax.rem(me + 2 * k, sp)
            keys_values(1, b, a_all[c, b], k_s, vt_s)
            return cc

        def other(k, cc):
            b = lax.rem(partner + 2 * k, sp)
            keys_values(1, b, a_all[c, b], k_s, vt_s)
            return cc

        lax.fori_loop(1, n_far, same, 0, unroll=True)
        for k in range(n_far):
            near(c, k).wait_recv()
        lax.fori_loop(0, n_far, other, 0, unroll=True)
        attend(1, c)

        @pl.when(c == 0)
        def _():
            relay(1)

        a_out[c] = norm_rows(feed(1, c))
        return carry

    lax.fori_loop(0, n_clips, second, 0)
    for c in range(n_clips):
        for k in range(n_far):
            near(c, k).wait_send()
            if k:
                far(c, k).wait_send()
    across.wait_send()
    beside.wait_send()
    relayed.wait_send()


def decode(sp, hid, w_ed, mask_all, pos_all, mask_token, wqkv, wproj, wup, wdown):
    _, n_clips, rows = mask_all.shape
    width = w_ed.shape[1]
    tok = rows * sp
    n_vis = tok // KEEP_DIV
    dma = pltpu.SemaphoreType.DMA
    return pl.pallas_call(
        functools.partial(decode_kernel, sp),
        out_shape=jax.ShapeDtypeStruct((n_clips, rows, width), BF),
        in_specs=[ANY, ANY, ANY, ANY, VMEM, ANY, ANY, ANY, ANY],
        out_specs=VMEM,
        scratch_shapes=[
            pltpu.VMEM(hid.shape, BF), pltpu.VMEM(w_ed.shape, BF), pltpu.VMEM(mask_all.shape, jnp.int32),
            pltpu.VMEM(pos_all.shape, BF), pltpu.VMEM(wqkv.shape, BF), pltpu.VMEM(wproj.shape, BF),
            pltpu.VMEM(wup.shape, BF), pltpu.VMEM(wdown.shape, BF),
            pltpu.VMEM((n_clips, n_vis, width), BF),
            pltpu.VMEM((n_clips, sp, rows), jnp.int32), pltpu.VMEM((n_clips, rows, width), BF), pltpu.VMEM((n_clips, rows, width), BF),
            pltpu.VMEM((n_clips, sp, rows, width), BF),
            pltpu.VMEM((tok, width), BF), pltpu.VMEM((width, tok), BF), pltpu.VMEM((n_clips, n_vis, width), F32),
            pltpu.VMEM((tok, width), BF), pltpu.VMEM((width, tok), BF), pltpu.VMEM((width, rows), BF),
            pltpu.VMEM((2, tok, rows), F32), pltpu.VMEM((width, rows), BF),
            dma((8,)), dma((3,)), dma((3,)), dma((n_clips, sp // 2)), dma((n_clips, sp // 2)), dma((n_clips, sp // 2)), dma((n_clips, sp // 2)),
        ],
        compiler_params=pltpu.CompilerParams(collective_id=2, has_side_effects=True, vmem_limit_bytes=56 << 20),
        name='decode',
    )(hid, w_ed, mask_all, pos_all, mask_token, wqkv, wproj, wup, wdown)


def solution(mesh):
    sp = mesh.shape['sp']

    def local_program(patches, vis_mask, enc_pos, dec_pos, w_pe, b_pe, enc_qkv, enc_proj, enc_up, enc_down, w_ed, mask_token, dec_qkv, dec_proj, dec_up, dec_down, w_out):
        n_layers, width = enc_qkv.shape[:2]
        d_width = dec_qkv.shape[1]
        enc_qkv_t = jnp.transpose(enc_qkv, (0, 2, 3, 4, 1)).reshape(n_layers, 3 * width, width)
        dec_qkv_t = jnp.transpose(dec_qkv, (0, 2, 3, 4, 1)).reshape(n_layers, 3 * d_width, d_width)
        hid, mask_all, pos_all = encode(sp, vis_mask, patches, enc_pos, dec_pos, w_pe, b_pe, enc_qkv_t,
                                          enc_proj.reshape(n_layers, width, width), enc_up, enc_down)
        acts = decode(sp, hid, w_ed, mask_all, pos_all, mask_token, dec_qkv_t,
                      dec_proj.reshape(n_layers, d_width, d_width), dec_up, dec_down)
        return jnp.einsum('cne,ep->cnp', acts, w_out, preferred_element_type=F32)

    row_spec = P('dp', 'sp', None)
    pos_spec = P(('dp', 'sp'), None)
    arg_specs = (row_spec, P('dp', 'sp'), pos_spec, pos_spec) + (P(),) * 13
    return jax.shard_map(local_program, mesh=mesh, in_specs=arg_specs, out_specs=row_spec, check_vma=False)
```
